128 devices in a mesh: ox: 8 (over z, x_lo), oy: 16 (over x_hi, y, core).
Axes of the slice: x: 4 (x_hi: 2, x_lo: 2; x = x_hi * 2 + x_lo), y: 4, z: 4, core: 2. Of those that a mesh axis runs over, the one named last changes fastest.
Arguments:
- zonal_flow: float32 [4, 1024, 2048], P(None, 'ox', 'oy'), may hold values from -3 to 3
- merid_flow: float32 [4, 1024, 2048], P(None, 'ox', 'oy'), may hold values from -3 to 3
- thickness: float32 [4, 1024, 2048], P(None, 'ox', 'oy'), may hold values from 0.8 to 2
- land_sea: int32 [1024, 2048], P('ox', 'oy'), may hold values 0 or 1
- viscosity: float32 [1024, 2048], P('ox', 'oy'), may hold values from 0.2 to 3
- wind_stress: float32 [2, 1024, 2048], P(None, 'ox', 'oy'), may hold values from -5 to 5
- reduced_gravity: float32 [4], replicated, may hold values from 0.1 to 1
- conv_first: bfloat16 [3, 3, 64, 4], replicated, may hold values from -1 to 1
- bias_first: float32 [64], replicated, may hold values from -3 to 3
- conv_second: bfloat16 [3, 3, 64, 64], replicated, may hold values from -0.25 to 0.25
- bias_second: float32 [64], replicated, may hold values from -3 to 3
- conv_last: bfloat16 [3, 3, 1, 64], replicated, may hold values from -0.25 to 0.25
Outputs:
- zonal_next: float32 [4, 1024, 2048], P(None, 'ox', 'oy')
- merid_next: float32 [4, 1024, 2048], P(None, 'ox', 'oy')
- thickness_next: float32 [4, 1024, 2048], P(None, 'ox', 'oy')
- viscosity_next: float32 [1024, 2048], P('ox', 'oy')
The draws below stay inside these ranges and needn't reach their ends.
Inputs may be any that keep to these rules, and one draw needn't show every extreme that they name: `land_sea`: 1 marks a sea cell.
All inputs are finite; a program needn't handle non-finite values. No bound on the sum of `land_sea` on one device may be relied on, other than what follows from the above.
Results may differ from the reference program's by a relative error of at most 0.0019.
Values may be sent and summed in bfloat16 or wider, within the bound.
A program may use at most 192 MiB of HBM per device.

```python
import math
import jax
import jax.numpy as jnp
from jax import lax

CX = 128
LAYERS = 4
FEATURES = 4
HIDDEN_SIZE = 64
NX = 1024
NY = 2048


def with_ends(entries, key, low, largest):
    place = [jax.random.randint(jax.random.fold_in(key, axis), (), 0, length) for axis, length in enumerate(entries.shape)]
    widest = entries.shape.index(max(entries.shape))
    neighbour = place[:widest] + [(place[widest] + 1) % entries.shape[widest]] + place[widest + 1:]
    return entries.at[tuple(place)].set(low).at[tuple(neighbour)].set(largest)


def block_scale(own_key, dims, split, low, top_value):
    loudness, own = 1.0, jax.random.fold_in(own_key, 6)
    for position, shards_of in split:
        steps = jnp.exp(jax.random.uniform(jax.random.fold_in(own, position), (shards_of,), jnp.float32, low / len(split), top_value / len(split)))
        loudness = loudness * jnp.repeat(steps, dims[position] // shards_of).reshape([-1 if axis == position else 1 for axis in range(len(dims))])
    return loudness


def scatter_about(rng, dims, scale, most, pieces=(), held_as=jnp.bfloat16):
    loudness = block_scale(rng, dims, pieces, -0.22, 0.18) if pieces else 1.0
    entries = jax.random.normal(rng, dims, jnp.float32) * scale * loudness
    return jnp.minimum(jnp.maximum(entries, -most), most).astype(held_as)


def setup_inputs(seed: int = 0) -> dict:
    splits = jax.random.split(jax.random.key(seed), 13)
    zonal_flow = scatter_about(splits[0], (LAYERS, NX, NY), 0.5, 3.0, ((1, 8), (2, 16)), jnp.float32)
    merid_flow = scatter_about(splits[1], (LAYERS, NX, NY), 0.5, 3.0, ((1, 8), (2, 16)), jnp.float32)
    thickness = jnp.clip(0.8 + 1.2 * jax.random.uniform(splits[2], (LAYERS, NX, NY), jnp.float32) ** block_scale(splits[2], (LAYERS, NX, NY), ((1, 8), (2, 16)), -0.2, 0.2), 0.8, 2.0)
    land_sea = with_ends((jax.random.randint(splits[3], (NX, NY), 0, 5) < 4).astype(jnp.int32), jax.random.fold_in(splits[3], 1), 0, 1)
    viscosity = jnp.clip(jnp.exp(math.log(3.0) - 2.7080502 * jax.random.uniform(splits[4], (NX, NY), jnp.float32) ** block_scale(splits[4], (NX, NY), ((0, 8), (1, 16)), -0.2, 0.2)), 0.2, 3.0)
    wind_stress = scatter_about(splits[5], (2, NX, NY), 1.0, 5.0, ((1, 8), (2, 16)), jnp.float32)
    reduced_gravity = jnp.clip(jnp.exp(jax.random.uniform(splits[6], (LAYERS,), jnp.float32, math.log(0.1), math.log(1.0))), 0.1, 1.0)
    conv_first = scatter_about(splits[7], (3, 3, HIDDEN_SIZE, FEATURES), (9 * FEATURES) ** -0.5, 1.0)
    bias_first = scatter_about(splits[8], (HIDDEN_SIZE,), 0.5, 3.0, (), jnp.float32)
    conv_second = scatter_about(splits[9], (3, 3, HIDDEN_SIZE, HIDDEN_SIZE), (9 * HIDDEN_SIZE) ** -0.5, 0.25)
    bias_second = scatter_about(splits[10], (HIDDEN_SIZE,), 0.5, 3.0, (), jnp.float32)
    conv_last = scatter_about(splits[11], (3, 3, 1, HIDDEN_SIZE), (9 * HIDDEN_SIZE) ** -0.5, 0.25)
    return dict(zonal_flow=zonal_flow, merid_flow=merid_flow, thickness=thickness, land_sea=land_sea, viscosity=viscosity, wind_stress=wind_stress, reduced_gravity=reduced_gravity, conv_first=conv_first, bias_first=bias_first, conv_second=conv_second, bias_second=bias_second, conv_last=conv_last)


TIME_STEP = 0.05
REST_DEPTH = 1.4
DRAG_RATE = 0.5


def neighbours(field):
    east = jnp.roll(field, -1, axis=-2)
    west = jnp.roll(field, 1, axis=-2)
    zeros = jnp.zeros_like(field[..., :1])
    north = jnp.concatenate([field[..., 1:], zeros], axis=-1)
    south = jnp.concatenate([zeros, field[..., :-1]], axis=-1)
    return east, west, north, south


def viscous(field, near, visc, visc_near):
    total = 0.5 * (visc + visc_near[0]) * (near[0] - field)
    for side in range(1, 4):
        total = total + 0.5 * (visc + visc_near[side]) * (near[side] - field)
    return total


def conv_valid(extended, weight):
    width = extended.shape[1] - 2
    height = extended.shape[2] - 2
    total = jnp.zeros((weight.shape[2], width, height), jnp.float32)
    for row_off in range(3):
        for col_off in range(3):
            total = total + jnp.einsum("oc,cxy->oxy", weight[row_off, col_off].astype(jnp.float32),
                                       extended[:, row_off:row_off + width, col_off:col_off + height])
    return total


def pad_lat(field):
    return jnp.pad(field, ((0, 0), (0, 0), (1, 1)))


def reference(zonal_flow, merid_flow, thickness, land_sea, viscosity, wind_stress, reduced_gravity,
              conv_first, bias_first, conv_second, bias_second, conv_last):
    sea = land_sea.astype(jnp.float32)
    zonal_m = zonal_flow * sea
    merid_m = merid_flow * sea
    flux_x = zonal_m * thickness
    flux_y = merid_m * thickness
    flux_e, flux_w, unused_n, unused_s = neighbours(flux_x)
    unused_e, unused_w, flux_n, flux_s = neighbours(flux_y)
    diverge = (flux_e - flux_w) * 0.5 + (flux_n - flux_s) * 0.5
    thickness_next = thickness - TIME_STEP * sea * diverge
    anomaly = thickness_next - REST_DEPTH
    interface = jnp.cumsum(anomaly[::-1], axis=0)[::-1]
    pressure = jnp.cumsum(reduced_gravity[:, None, None] * interface, axis=0)
    press_e, press_w, press_n, press_s = neighbours(pressure)
    grad_x = (press_e - press_w) * 0.5
    grad_y = (press_n - press_s) * 0.5
    visc_near = neighbours(viscosity)
    zonal_visc = viscous(zonal_m, neighbours(zonal_m), viscosity, visc_near)
    merid_visc = viscous(merid_m, neighbours(merid_m), viscosity, visc_near)
    lat_rows = jnp.arange(NY).astype(jnp.float32)
    coriolis = 0.3 + 1.4 * (lat_rows + 0.5) / NY
    layer_ids = jnp.arange(LAYERS)
    top = (layer_ids == 0).astype(jnp.float32)[:, None, None]
    bottom = (layer_ids == LAYERS - 1).astype(jnp.float32)[:, None, None]
    force_x = wind_stress[0] / thickness_next[0]
    force_y = wind_stress[1] / thickness_next[0]
    zonal_next = sea * (zonal_m + TIME_STEP * (coriolis * merid_m - grad_x + zonal_visc + top * force_x
                                               - DRAG_RATE * bottom * zonal_m))
    merid_next = sea * (merid_m + TIME_STEP * (-coriolis * zonal_m - grad_y + merid_visc + top * force_y
                                               - DRAG_RATE * bottom * merid_m))
    energy = 0.5 * jnp.sum(thickness_next * (zonal_next * zonal_next + merid_next * merid_next), axis=0)
    energy = energy / jnp.sum(thickness_next, axis=0)
    features = jnp.stack([zonal_next[0], merid_next[0], sea * (thickness_next[0] - REST_DEPTH),
                          sea * energy]).astype(jnp.bfloat16)

    def net_block(block):
        columns = ((block * CX - 3 + jnp.arange(CX + 6)) % NX).astype(jnp.int32)
        hidden = jnp.take(features, columns, axis=1).astype(jnp.float32)
        for weight, bias_term in ((conv_first, bias_first), (conv_second, bias_second)):
            summed = conv_valid(pad_lat(hidden), weight) + bias_term[:, None, None]
            rounded = jax.nn.silu(summed).astype(jnp.bfloat16)
            hidden = lax.optimization_barrier(rounded).astype(jnp.float32)
        output = conv_valid(pad_lat(hidden), conv_last)
        return jnp.exp(output[0])

    blocks = lax.map(net_block, jnp.arange(NX // CX).astype(jnp.int32))
    viscosity_next = blocks.reshape(NX, NY)
    return zonal_next, merid_next, thickness_next, viscosity_next
```

```python
import jax
import jax.numpy as jnp
from jax import lax
from jax.experimental import pallas as pl
from jax.experimental.pallas import tpu as pltpu
from jax.sharding import PartitionSpec as P

MESH = pl.DeviceIdType.MESH
F32 = jnp.float32
BF16 = jnp.bfloat16

DT = 0.05
REST = 1.4
DRAG = 0.5
LAYERS = 4
N = 128
HID = 64
FIELDS = 16
SEA, VISC, WIND = 12, 13, 14
EXT = N + 16
PAD = N + 32
WINDOWS = 17
GROUPS = 33
STEP = 3


def exchange_kernel(
    z, v, h, ls, vi, w, xw, xe, nh, sh, own, sea_i, sb, nb, load_sem, send_sem, recv_sem
):
    ox, oy = lax.axis_index("ox"), lax.axis_index("oy")
    nx, ny = lax.axis_size("ox"), lax.axis_size("oy")
    east, west = lax.rem(ox + 1, nx), lax.rem(ox + nx - 1, nx)
    north, south = lax.rem(oy + 1, ny), lax.rem(oy + ny - 1, ny)
    peers = (
        (east, oy), (west, oy), (ox, north), (ox, south),
        (east, north), (east, south), (west, north), (west, south),
    )
    barrier = pltpu.get_barrier_semaphore()
    for peer in peers:
        pl.semaphore_signal(barrier, inc=1, device_id=peer, device_id_type=MESH)
    loads = [
        pltpu.make_async_copy(src, dst, load_sem.at[k])
        for k, (src, dst) in enumerate((
            (z, own.at[0:4]), (v, own.at[4:8]), (h, own.at[8:12]), (ls, sea_i),
            (vi, own.at[VISC]), (w, own.at[WIND : WIND + 2]),
        ))
    ]
    for copy in loads:
        copy.start()
    for copy in loads:
        copy.wait()

    lane = lax.broadcasted_iota(jnp.int32, (8, N), 1)
    low = lax.rem(lane, 16) < 8

    def pack(k, carry):
        rows = pl.ds(pl.multiple_of(8 * k, 8), 8)
        own[SEA, rows, :] = sea_i[rows, :].astype(F32)
        halves = []
        for m in range(2):
            packed = own[8 * m, rows, :]
            for j in range(1, 8):
                moved = pltpu.roll(own[8 * m + j, rows, :], 16 * j, 1)
                packed = jnp.where((lane >= 16 * j - 8) & (lane < 16 * j + 8), moved, packed)
            halves.append(packed)
        sb[rows, :] = jnp.where(low, halves[0], pltpu.roll(halves[1], 8, 1))
        nb[rows, :] = jnp.where(low, pltpu.roll(halves[1], N - 8, 1), halves[0])
        return carry

    lax.fori_loop(0, N // 8, pack, 0)
    pl.semaphore_wait(barrier, 8)

    first, last = pl.ds(0, 8), pl.ds(N - 8, 8)
    moves = (
        (own.at[:, last], xw, (east, oy)),
        (own.at[:, first], xe, (west, oy)),
        (nb, sh.at[8 : 8 + N], (ox, north)),
        (sb, nh.at[8 : 8 + N], (ox, south)),
        (nb.at[last], sh.at[0:8], (east, north)),
        (sb.at[last], nh.at[0:8], (east, south)),
        (nb.at[first], sh.at[N + 8 : EXT], (west, north)),
        (sb.at[first], nh.at[N + 8 : EXT], (west, south)),
    )
    sends = [
        pltpu.make_async_remote_copy(
            src_ref=src, dst_ref=dst, send_sem=send_sem.at[k], recv_sem=recv_sem.at[k],
            device_id=peer, device_id_type=MESH,
        )
        for k, (src, dst, peer) in enumerate(moves)
    ]
    for copy in reversed(sends):
        copy.start()
    for copy in sends:
        copy.wait()


def exchange(z, v, h, ls, vi, w):
    any_spec = pl.BlockSpec(memory_space=pl.ANY)
    strip = jax.ShapeDtypeStruct((FIELDS, 8, N), F32)
    side = jax.ShapeDtypeStruct((EXT, N), F32)
    return pl.pallas_call(
        exchange_kernel,
        out_shape=(strip, strip, side, side),
        in_specs=[any_spec] * 6,
        out_specs=[any_spec] * 4,
        scratch_shapes=[
            pltpu.VMEM((FIELDS, N, N), F32),
            pltpu.VMEM((N, N), jnp.int32),
            pltpu.VMEM((N, N), F32),
            pltpu.VMEM((N, N), F32),
            pltpu.SemaphoreType.DMA((6,)),
            pltpu.SemaphoreType.DMA((8,)),
            pltpu.SemaphoreType.DMA((8,)),
        ],
        compiler_params=pltpu.CompilerParams(collective_id=0, has_side_effects=True),
        name="exchange",
    )(z, v, h, ls, vi, w)


def step_kernel(
    z, v, h, ls, vi, w, xw, xe, nh, sh, grav, first_w, first_b, second_w, second_b, last_w,
    z_out, v_out, h_out, visc_out,
    f0, f1, sea_i, ns, p0, p1, t0, t1, zo, vo, fs, h1, rs, re, load_sem, store_sem,
):
    oy, ny = lax.axis_index("oy"), lax.axis_size("oy")
    mid = pl.ds(16, N)
    loads = [
        pltpu.make_async_copy(src, dst, load_sem.at[k])
        for k, (src, dst) in enumerate((
            (z, f0.at[0:4, mid]), (v, f0.at[4:8, mid]), (h, f0.at[8:12, mid]), (ls, sea_i),
            (vi, f0.at[VISC, mid]), (w, f0.at[WIND : WIND + 2, mid]),
            (xw, f0.at[:, 8:16]), (xe, f0.at[:, N + 16 : N + 24]), (nh, ns.at[0]), (sh, ns.at[1]),
        ))
    ]
    for copy in loads:
        copy.start()

    ones = jnp.ones((8, N), F32)
    for rows in (pl.ds(0, 8), pl.ds(PAD - 8, 8)):
        for k in range(FIELDS):
            f0[k, rows, :] = ones
            f1[k, rows, :] = ones
        for k in range(LAYERS):
            p0[k, rows, :] = ones
            p1[k, rows, :] = ones

    lane = lax.broadcasted_iota(jnp.int32, (8, N), 1)
    low = lax.rem(lane, 16) < 8
    has_north = (oy < ny - 1).astype(F32)
    has_south = (oy > 0).astype(F32)
    inside = jnp.where(lane < N // 2, has_north, has_south)
    first_lane, last_lane = lane == 0, lane == N - 1

    def north(a, b):
        a, b = pltpu.roll(a, N - 1, 1), pltpu.roll(b, N - 1, 1)
        return jnp.where(last_lane, b, a), jnp.where(last_lane, a, b)

    def south(a, b):
        a, b = pltpu.roll(a, 1, 1), pltpu.roll(b, 1, 1)
        return jnp.where(first_lane, b, a), jnp.where(first_lane, a, b)

    for copy in loads:
        copy.wait()

    def centre_sea(k, carry):
        f0[SEA, pl.ds(pl.multiple_of(8 * k + 16, 8), 8), :] = sea_i[
            pl.ds(pl.multiple_of(8 * k, 8), 8), :
        ].astype(F32)
        return carry

    lax.fori_loop(0, N // 8, centre_sea, 0)

    def spread(k, carry):
        rows = pl.ds(pl.multiple_of(8 * k + 8, 8), 8)
        src = pl.ds(pl.multiple_of(8 * k, 8), 8)
        a, b = ns[0, src, :], ns[1, src, :]
        packs = (
            jnp.where(low, a, b),
            jnp.where(low, pltpu.roll(a, N - 8, 1), pltpu.roll(b, 8, 1)),
        )

        def side(field):
            pack, j = packs[field // 8], field % 8
            return pltpu.roll(pack, N - 16 * j, 1) if j else pack

        sea0 = f0[SEA, rows, :]
        sea1 = side(SEA) * inside
        f1[SEA, rows, :] = sea1
        f1[VISC, rows, :] = side(VISC) * inside
        for field in (8, 9, 10, 11, WIND, WIND + 1):
            f1[field, rows, :] = side(field)
        for field in range(8):
            f1[field, rows, :] = side(field) * sea1
            f0[field, rows, :] = f0[field, rows, :] * sea0
        return carry

    lax.fori_loop(0, EXT // 8, spread, 0)

    fields = (f0, f1)
    press = (p0, p1)
    depth = (t0, t1)

    def continuity(k, carry):
        start = 8 * k + 8
        rows = pl.ds(pl.multiple_of(start, 8), 8)
        up, down = pl.ds(start + 1, 8), pl.ds(start - 1, 8)
        seas = [f[SEA, rows, :] for f in fields]
        anomaly = [[], []]
        for l in range(LAYERS):
            thick = [f[8 + l, rows, :] for f in fields]
            fy = [f[4 + l, rows, :] * t for f, t in zip(fields, thick)]
            fn, fso = north(*fy), south(*fy)
            for t, f in enumerate(fields):
                fe = f[l, up, :] * f[8 + l, up, :]
                fw = f[l, down, :] * f[8 + l, down, :]
                diverge = (fe - fw) * 0.5 + (fn[t] - fso[t]) * 0.5
                new = thick[t] - DT * seas[t] * diverge
                depth[t][l, rows, :] = new
                anomaly[t].append(new - REST)
        for t in range(2):
            faces = [anomaly[t][3]]
            for l in (2, 1, 0):
                faces.insert(0, faces[0] + anomaly[t][l])
            total = None
            for l in range(LAYERS):
                term = grav[l] * faces[l]
                total = term if total is None else total + term
                press[t][l, rows, :] = total * inside if t else total
        return carry

    lax.fori_loop(0, EXT // 8, continuity, 0)

    copy_h = pltpu.make_async_copy(t0.at[:, mid], h_out, store_sem.at[0])
    copy_h.start()

    total_rows = N * ny
    base_row = oy * N
    shift = jnp.where(lane < N // 2, N, 0)
    row_ids = (
        (base_row + lane).astype(F32),
        (base_row + lane + jnp.where(lane < N // 2, N, -N)).astype(F32),
    )
    del shift
    coriolis = [0.3 + 1.4 * (r + 0.5) / total_rows for r in row_ids]

    def momentum(k, carry):
        start = 8 * k + 8
        rows = pl.ds(pl.multiple_of(start, 8), 8)
        up, down = pl.ds(start + 1, 8), pl.ds(start - 1, 8)
        seas = [f[SEA, rows, :] for f in fields]
        visc = [f[VISC, rows, :] for f in fields]
        vn, vs = north(*visc), south(*visc)
        coef = []
        for t, f in enumerate(fields):
            coef.append([
                0.5 * (visc[t] + other)
                for other in (f[VISC, up, :], f[VISC, down, :], vn[t], vs[t])
            ])
        kinetic = [None, None]
        column = [None, None]
        top = []
        for l in range(LAYERS):
            zc = [f[l, rows, :] for f in fields]
            vc = [f[4 + l, rows, :] for f in fields]
            pc = [p[l, rows, :] for p in press]
            zn, zs = north(*zc), south(*zc)
            wn, ws = north(*vc), south(*vc)
            pn, ps = north(*pc), south(*pc)
            for t, f in enumerate(fields):
                gx = (press[t][l, up, :] - press[t][l, down, :]) * 0.5
                gy = (pn[t] - ps[t]) * 0.5

                def lap(field, centre, n, s):
                    sides = (f[field, up, :], f[field, down, :], n, s)
                    total = coef[t][0] * (sides[0] - centre)
                    for c, q in zip(coef[t][1:], sides[1:]):
                        total = total + c * (q - centre)
                    return total

                thick = depth[t][l, rows, :]
                fz = coriolis[t] * vc[t] - gx + lap(l, zc[t], zn[t], zs[t])
                fv = -coriolis[t] * zc[t] - gy + lap(4 + l, vc[t], wn[t], ws[t])
                if l == 0:
                    fz = fz + f[WIND, rows, :] / thick
                    fv = fv + f[WIND + 1, rows, :] / thick
                if l == LAYERS - 1:
                    fz = fz - DRAG * zc[t]
                    fv = fv - DRAG * vc[t]
                z_new = seas[t] * (zc[t] + DT * fz)
                v_new = seas[t] * (vc[t] + DT * fv)
                if t == 0:
                    zo[l, rows, :] = z_new
                    vo[l, rows, :] = v_new
                part = thick * (z_new * z_new + v_new * v_new)
                kinetic[t] = part if l == 0 else kinetic[t] + part
                column[t] = thick if l == 0 else column[t] + thick
                if l == 0:
                    top.append([z_new, v_new, seas[t] * (thick - REST)])
        for t in range(2):
            top[t].append(seas[t] * (0.5 * kinetic[t] / column[t]))
        for c in range(4):
            pair = top[0][c], top[1][c]
            for b, both in enumerate((south(*pair), pair, north(*pair))):
                for t in range(2):
                    fs[4 * b + c, t, rows, :] = both[t]
        return carry

    lax.fori_loop(0, EXT // 8, momentum, 0)

    copy_z = pltpu.make_async_copy(zo.at[:, mid], z_out, store_sem.at[1])
    copy_v = pltpu.make_async_copy(vo.at[:, mid], v_out, store_sem.at[2])
    copy_z.start()
    copy_v.start()

    edge_row = lax.broadcasted_iota(jnp.int32, (EXT, N), 0)
    keep = jnp.where(edge_row < N, 1.0, jnp.where(edge_row < N + 8, has_north, has_south)) > 0.5
    half = lax.broadcasted_iota(jnp.int32, (16, 12 * 16), 0) < 8
    weights1 = first_w[...]
    bias1 = first_b[...]
    bias2 = second_b[...]

    def silu_of_half(x):
        return x + x * jnp.tanh(x)

    def first_layer(k, carry):
        rows = pl.ds(pl.multiple_of(8 * k + 8, 8), 16)
        turned = []
        for t in range(2):
            block = fs[:, t, rows, :].reshape(12 * 16, N)
            turned.append(block.T)
        edge = jnp.where(half, turned[1][0:16], turned[1][N - 16 : N])
        left = jnp.concatenate([turned[0], edge], axis=0).astype(BF16)
        for q in range(4):
            out = jnp.dot(left, weights1[:, 128 * q : 128 * q + 128], preferred_element_type=F32)
            out = silu_of_half(out + bias1)
            out = jnp.where(keep, out, 0.0)
            where = (2 * k + q // 2, q % 2)
            h1[(0, *where)] = pltpu.roll(out, 1, 0).astype(BF16)
            h1[(1, *where)] = out.astype(BF16)
            h1[(2, *where)] = pltpu.roll(out, EXT - 1, 0).astype(BF16)
        return carry

    lax.fori_loop(0, WINDOWS, first_layer, 0)

    keep_two = jnp.concatenate([keep, keep], axis=1)

    def second_layer(k, carry):
        g = k * STEP
        parts = []
        for b in range(3):
            for d in range(3):
                block = h1[b, pl.ds(g + d // 2, STEP), d % 2]
                parts.append(block.reshape(STEP * EXT, N))
        left = jnp.concatenate(parts, axis=1)
        out = jnp.dot(left, second_w[...], preferred_element_type=F32)
        for i in range(STEP):
            one = silu_of_half(out[i * EXT : (i + 1) * EXT] + bias2)
            one = jnp.where(keep_two, one, 0.0).astype(BF16)
            sums = lax.dot_general(
                last_w[...], one, (((1,), (1,)), ((), ())), preferred_element_type=F32
            )
            rs[g + i] = sums[0:24, 0:N]
            re[g + i, :, 0:16] = sums[0:24, N:EXT]
        return carry

    lax.fori_loop(0, GROUPS // STEP, second_layer, 0)

    upper = lax.broadcasted_iota(jnp.int32, (8, N), 0) < 4

    def last_layer(k, carry):
        g = 2 * k

        def column_sums(ref, b):
            x, y, zz = (ref[g + i, 8 * b : 8 * b + 8, :] for i in range(3))
            y = pltpu.roll(y, 4, 0)
            return jnp.where(upper, x, y) + jnp.where(upper, y, zz)

        inner = [column_sums(rs, b) for b in range(3)]
        from_south = column_sums(re, 0)
        from_north = column_sums(re, 2)
        low_part = jnp.where(
            first_lane, pltpu.roll(from_south, N - 15, 1), pltpu.roll(inner[0], 1, 1)
        )
        high_part = jnp.where(
            last_lane, pltpu.roll(from_north, N - 1, 1), pltpu.roll(inner[2], N - 1, 1)
        )
        visc_out[pl.ds(pl.multiple_of(8 * k, 8), 8), :] = jnp.exp(low_part + inner[1] + high_part)
        return carry

    lax.fori_loop(0, N // 8, last_layer, 0)
    copy_h.wait()
    copy_z.wait()
    copy_v.wait()


def step(fields, strips, grav, first_w, first_b, second_w, second_b, last_w):
    any_spec = pl.BlockSpec(memory_space=pl.ANY)
    vmem = pl.BlockSpec(memory_space=pltpu.VMEM)
    whole = jax.ShapeDtypeStruct((LAYERS, N, N), F32)
    return pl.pallas_call(
        step_kernel,
        out_shape=(whole, whole, whole, jax.ShapeDtypeStruct((N, N), F32)),
        in_specs=[any_spec] * 10 + [pl.BlockSpec(memory_space=pltpu.SMEM)] + [vmem] * 5,
        out_specs=[any_spec] * 3 + [vmem],
        scratch_shapes=[
            pltpu.VMEM((FIELDS, PAD, N), F32),
            pltpu.VMEM((FIELDS, PAD, N), F32),
            pltpu.VMEM((N, N), jnp.int32),
            pltpu.VMEM((2, EXT, N), F32),
            pltpu.VMEM((LAYERS, PAD, N), F32),
            pltpu.VMEM((LAYERS, PAD, N), F32),
            pltpu.VMEM((LAYERS, PAD, N), F32),
            pltpu.VMEM((LAYERS, PAD, N), F32),
            pltpu.VMEM((LAYERS, PAD, N), F32),
            pltpu.VMEM((LAYERS, PAD, N), F32),
            pltpu.VMEM((12, 2, PAD, N), F32),
            pltpu.VMEM((3, 2 * WINDOWS, 2, EXT, N), BF16),
            pltpu.VMEM((GROUPS, 24, N), F32),
            pltpu.VMEM((GROUPS, 24, N), F32),
            pltpu.SemaphoreType.DMA((10,)),
            pltpu.SemaphoreType.DMA((3,)),
        ],
        compiler_params=pltpu.CompilerParams(vmem_limit_bytes=56 * 2**20),
        name="step",
    )(*fields, *strips, grav, first_w, first_b, second_w, second_b, last_w)


def first_weights(conv, bias):
    taps = jnp.transpose(conv, (1, 3, 0, 2)) * BF16(0.5)
    out = [jnp.pad(taps, ((0, 0), (0, 0), (j + 4, 9 - j), (0, 0))) for j in range(8)]
    matrix = jnp.stack(out, axis=3).reshape(12 * 16, 8 * HID)
    return matrix, jnp.tile(bias * 0.5, 2)[None]


def second_weights(conv, bias):
    taps = jnp.transpose(conv, (1, 0, 3, 2)) * BF16(0.5)
    out = [jnp.pad(taps, ((0, 0), (j, 3 - j), (0, 0), (0, 0))) for j in range(4)]
    matrix = jnp.stack(out, axis=3).reshape(3 * 6 * HID, 4 * HID)
    return matrix, jnp.tile(bias * 0.5, 4)[None]


def last_weights(conv):
    taps = conv[:, :, 0, :]
    zero = jnp.zeros((3, HID), BF16)
    rows = []
    for place in (3, 4, 5, None, None, 0, 1, 2):
        row = []
        for m in range(4):
            a = -1 if place is None else m - place + 2
            row.append(taps[a] if 0 <= a < 3 else zero)
        rows.append(jnp.concatenate(row, axis=1))
    matrix = jnp.stack(rows, axis=1).reshape(24, 4 * HID)
    return jnp.pad(matrix, ((0, 8), (0, 0)))


def local(z, v, h, ls, vi, w, grav, conv1, bias1, conv2, bias2, conv3):
    fields = (z, v, h, ls, vi, w)
    strips = exchange(*fields)
    w1, b1 = first_weights(conv1, bias1)
    w2, b2 = second_weights(conv2, bias2)
    return step(fields, strips, grav, w1, b1, w2, b2, last_weights(conv3))


def solution(mesh):
    block, flat = P(None, "ox", "oy"), P("ox", "oy")
    return jax.shard_map(
        local,
        mesh=mesh,
        in_specs=(block, block, block, flat, flat, block) + (P(),) * 6,
        out_specs=(block, block, block, flat),
        check_vma=False,
    )
```

```python
import jax
import jax.numpy as jnp
from jax import lax
from jax.experimental import pallas as pl
from jax.experimental.pallas import tpu as pltpu
from jax.sharding import PartitionSpec as P

MESH = pl.DeviceIdType.MESH
F32 = jnp.float32
BF16 = jnp.bfloat16

DT = 0.05
REST = 1.4
DRAG = 0.5
LAYERS = 4
N = 128
HID = 64
FIELDS = 16
SEA, VISC, WIND = 12, 13, 14
EXT = N + 16
PAD = N + 32
TALL = N + 40
PAIRS = 72
GROUPS = 33
STEP = 3
TILES = EXT // 16
BLOCK = STEP * EXT


def exchange_kernel(
    z, v, h, ls, vi, w, xw, xe, nh, sh, own, sea_i, sb, nb, load_sem, send_sem, recv_sem
):
    ox, oy = lax.axis_index("ox"), lax.axis_index("oy")
    nx, ny = lax.axis_size("ox"), lax.axis_size("oy")
    east, west = lax.rem(ox + 1, nx), lax.rem(ox + nx - 1, nx)
    north, south = lax.rem(oy + 1, ny), lax.rem(oy + ny - 1, ny)
    peers = (
        (east, oy), (west, oy), (ox, north), (ox, south),
        (east, north), (east, south), (west, north), (west, south),
    )
    barrier = pltpu.get_barrier_semaphore()
    for peer in peers:
        pl.semaphore_signal(barrier, inc=1, device_id=peer, device_id_type=MESH)
    loads = [
        pltpu.make_async_copy(src, dst, load_sem.at[k])
        for k, (src, dst) in enumerate((
            (z, own.at[0:4]), (v, own.at[4:8]), (h, own.at[8:12]), (ls, sea_i),
            (vi, own.at[VISC]), (w, own.at[WIND : WIND + 2]),
        ))
    ]
    for copy in loads:
        copy.start()
    for copy in loads:
        copy.wait()

    lane = lax.broadcasted_iota(jnp.int32, (8, N), 1)
    low = lax.rem(lane, 16) < 8

    def pack(k, carry):
        rows = pl.ds(pl.multiple_of(8 * k, 8), 8)
        own[SEA, rows, :] = sea_i[rows, :].astype(F32)
        halves = []
        for m in range(2):
            packed = own[8 * m, rows, :]
            for j in range(1, 8):
                moved = pltpu.roll(own[8 * m + j, rows, :], 16 * j, 1)
                packed = jnp.where((lane >= 16 * j - 8) & (lane < 16 * j + 8), moved, packed)
            halves.append(packed)
        sb[rows, :] = jnp.where(low, halves[0], pltpu.roll(halves[1], 8, 1))
        nb[rows, :] = jnp.where(low, pltpu.roll(halves[1], N - 8, 1), halves[0])
        return carry

    lax.fori_loop(0, N // 8, pack, 0)
    pl.semaphore_wait(barrier, 8)

    first, last = pl.ds(0, 8), pl.ds(N - 8, 8)
    moves = (
        (own.at[:, last], xw, (east, oy)),
        (own.at[:, first], xe, (west, oy)),
        (nb, sh.at[8 : 8 + N], (ox, north)),
        (sb, nh.at[8 : 8 + N], (ox, south)),
        (nb.at[last], sh.at[0:8], (east, north)),
        (sb.at[last], nh.at[0:8], (east, south)),
        (nb.at[first], sh.at[N + 8 : EXT], (west, north)),
        (sb.at[first], nh.at[N + 8 : EXT], (west, south)),
    )
    sends = [
        pltpu.make_async_remote_copy(
            src_ref=src, dst_ref=dst, send_sem=send_sem.at[k], recv_sem=recv_sem.at[k],
            device_id=peer, device_id_type=MESH,
        )
        for k, (src, dst, peer) in enumerate(moves)
    ]
    for copy in reversed(sends):
        copy.start()
    for copy in sends:
        copy.wait()


def exchange(z, v, h, ls, vi, w):
    any_spec = pl.BlockSpec(memory_space=pl.ANY)
    strip = jax.ShapeDtypeStruct((FIELDS, 8, N), F32)
    side = jax.ShapeDtypeStruct((EXT, N), F32)
    return pl.pallas_call(
        exchange_kernel,
        out_shape=(strip, strip, side, side),
        in_specs=[any_spec] * 6,
        out_specs=[any_spec] * 4,
        scratch_shapes=[
            pltpu.VMEM((FIELDS, N, N), F32),
            pltpu.VMEM((N, N), jnp.int32),
            pltpu.VMEM((N, N), F32),
            pltpu.VMEM((N, N), F32),
            pltpu.SemaphoreType.DMA((6,)),
            pltpu.SemaphoreType.DMA((8,)),
            pltpu.SemaphoreType.DMA((8,)),
        ],
        compiler_params=pltpu.CompilerParams(collective_id=0, has_side_effects=True),
        name="exchange",
    )(z, v, h, ls, vi, w)


def build_weights(conv1, conv2, conv3, first_w, second_w, last_w, rows24):
    lane = lax.broadcasted_iota(jnp.int32, (8, N), 1)
    right = lane >= HID
    row = lax.broadcasted_iota(jnp.int32, (8, N), 0)

    scale = lax.broadcasted_iota(jnp.int32, (16, 4), 0) == lax.broadcasted_iota(jnp.int32, (16, 4), 1)
    scale = jnp.where(scale, 0.5, 0.0).astype(BF16)
    nt = (((1,), (1,)), ((), ()))
    taps = {}
    for a in range(3):
        for b in range(3):
            one = conv1[a, b]
            both = jnp.concatenate([one, one], axis=0)
            taps[a, b] = lax.dot_general(scale, both, nt, preferred_element_type=F32)
    for b in range(3):
        for c in range(4):
            vecs = [jnp.broadcast_to(taps[a, b][c : c + 1], (8, N)) for a in range(3)]
            for jp in range(8):
                parts = []
                for i in range(4):
                    gap = row + 8 * i - 2 * jp - jnp.where(right, 1, 0) - 4
                    val = jnp.zeros((8, N), F32)
                    for a in range(3):
                        val = jnp.where(gap == a, vecs[a], val)
                    parts.append(val)
                start = 128 * b + 32 * c
                first_w[start : start + 32, N * jp : N * jp + N] = jnp.concatenate(parts, 0).astype(BF16)

    eye = lax.broadcasted_iota(jnp.int32, (HID, HID), 0) == lax.broadcasted_iota(jnp.int32, (HID, HID), 1)
    eye = jnp.where(eye, 0.5, 0.0).astype(BF16)
    side = lax.broadcasted_iota(jnp.int32, (HID, N), 1) >= HID
    for b in range(3):
        turned = []
        for a in range(3):
            one = conv2[a, b]
            both = jnp.concatenate([one, one], axis=0)
            turned.append(lax.dot_general(eye, both, nt, preferred_element_type=F32))
        zero = jnp.zeros((HID, N), F32)
        for m in range(6):
            for jp in range(2):
                tap = m - 2 * jp
                left = turned[tap] if 0 <= tap < 3 else zero
                other = turned[tap - 1] if 0 <= tap - 1 < 3 else zero
                start = (6 * b + m) * HID
                second_w[start : start + HID, N * jp : N * jp + N] = jnp.where(side, other, left).astype(BF16)

    rows24[...] = jnp.zeros((32, 2 * N), F32)
    for b in range(3):
        for place, i in ((0, 3), (1, 4), (2, 5), (5, 0), (6, 1), (7, 2)):
            for m in range(4):
                a = m - i + 2
                if 0 <= a < 3:
                    rows24[8 * b + place : 8 * b + place + 1, HID * m : HID * m + HID] = conv3[a, b].astype(F32)
    last_w[...] = rows24[...].astype(BF16)


def step_kernel(
    z, v, h, ls, vi, w, xw, xe, nh, sh, grav, conv1, bias1, conv2, bias2, conv3,
    z_out, v_out, h_out, visc_out,
    f0, f1, sea_i, ns, p0, p1, t0, t1, zo, vo, fs, ft, h1, d0, d1, rs, re, nat,
    first_w, second_w, last_w, rows24, load_sem, store_sem,
):
    oy, ny = lax.axis_index("oy"), lax.axis_size("oy")
    mid = pl.ds(16, N)
    loads = [
        pltpu.make_async_copy(src, dst, load_sem.at[k])
        for k, (src, dst) in enumerate((
            (z, f0.at[0:4, mid]), (v, f0.at[4:8, mid]), (h, f0.at[8:12, mid]), (ls, sea_i),
            (vi, f0.at[VISC, mid]), (w, f0.at[WIND : WIND + 2, mid]),
            (xw, f0.at[:, 8:16]), (xe, f0.at[:, N + 16 : N + 24]), (nh, ns.at[0]), (sh, ns.at[1]),
        ))
    ]
    for copy in loads:
        copy.start()

    ones = jnp.ones((8, N), F32)
    for rows in (pl.ds(0, 8), pl.ds(PAD - 8, 8)):
        for k in range(FIELDS):
            f0[k, rows, :] = ones
            f1[k, rows, :] = ones
        for k in range(LAYERS):
            p0[k, rows, :] = ones
            p1[k, rows, :] = ones
    for c in range(4):
        for t in range(2):
            fs[c, t, EXT + 8 : TALL, :] = jnp.zeros((TALL - EXT - 8, N), F32)
    build_weights(conv1, conv2, conv3, first_w, second_w, last_w, rows24)

    has_north = (oy < ny - 1).astype(F32)
    has_south = (oy > 0).astype(F32)

    for copy in loads:
        copy.wait()

    def lanes(rows):
        return lax.broadcasted_iota(jnp.int32, (rows, N), 1)

    def north(a, b):
        last_lane = lanes(a.shape[0]) == N - 1
        a, b = pltpu.roll(a, N - 1, 1), pltpu.roll(b, N - 1, 1)
        return jnp.where(last_lane, b, a), jnp.where(last_lane, a, b)

    def south(a, b):
        first_lane = lanes(a.shape[0]) == 0
        a, b = pltpu.roll(a, 1, 1), pltpu.roll(b, 1, 1)
        return jnp.where(first_lane, b, a), jnp.where(first_lane, a, b)

    f0[SEA, mid, :] = sea_i[...].astype(F32)

    def spread(k, carry):
        size = SPREAD
        lane = lanes(size)
        low = lax.rem(lane, 16) < 8
        inside = jnp.where(lane < N // 2, has_north, has_south)
        rows = pl.ds(pl.multiple_of(size * k + 8, 8), size)
        src = pl.ds(pl.multiple_of(size * k, 8), size)
        a, b = ns[0, src, :], ns[1, src, :]
        packs = (
            jnp.where(low, a, b),
            jnp.where(low, pltpu.roll(a, N - 8, 1), pltpu.roll(b, 8, 1)),
        )

        def side(field):
            pack, j = packs[field // 8], field % 8
            return pltpu.roll(pack, N - 16 * j, 1) if j else pack

        sea0 = f0[SEA, rows, :]
        sea1 = side(SEA) * inside
        f1[SEA, rows, :] = sea1
        f1[VISC, rows, :] = side(VISC) * inside
        for field in (8, 9, 10, 11, WIND, WIND + 1):
            f1[field, rows, :] = side(field)
        for field in range(8):
            f1[field, rows, :] = side(field) * sea1
            f0[field, rows, :] = f0[field, rows, :] * sea0
        return carry

    lax.fori_loop(0, EXT // SPREAD, spread, 0)

    fields = (f0, f1)
    press = (p0, p1)
    depth = (t0, t1)

    def continuity(k, carry):
        size = CONT
        inside = jnp.where(lanes(size) < N // 2, has_north, has_south)
        start = size * k + 8
        rows = pl.ds(pl.multiple_of(start, 8), size)
        up, down = pl.ds(start + 1, size), pl.ds(start - 1, size)
        seas = [f[SEA, rows, :] for f in fields]
        anomaly = [[], []]
        for l in range(LAYERS):
            thick = [f[8 + l, rows, :] for f in fields]
            fy = [f[4 + l, rows, :] * t for f, t in zip(fields, thick)]
            fn, fso = north(*fy), south(*fy)
            for t, f in enumerate(fields):
                fe = f[l, up, :] * f[8 + l, up, :]
                fw = f[l, down, :] * f[8 + l, down, :]
                diverge = (fe - fw) * 0.5 + (fn[t] - fso[t]) * 0.5
                new = thick[t] - DT * seas[t] * diverge
                depth[t][l, rows, :] = new
                anomaly[t].append(new - REST)
        for t in range(2):
            faces = [anomaly[t][3]]
            for l in (2, 1, 0):
                faces.insert(0, faces[0] + anomaly[t][l])
            total = None
            for l in range(LAYERS):
                term = grav[l] * faces[l]
                total = term if total is None else total + term
                press[t][l, rows, :] = total * inside if t else total
        return carry

    lax.fori_loop(0, EXT // CONT, continuity, 0)

    copy_h = pltpu.make_async_copy(t0.at[:, mid], h_out, store_sem.at[0])
    copy_h.start()

    total_rows = N * ny
    base_row = oy * N

    def momentum(k, carry):
        size = MOM
        lane = lanes(size)
        start = size * k + 8
        rows = pl.ds(pl.multiple_of(start, 8), size)
        up, down = pl.ds(start + 1, size), pl.ds(start - 1, size)
        row_ids = (
            (base_row + lane).astype(F32),
            (base_row + lane + jnp.where(lane < N // 2, N, -N)).astype(F32),
        )
        coriolis = [0.3 + 1.4 * (r + 0.5) / total_rows for r in row_ids]
        seas = [f[SEA, rows, :] for f in fields]
        visc = [f[VISC, rows, :] for f in fields]
        vn, vs = north(*visc), south(*visc)
        coef = []
        for t, f in enumerate(fields):
            coef.append([
                0.5 * (visc[t] + other)
                for other in (f[VISC, up, :], f[VISC, down, :], vn[t], vs[t])
            ])
        kinetic = [None, None]
        column = [None, None]
        for l in range(LAYERS):
            zc = [f[l, rows, :] for f in fields]
            vc = [f[4 + l, rows, :] for f in fields]
            pc = [p[l, rows, :] for p in press]
            zn, zs = north(*zc), south(*zc)
            wn, ws = north(*vc), south(*vc)
            pn, ps = north(*pc), south(*pc)
            for t, f in enumerate(fields):
                gx = (press[t][l, up, :] - press[t][l, down, :]) * 0.5
                gy = (pn[t] - ps[t]) * 0.5

                def lap(field, centre, n, s):
                    sides = (f[field, up, :], f[field, down, :], n, s)
                    total = coef[t][0] * (sides[0] - centre)
                    for c, q in zip(coef[t][1:], sides[1:]):
                        total = total + c * (q - centre)
                    return total

                thick = depth[t][l, rows, :]
                fz = coriolis[t] * vc[t] - gx + lap(l, zc[t], zn[t], zs[t])
                fv = -coriolis[t] * zc[t] - gy + lap(4 + l, vc[t], wn[t], ws[t])
                if l == 0:
                    fz = fz + f[WIND, rows, :] / thick
                    fv = fv + f[WIND + 1, rows, :] / thick
                if l == LAYERS - 1:
                    fz = fz - DRAG * zc[t]
                    fv = fv - DRAG * vc[t]
                z_new = seas[t] * (zc[t] + DT * fz)
                v_new = seas[t] * (vc[t] + DT * fv)
                if t == 0:
                    zo[l, rows, :] = z_new
                    vo[l, rows, :] = v_new
                part = thick * (z_new * z_new + v_new * v_new)
                kinetic[t] = part if l == 0 else kinetic[t] + part
                column[t] = thick if l == 0 else column[t] + thick
                if l == 0:
                    fs[0, t, rows, :] = z_new
                    fs[1, t, rows, :] = v_new
                    fs[2, t, rows, :] = seas[t] * (thick - REST)
        for t in range(2):
            fs[3, t, rows, :] = seas[t] * (0.5 * kinetic[t] / column[t])
        return carry

    lax.fori_loop(0, EXT // MOM, momentum, 0)

    copy_z = pltpu.make_async_copy(zo.at[:, mid], z_out, store_sem.at[1])
    copy_v = pltpu.make_async_copy(vo.at[:, mid], v_out, store_sem.at[2])
    copy_z.start()
    copy_v.start()

    def turn(k, carry):
        rows = pl.ds(pl.multiple_of(16 * k + 8, 8), 32)
        blocks = [fs[:, t, rows, :].reshape(N, N).T for t in range(2)]
        ft[k, 8 : N + 8, :] = blocks[0]
        ft[k, N + 8 : N + 16, :] = blocks[1][0:8]
        ft[k, N + 16 : N + 24, :] = blocks[1][N - 8 : N]
        ft[k, 0:8, :] = blocks[1][N - 8 : N]
        ft[k, N + 24 : N + 32, :] = blocks[0][0:8]
        return carry

    lax.fori_loop(0, 9, turn, 0)

    order = lax.broadcasted_iota(jnp.int32, (EXT, 2 * N), 0)
    lat = 9 * lax.rem(order, 16) + order // 16
    keep = jnp.where(lat < N, 1.0, jnp.where(lat < N + 8, has_north, has_south)) > 0.5
    b1 = jnp.concatenate([bias1[...].reshape(1, HID) * 0.5] * 4, axis=1)
    b2 = jnp.concatenate([bias2[...].reshape(1, HID) * 0.5] * 4, axis=1)

    def activate(x, bias):
        x = x + bias
        return jnp.where(keep, x + x * jnp.tanh(x), 0.0)

    def first_layer(k, quarters):
        parts = []
        for b in range(3):
            pieces = []
            for t in range(TILES):
                for half in range(2):
                    pieces.append(ft[k, pl.ds(7 + t + b + 72 * half, 8, stride=9), :])
            parts.append(jnp.concatenate(pieces, axis=0).astype(BF16))
        left = jnp.concatenate(parts, axis=1)
        for q in range(quarters):
            out = jnp.dot(left, first_w[:, 256 * q : 256 * q + 256], preferred_element_type=F32)
            out = activate(out, b1)
            for p in range(2):
                one = out[:, N * p : N * p + N]
                h1[4 * k + q, p, 16 : 16 + EXT, :] = one.astype(BF16)
                h1[4 * k + q, p, 0:16, :] = pltpu.roll(one[EXT - 16 : EXT], 1, 0).astype(BF16)
                h1[4 * k + q, p, 16 + EXT : 32 + EXT, :] = pltpu.roll(one[0:16], 15, 0).astype(BF16)

    def first_body(k, carry):
        first_layer(k, 4)
        return carry

    lax.fori_loop(0, 8, first_body, 0)
    first_layer(8, 2)

    def second_matmul(k, ref):
        g = k * STEP
        parts = []
        for b in range(3):
            for d in range(3):
                block = h1[pl.ds(g + d // 2, STEP), d % 2, 16 * b : 16 * b + EXT, :]
                parts.append(block.reshape(BLOCK, N))
        left = jnp.concatenate(parts, axis=1)
        ref[...] = jnp.dot(left, second_w[...], preferred_element_type=F32)

    def finish(k, ref):
        for i in range(STEP):
            one = activate(ref[i * EXT : (i + 1) * EXT], b2).astype(BF16)
            sums = lax.dot_general(
                last_w[...], one, (((1,), (1,)), ((), ())), preferred_element_type=F32
            )
            rs[k * STEP + i] = sums[0:24, 0:N]
            re[k * STEP + i, :, 0:16] = sums[0:24, N:EXT]

    second_matmul(0, d0)

    def second_layer(k, carry):
        second_matmul(2 * k + 1, d1)
        finish(2 * k, d0)
        second_matmul(2 * k + 2, d0)
        finish(2 * k + 1, d1)
        return carry

    lax.fori_loop(0, 5, second_layer, 0)
    finish(10, d0)

    upper = lax.broadcasted_iota(jnp.int32, (8, N), 0) < 4
    for b in range(3):
        blocks = []
        for ref in (rs, re):
            rows = []
            for k in range(N // 8):
                x, y, zz = (ref[2 * k + i, 8 * b : 8 * b + 8, :] for i in range(3))
                y = pltpu.roll(y, 4, 0)
                rows.append(jnp.where(upper, x, y) + jnp.where(upper, y, zz))
            blocks.append(jnp.concatenate(rows, axis=0).T)
        for t in range(TILES):
            for half in range(2):
                block, at = (blocks[0], 16 * t) if t < 8 else (blocks[1], 0)
                at = at + 8 * half
                nat[b, pl.ds(8 + t + 72 * half, 8, stride=9), :] = block[at : at + 8]
        nat[b, 0:8, :] = nat[b, EXT : EXT + 8, :]
    total = nat[0, 7 : 7 + N, :] + nat[1, 8 : 8 + N, :] + nat[2, 9 : 9 + N, :]
    visc_out[...] = jnp.exp(total.T)
    copy_h.wait()
    copy_z.wait()
    copy_v.wait()


SPREAD, CONT, MOM = 48, 24, 16


def step(fields, strips, grav, conv1, bias1, conv2, bias2, conv3):
    any_spec = pl.BlockSpec(memory_space=pl.ANY)
    vmem = pl.BlockSpec(memory_space=pltpu.VMEM)
    whole = jax.ShapeDtypeStruct((LAYERS, N, N), F32)
    return pl.pallas_call(
        step_kernel,
        out_shape=(whole, whole, whole, jax.ShapeDtypeStruct((N, N), F32)),
        in_specs=[any_spec] * 10 + [pl.BlockSpec(memory_space=pltpu.SMEM)] + [vmem] * 5,
        out_specs=[any_spec] * 3 + [vmem],
        scratch_shapes=[
            pltpu.VMEM((FIELDS, PAD, N), F32),
            pltpu.VMEM((FIELDS, PAD, N), F32),
            pltpu.VMEM((N, N), jnp.int32),
            pltpu.VMEM((2, EXT, N), F32),
            pltpu.VMEM((LAYERS, PAD, N), F32),
            pltpu.VMEM((LAYERS, PAD, N), F32),
            pltpu.VMEM((LAYERS, PAD, N), F32),
            pltpu.VMEM((LAYERS, PAD, N), F32),
            pltpu.VMEM((LAYERS, PAD, N), F32),
            pltpu.VMEM((LAYERS, PAD, N), F32),
            pltpu.VMEM((4, 2, TALL, N), F32),
            pltpu.VMEM((9, EXT + 16, N), F32),
            pltpu.VMEM((PAIRS // 2, 2, EXT + 32, N), BF16),
            pltpu.VMEM((BLOCK, 2 * N), F32),
            pltpu.VMEM((BLOCK, 2 * N), F32),
            pltpu.VMEM((GROUPS, 24, N), F32),
            pltpu.VMEM((GROUPS, 24, N), F32),
            pltpu.VMEM((3, EXT + 16, N), F32),
            pltpu.VMEM((3 * N, 16 * HID), BF16),
            pltpu.VMEM((18 * HID, 4 * HID), BF16),
            pltpu.VMEM((32, 2 * N), BF16),
            pltpu.VMEM((32, 2 * N), F32),
            pltpu.SemaphoreType.DMA((10,)),
            pltpu.SemaphoreType.DMA((3,)),
        ],
        compiler_params=pltpu.CompilerParams(vmem_limit_bytes=56 * 2**20),
        name="step",
    )(*fields, *strips, grav, conv1, bias1, conv2, bias2, conv3)


def local(z, v, h, ls, vi, w, grav, conv1, bias1, conv2, bias2, conv3):
    fields = (z, v, h, ls, vi, w)
    strips = exchange(*fields)
    return step(fields, strips, grav, conv1, bias1, conv2, bias2, conv3)


def solution(mesh):
    block, flat = P(None, "ox", "oy"), P("ox", "oy")
    return jax.shard_map(
        local,
        mesh=mesh,
        in_specs=(block, block, block, flat, flat, block) + (P(),) * 6,
        out_specs=(block, block, block, flat),
        check_vma=False,
    )
```

```python
import jax
import jax.numpy as jnp
from jax import lax
from jax.experimental import pallas as pl
from jax.experimental.pallas import tpu as pltpu
from jax.sharding import PartitionSpec as P

MESH = pl.DeviceIdType.MESH
F32 = jnp.float32
BF16 = jnp.bfloat16

DT = 0.05
REST = 1.4
DRAG = 0.5
LAYERS = 4
N = 128
HID = 64
FIELDS = 16
SEA, VISC, WIND = 12, 13, 14
EXT = N + 16
PAD = N + 32
TALL = N + 40
PAIRS = 72
GROUPS = 33
STEP = 3
TILES = EXT // 16
BLOCK = STEP * EXT


def build_weights(conv1, conv2, conv3, first_w, second_w, last_w, rows24):
    lane = lax.broadcasted_iota(jnp.int32, (8, N), 1)
    right = lane >= HID
    row = lax.broadcasted_iota(jnp.int32, (8, N), 0)

    nt = (((1,), (1,)), ((), ()))
    taps = {}
    for a in range(3):
        for b in range(3):
            one = conv1[a, b].astype(F32) * 0.5
            taps[a, b] = jnp.concatenate([one, one], axis=1)
    for b in range(3):
        for c in range(4):
            vecs = [jnp.broadcast_to(taps[a, b][c : c + 1], (8, N)) for a in range(3)]
            for jp in range(8):
                parts = []
                for i in range(4):
                    gap = row + 8 * i - 2 * jp - jnp.where(right, 1, 0) - 4
                    val = jnp.zeros((8, N), F32)
                    for a in range(3):
                        val = jnp.where(gap == a, vecs[a], val)
                    parts.append(val)
                start = 128 * b + 32 * c
                first_w[start : start + 32, N * jp : N * jp + N] = jnp.concatenate(parts, 0).astype(BF16)

    eye = lax.broadcasted_iota(jnp.int32, (HID, HID), 0) == lax.broadcasted_iota(jnp.int32, (HID, HID), 1)
    eye = jnp.where(eye, 0.5, 0.0).astype(BF16)
    side = lax.broadcasted_iota(jnp.int32, (HID, N), 1) >= HID
    for b in range(3):
        turned = []
        for a in range(3):
            one = conv2[a, b]
            both = jnp.concatenate([one, one], axis=0)
            turned.append(lax.dot_general(eye, both, nt, preferred_element_type=F32))
        zero = jnp.zeros((HID, N), F32)
        for m in range(6):
            for jp in range(2):
                tap = m - 2 * jp
                left = turned[tap] if 0 <= tap < 3 else zero
                other = turned[tap - 1] if 0 <= tap - 1 < 3 else zero
                start = (6 * b + m) * HID
                second_w[start : start + HID, N * jp : N * jp + N] = jnp.where(side, other, left).astype(BF16)

    rows24[...] = jnp.zeros((32, 2 * N), F32)
    for b in range(3):
        for place, i in ((0, 3), (1, 4), (2, 5), (5, 0), (6, 1), (7, 2)):
            for m in range(4):
                a = m - i + 2
                if 0 <= a < 3:
                    rows24[8 * b + place : 8 * b + place + 1, HID * m : HID * m + HID] = conv3[a, 0, b : b + 1].astype(F32)
    last_w[...] = rows24[...].astype(BF16)


def step_kernel(
    z, v, h, ls, vi, w, grav, conv1, bias1, conv2, bias2, conv3,
    z_out, v_out, h_out, visc_out,
    f0, f1, sea_i, ns, p0, p1, t0, t1, zo, vo, fs, ft, h1, d0, d1, rs, re, nat,
    first_w, second_w, last_w, rows24, sb, nb, xw, xe, load_sem, store_sem, send_sem, recv_sem,
):
    ox, oy = lax.axis_index("ox"), lax.axis_index("oy")
    nx, ny = lax.axis_size("ox"), lax.axis_size("oy")
    east, west = lax.rem(ox + 1, nx), lax.rem(ox + nx - 1, nx)
    above, below = lax.rem(oy + 1, ny), lax.rem(oy + ny - 1, ny)
    peers = (
        (east, oy), (west, oy), (ox, above), (ox, below),
        (east, above), (east, below), (west, above), (west, below),
    )
    barrier = pltpu.get_barrier_semaphore()
    for peer in peers:
        pl.semaphore_signal(barrier, inc=1, device_id=peer, device_id_type=MESH)
    mid = pl.ds(16, N)
    loads = [
        pltpu.make_async_copy(src, dst, load_sem.at[k])
        for k, (src, dst) in enumerate((
            (z, f0.at[0:4, mid]), (v, f0.at[4:8, mid]), (h, f0.at[8:12, mid]), (ls, sea_i),
            (vi, f0.at[VISC, mid]), (w, f0.at[WIND : WIND + 2, mid]),
        ))
    ]
    for copy in loads:
        copy.start()

    ones = jnp.ones((8, N), F32)
    for rows in (pl.ds(0, 8), pl.ds(PAD - 8, 8)):
        for k in range(FIELDS):
            f0[k, rows, :] = ones
            f1[k, rows, :] = ones
        for k in range(LAYERS):
            p0[k, rows, :] = ones
            p1[k, rows, :] = ones
    for c in range(4):
        for t in range(2):
            fs[c, t, EXT + 8 : TALL, :] = jnp.zeros((TALL - EXT - 8, N), F32)

    has_north = (oy < ny - 1).astype(F32)
    has_south = (oy > 0).astype(F32)

    for copy in loads:
        copy.wait()

    def lanes(rows):
        return lax.broadcasted_iota(jnp.int32, (rows, N), 1)

    f0[SEA, mid, :] = sea_i[...].astype(F32)
    for k in range(8):
        f0[k, mid, :] = f0[k, mid, :] * f0[SEA, mid, :]

    def pack(k, carry):
        rows = pl.ds(pl.multiple_of(PACK * k, 8), PACK)
        src = pl.ds(pl.multiple_of(PACK * k + 16, 8), PACK)
        lane = lanes(PACK)
        low = lax.rem(lane, 16) < 8
        halves = []
        for m in range(2):
            packed = f0[8 * m, src, :]
            for j in range(1, 8):
                moved = pltpu.roll(f0[8 * m + j, src, :], 16 * j, 1)
                packed = jnp.where((lane >= 16 * j - 8) & (lane < 16 * j + 8), moved, packed)
            halves.append(packed)
        sb[rows, :] = jnp.where(low, halves[0], pltpu.roll(halves[1], 8, 1))
        nb[rows, :] = jnp.where(low, pltpu.roll(halves[1], N - 8, 1), halves[0])
        return carry

    lax.fori_loop(0, N // PACK, pack, 0)
    pl.semaphore_wait(barrier, 8)

    first, last = pl.ds(0, 8), pl.ds(N - 8, 8)
    moves = (
        (nb, ns.at[1, 8 : 8 + N], (ox, above)),
        (sb, ns.at[0, 8 : 8 + N], (ox, below)),
        (f0.at[:, N + 8 : N + 16], xw, (east, oy)),
        (f0.at[:, 16:24], xe, (west, oy)),
        (nb.at[last], ns.at[1, 0:8], (east, above)),
        (sb.at[last], ns.at[0, 0:8], (east, below)),
        (nb.at[first], ns.at[1, N + 8 : EXT], (west, above)),
        (sb.at[first], ns.at[0, N + 8 : EXT], (west, below)),
    )
    sends = [
        pltpu.make_async_remote_copy(
            src_ref=src, dst_ref=dst, send_sem=send_sem.at[k], recv_sem=recv_sem.at[k],
            device_id=peer, device_id_type=MESH,
        )
        for k, (src, dst, peer) in enumerate(moves)
    ]
    for copy in reversed(sends):
        copy.start()
    build_weights(conv1, conv2, conv3, first_w, second_w, last_w, rows24)
    for copy in sends:
        copy.wait()
    for k in range(FIELDS):
        f0[k, 8:16, :] = xw[k]
        f0[k, N + 16 : N + 24, :] = xe[k]

    def north(a, b):
        last_lane = lanes(a.shape[0]) == N - 1
        a, b = pltpu.roll(a, N - 1, 1), pltpu.roll(b, N - 1, 1)
        return jnp.where(last_lane, b, a), jnp.where(last_lane, a, b)

    def south(a, b):
        first_lane = lanes(a.shape[0]) == 0
        a, b = pltpu.roll(a, 1, 1), pltpu.roll(b, 1, 1)
        return jnp.where(first_lane, b, a), jnp.where(first_lane, a, b)

    def spread(k, carry):
        size = SPREAD
        lane = lanes(size)
        low = lax.rem(lane, 16) < 8
        inside = jnp.where(lane < N // 2, has_north, has_south)
        rows = pl.ds(pl.multiple_of(size * k + 8, 8), size)
        src = pl.ds(pl.multiple_of(size * k, 8), size)
        a, b = ns[0, src, :], ns[1, src, :]
        packs = (
            jnp.where(low, a, b),
            jnp.where(low, pltpu.roll(a, N - 8, 1), pltpu.roll(b, 8, 1)),
        )

        def side(field):
            pack, j = packs[field // 8], field % 8
            return pltpu.roll(pack, N - 16 * j, 1) if j else pack

        sea1 = side(SEA) * inside
        f1[SEA, rows, :] = sea1
        f1[VISC, rows, :] = side(VISC) * inside
        for field in (8, 9, 10, 11, WIND, WIND + 1):
            f1[field, rows, :] = side(field)
        for field in range(8):
            f1[field, rows, :] = side(field) * inside
        return carry

    lax.fori_loop(0, EXT // SPREAD, spread, 0)

    fields = (f0, f1)
    press = (p0, p1)
    depth = (t0, t1)

    def continuity(k, carry):
        size = CONT
        inside = jnp.where(lanes(size) < N // 2, has_north, has_south)
        start = size * k + 8
        rows = pl.ds(pl.multiple_of(start, 8), size)
        up, down = pl.ds(start + 1, size), pl.ds(start - 1, size)
        seas = [f[SEA, rows, :] for f in fields]
        anomaly = [[], []]
        for l in range(LAYERS):
            thick = [f[8 + l, rows, :] for f in fields]
            fy = [f[4 + l, rows, :] * t for f, t in zip(fields, thick)]
            fn, fso = north(*fy), south(*fy)
            for t, f in enumerate(fields):
                fe = f[l, up, :] * f[8 + l, up, :]
                fw = f[l, down, :] * f[8 + l, down, :]
                diverge = (fe - fw) * 0.5 + (fn[t] - fso[t]) * 0.5
                new = thick[t] - DT * seas[t] * diverge
                depth[t][l, rows, :] = new
                anomaly[t].append(new - REST)
        for t in range(2):
            faces = [anomaly[t][3]]
            for l in (2, 1, 0):
                faces.insert(0, faces[0] + anomaly[t][l])
            total = None
            for l in range(LAYERS):
                term = grav[l] * faces[l]
                total = term if total is None else total + term
                press[t][l, rows, :] = total * inside if t else total
        return carry

    lax.fori_loop(0, EXT // CONT, continuity, 0)

    copy_h = pltpu.make_async_copy(t0.at[:, mid], h_out, store_sem.at[0])
    copy_h.start()

    total_rows = N * ny
    base_row = oy * N

    def momentum(k, carry):
        size = MOM
        lane = lanes(size)
        start = size * k + 8
        rows = pl.ds(pl.multiple_of(start, 8), size)
        up, down = pl.ds(start + 1, size), pl.ds(start - 1, size)
        row_ids = (
            (base_row + lane).astype(F32),
            (base_row + lane + jnp.where(lane < N // 2, N, -N)).astype(F32),
        )
        coriolis = [0.3 + 1.4 * (r + 0.5) / total_rows for r in row_ids]
        seas = [f[SEA, rows, :] for f in fields]
        visc = [f[VISC, rows, :] for f in fields]
        vn, vs = north(*visc), south(*visc)
        coef = []
        for t, f in enumerate(fields):
            coef.append([
                0.5 * (visc[t] + other)
                for other in (f[VISC, up, :], f[VISC, down, :], vn[t], vs[t])
            ])
        kinetic = [None, None]
        column = [None, None]
        for l in range(LAYERS):
            zc = [f[l, rows, :] for f in fields]
            vc = [f[4 + l, rows, :] for f in fields]
            pc = [p[l, rows, :] for p in press]
            zn, zs = north(*zc), south(*zc)
            wn, ws = north(*vc), south(*vc)
            pn, ps = north(*pc), south(*pc)
            for t, f in enumerate(fields):
                gx = (press[t][l, up, :] - press[t][l, down, :]) * 0.5
                gy = (pn[t] - ps[t]) * 0.5

                def lap(field, centre, n, s):
                    sides = (f[field, up, :], f[field, down, :], n, s)
                    total = coef[t][0] * (sides[0] - centre)
                    for c, q in zip(coef[t][1:], sides[1:]):
                        total = total + c * (q - centre)
                    return total

                thick = depth[t][l, rows, :]
                fz = coriolis[t] * vc[t] - gx + lap(l, zc[t], zn[t], zs[t])
                fv = -coriolis[t] * zc[t] - gy + lap(4 + l, vc[t], wn[t], ws[t])
                if l == 0:
                    fz = fz + f[WIND, rows, :] / thick
                    fv = fv + f[WIND + 1, rows, :] / thick
                if l == LAYERS - 1:
                    fz = fz - DRAG * zc[t]
                    fv = fv - DRAG * vc[t]
                z_new = seas[t] * (zc[t] + DT * fz)
                v_new = seas[t] * (vc[t] + DT * fv)
                if t == 0:
                    zo[l, rows, :] = z_new
                    vo[l, rows, :] = v_new
                part = thick * (z_new * z_new + v_new * v_new)
                kinetic[t] = part if l == 0 else kinetic[t] + part
                column[t] = thick if l == 0 else column[t] + thick
                if l == 0:
                    fs[0, t, rows, :] = z_new
                    fs[1, t, rows, :] = v_new
                    fs[2, t, rows, :] = seas[t] * (thick - REST)
        for t in range(2):
            fs[3, t, rows, :] = seas[t] * (0.5 * kinetic[t] / column[t])
        return carry

    lax.fori_loop(0, EXT // MOM, momentum, 0)

    copy_z = pltpu.make_async_copy(zo.at[:, mid], z_out, store_sem.at[1])
    copy_v = pltpu.make_async_copy(vo.at[:, mid], v_out, store_sem.at[2])
    copy_z.start()
    copy_v.start()

    def turn(k, carry):
        rows = pl.ds(pl.multiple_of(16 * k + 8, 8), 32)
        blocks = [fs[:, t, rows, :].reshape(N, N).T for t in range(2)]
        ft[k, 8 : N + 8, :] = blocks[0]
        ft[k, N + 8 : N + 16, :] = blocks[1][0:8]
        ft[k, N + 16 : N + 24, :] = blocks[1][N - 8 : N]
        ft[k, 0:8, :] = blocks[1][N - 8 : N]
        ft[k, N + 24 : N + 32, :] = blocks[0][0:8]
        return carry

    lax.fori_loop(0, 9, turn, 0)

    order = lax.broadcasted_iota(jnp.int32, (EXT, 2 * N), 0)
    lat = 9 * lax.rem(order, 16) + order // 16
    keep = jnp.where(lat < N, 1.0, jnp.where(lat < N + 8, has_north, has_south)) > 0.5
    b1 = jnp.concatenate([bias1[...].reshape(1, HID) * 0.5] * 4, axis=1)
    b2 = jnp.concatenate([bias2[...].reshape(1, HID) * 0.5] * 4, axis=1)

    def activate(x, bias):
        x = x + bias
        return jnp.where(keep, x + x * jnp.tanh(x), 0.0)

    def first_layer(k, quarters):
        parts = []
        for b in range(3):
            pieces = []
            for t in range(TILES):
                for half in range(2):
                    pieces.append(ft[k, pl.ds(7 + t + b + 72 * half, 8, stride=9), :])
            parts.append(jnp.concatenate(pieces, axis=0).astype(BF16))
        left = jnp.concatenate(parts, axis=1)
        for q in range(quarters):
            out = jnp.dot(left, first_w[:, 256 * q : 256 * q + 256], preferred_element_type=F32)
            out = activate(out, b1)
            for p in range(2):
                one = out[:, N * p : N * p + N]
                h1[4 * k + q, p, 16 : 16 + EXT, :] = one.astype(BF16)
                h1[4 * k + q, p, 0:16, :] = pltpu.roll(one[EXT - 16 : EXT], 1, 0).astype(BF16)
                h1[4 * k + q, p, 16 + EXT : 32 + EXT, :] = pltpu.roll(one[0:16], 15, 0).astype(BF16)

    def first_body(k, carry):
        first_layer(k, 4)
        return carry

    lax.fori_loop(0, 8, first_body, 0)
    first_layer(8, 2)

    def second_matmul(k, ref):
        g = k * STEP
        parts = []
        for b in range(3):
            for d in range(3):
                block = h1[pl.ds(g + d // 2, STEP), d % 2, 16 * b : 16 * b + EXT, :]
                parts.append(block.reshape(BLOCK, N))
        left = jnp.concatenate(parts, axis=1)
        ref[...] = jnp.dot(left, second_w[...], preferred_element_type=F32)

    def finish(k, ref):
        for i in range(STEP):
            one = activate(ref[i * EXT : (i + 1) * EXT], b2).astype(BF16)
            sums = lax.dot_general(
                last_w[...], one, (((1,), (1,)), ((), ())), preferred_element_type=F32
            )
            rs[k * STEP + i] = sums[0:24, 0:N]
            re[k * STEP + i, :, 0:16] = sums[0:24, N:EXT]

    second_matmul(0, d0)

    def second_layer(k, carry):
        second_matmul(2 * k + 1, d1)
        finish(2 * k, d0)
        second_matmul(2 * k + 2, d0)
        finish(2 * k + 1, d1)
        return carry

    lax.fori_loop(0, 5, second_layer, 0)
    finish(10, d0)

    upper = lax.broadcasted_iota(jnp.int32, (8, N), 0) < 4
    for b in range(3):
        blocks = []
        for ref in (rs, re):
            rows = []
            for k in range(N // 8):
                x, y, zz = (ref[2 * k + i, 8 * b : 8 * b + 8, :] for i in range(3))
                y = pltpu.roll(y, 4, 0)
                rows.append(jnp.where(upper, x, y) + jnp.where(upper, y, zz))
            blocks.append(jnp.concatenate(rows, axis=0).T)
        for t in range(TILES):
            for half in range(2):
                block, at = (blocks[0], 16 * t) if t < 8 else (blocks[1], 0)
                at = at + 8 * half
                nat[b, pl.ds(8 + t + 72 * half, 8, stride=9), :] = block[at : at + 8]
        nat[b, 0:8, :] = nat[b, EXT : EXT + 8, :]
    total = nat[0, 7 : 7 + N, :] + nat[1, 8 : 8 + N, :] + nat[2, 9 : 9 + N, :]
    visc_out[...] = jnp.exp(total.T)
    copy_h.wait()
    copy_z.wait()
    copy_v.wait()


PACK, SPREAD, CONT, MOM = 32, 48, 24, 16


def step(fields, grav, conv1, bias1, conv2, bias2, conv3):
    any_spec = pl.BlockSpec(memory_space=pl.ANY)
    vmem = pl.BlockSpec(memory_space=pltpu.VMEM)
    whole = jax.ShapeDtypeStruct((LAYERS, N, N), F32)
    return pl.pallas_call(
        step_kernel,
        out_shape=(whole, whole, whole, jax.ShapeDtypeStruct((N, N), F32)),
        in_specs=[any_spec] * 6 + [pl.BlockSpec(memory_space=pltpu.SMEM)] + [vmem] * 5,
        out_specs=[any_spec] * 3 + [vmem],
        scratch_shapes=[
            pltpu.VMEM((FIELDS, PAD, N), F32),
            pltpu.VMEM((FIELDS, PAD, N), F32),
            pltpu.VMEM((N, N), jnp.int32),
            pltpu.VMEM((2, EXT, N), F32),
            pltpu.VMEM((LAYERS, PAD, N), F32),
            pltpu.VMEM((LAYERS, PAD, N), F32),
            pltpu.VMEM((LAYERS, PAD, N), F32),
            pltpu.VMEM((LAYERS, PAD, N), F32),
            pltpu.VMEM((LAYERS, PAD, N), F32),
            pltpu.VMEM((LAYERS, PAD, N), F32),
            pltpu.VMEM((4, 2, TALL, N), F32),
            pltpu.VMEM((9, EXT + 16, N), F32),
            pltpu.VMEM((PAIRS // 2, 2, EXT + 32, N), BF16),
            pltpu.VMEM((BLOCK, 2 * N), F32),
            pltpu.VMEM((BLOCK, 2 * N), F32),
            pltpu.VMEM((GROUPS, 24, N), F32),
            pltpu.VMEM((GROUPS, 24, N), F32),
            pltpu.VMEM((3, EXT + 16, N), F32),
            pltpu.VMEM((3 * N, 16 * HID), BF16),
            pltpu.VMEM((18 * HID, 4 * HID), BF16),
            pltpu.VMEM((32, 2 * N), BF16),
            pltpu.VMEM((32, 2 * N), F32),
            pltpu.VMEM((N, N), F32),
            pltpu.VMEM((N, N), F32),
            pltpu.VMEM((FIELDS, 8, N), F32),
            pltpu.VMEM((FIELDS, 8, N), F32),
            pltpu.SemaphoreType.DMA((6,)),
            pltpu.SemaphoreType.DMA((3,)),
            pltpu.SemaphoreType.DMA((8,)),
            pltpu.SemaphoreType.DMA((8,)),
        ],
        compiler_params=pltpu.CompilerParams(
            collective_id=0, has_side_effects=True, vmem_limit_bytes=56 * 2**20
        ),
        name="step",
    )(*fields, grav, conv1, bias1, conv2, bias2, conv3)


def local(z, v, h, ls, vi, w, grav, conv1, bias1, conv2, bias2, conv3):
    fields = (z, v, h, ls, vi, w)
    conv1 = jnp.transpose(conv1, (0, 1, 3, 2))
    conv3 = jnp.transpose(conv3, (0, 2, 1, 3))
    return step(fields, grav, conv1, bias1, conv2, bias2, conv3)


def solution(mesh):
    block, flat = P(None, "ox", "oy"), P("ox", "oy")
    return jax.shard_map(
        local,
        mesh=mesh,
        in_specs=(block, block, block, flat, flat, block) + (P(),) * 6,
        out_specs=(block, block, block, flat),
        check_vma=False,
    )
```

```python
import jax
import jax.numpy as jnp
from jax import lax
from jax.experimental import pallas as pl
from jax.experimental.pallas import tpu as pltpu
from jax.sharding import PartitionSpec as P

MESH = pl.DeviceIdType.MESH
F32 = jnp.float32
BF16 = jnp.bfloat16

DT = 0.05
REST = 1.4
DRAG = 0.5
LAYERS = 4
N = 128
HID = 64
FIELDS = 16
SEA, VISC, WIND = 12, 13, 14
EXT = N + 16
PAD = N + 32
TALL = N + 40
PAIRS = 72
GROUPS = 33
STEP = 3
TILES = EXT // 16
BLOCK = STEP * EXT


HBM = pltpu.HBM
EDGE = 32


def lanes(rows):
    return lax.broadcasted_iota(jnp.int32, (rows, N), 1)


def near(x):
    return pltpu.roll(x, N - 1, 1), pltpu.roll(x, 1, 1)


def shifted(start, size):
    aligned = start if isinstance(start, int) else pl.multiple_of(start, 8)
    return pl.ds(aligned, size), pl.ds(start + 1, size), pl.ds(start - 1, size)


def continuity(f, press, depth, grav, start, size):
    rows, up, down = shifted(start, size)
    sea = f[SEA, rows, :]
    anomaly = []
    for l in range(LAYERS):
        thick = f[8 + l, rows, :]
        fn, fs = near(f[4 + l, rows, :] * thick)
        fe = f[l, up, :] * f[8 + l, up, :]
        fw = f[l, down, :] * f[8 + l, down, :]
        diverge = (fe - fw) * 0.5 + (fn - fs) * 0.5
        new = thick - DT * sea * diverge
        depth[l, rows, :] = new
        anomaly.append(new - REST)
    faces = [anomaly[3]]
    for l in (2, 1, 0):
        faces.insert(0, faces[0] + anomaly[l])
    total = grav[0] * faces[0]
    press[0, rows, :] = total
    for l in range(1, LAYERS):
        total = total + grav[l] * faces[l]
        press[l, rows, :] = total


def coefficients(visc, up, down):
    return [0.5 * (visc + other) for other in (up, down, *near(visc))]


def viscous(coef, centre, up, down):
    total = None
    for c, q in zip(coef, (up, down, *near(centre))):
        term = c * (q - centre)
        total = term if total is None else total + term
    return total


def coriolis_of(lat, ny):
    return 0.3 + 1.4 * (lat.astype(F32) + 0.5) / (N * ny)


def momentum(f, press, depth, zo, vo, feature_refs, coriolis, start, size):
    rows, up, down = shifted(start, size)
    sea = f[SEA, rows, :]
    coef = coefficients(f[VISC, rows, :], f[VISC, up, :], f[VISC, down, :])
    kinetic = column = None
    for l in range(LAYERS):
        zc, vc = f[l, rows, :], f[4 + l, rows, :]
        pn, ps = near(press[l, rows, :])
        gx = (press[l, up, :] - press[l, down, :]) * 0.5
        gy = (pn - ps) * 0.5
        thick = depth[l, rows, :]
        fz = coriolis * vc - gx + viscous(coef, zc, f[l, up, :], f[l, down, :])
        fv = -coriolis * zc - gy + viscous(coef, vc, f[4 + l, up, :], f[4 + l, down, :])
        if l == 0:
            fz = fz + f[WIND, rows, :] / thick
            fv = fv + f[WIND + 1, rows, :] / thick
        if l == LAYERS - 1:
            fz = fz - DRAG * zc
            fv = fv - DRAG * vc
        z_new = sea * (zc + DT * fz)
        v_new = sea * (vc + DT * fv)
        zo[l, rows, :] = z_new
        vo[l, rows, :] = v_new
        part = thick * (z_new * z_new + v_new * v_new)
        kinetic = part if l == 0 else kinetic + part
        column = thick if l == 0 else column + thick
        if l == 0:
            feature_refs[0][0, rows, :] = z_new
            feature_refs[0][1, rows, :] = v_new
            feature_refs[0][2, rows, :] = sea * (thick - REST)
    feature_refs[0][3, rows, :] = sea * (0.5 * kinetic / column)


def own_pack(read, lane):
    packed = None
    for l in range(4):
        field = read(l)
        for at, shift in ((32 * l + 8, 32 * l + 8), (32 * l + 16, 32 * l + 16 + 8)):
            moved = pltpu.roll(field, shift % N, 1)
            packed = moved if packed is None else jnp.where((lane >= at) & (lane < at + 8), moved, packed)
    return packed


def exchange_kernel(
    z, v, h, ls, vi, w, grav_in, conv1, conv2, conv3, bias1, bias2,
    f0, p0, t0, zo, vo, fs, ft, own, ns, xw, xe, first_w, second_w, last_w, consts,
    sea_i, sb, nb, rows24, c1, c2, c3, grav, s1, s2, load_sem, send_sem, recv_sem,
):
    ox, oy = lax.axis_index("ox"), lax.axis_index("oy")
    nx, ny = lax.axis_size("ox"), lax.axis_size("oy")
    east, west = lax.rem(ox + 1, nx), lax.rem(ox + nx - 1, nx)
    above, below = lax.rem(oy + 1, ny), lax.rem(oy + ny - 1, ny)
    peers = (
        (east, oy), (west, oy), (ox, above), (ox, below),
        (east, above), (east, below), (west, above), (west, below),
    )
    barrier = pltpu.get_barrier_semaphore()
    for peer in peers:
        pl.semaphore_signal(barrier, inc=1, device_id=peer, device_id_type=MESH)
    mid = pl.ds(16, N)
    loads = [
        pltpu.make_async_copy(src, dst, load_sem.at[k])
        for k, (src, dst) in enumerate((
            (ls, sea_i), (z, f0.at[0:4, mid]), (v, f0.at[4:8, mid]), (h, f0.at[8:12, mid]),
            (vi, f0.at[VISC, mid]), (w, f0.at[WIND : WIND + 2, mid]),
            (conv1, c1), (conv2, c2), (conv3, c3), (grav_in, grav), (bias1, s1), (bias2, s2),
        ))
    ]
    for copy in loads:
        copy.start()
    ones = jnp.ones((8, N), F32)
    for rows in (pl.ds(8, 8), pl.ds(N + 16, 8)):
        for k in range(FIELDS):
            f0[k, rows, :] = ones
        for k in range(LAYERS):
            p0[k, rows, :] = ones
    for copy in loads[:6]:
        copy.wait()

    def pack(k, carry):
        src = pl.ds(pl.multiple_of(PACK * k + 16, 8), PACK)
        rows = pl.ds(pl.multiple_of(PACK * k, 8), PACK)
        lane = lanes(PACK)
        sea = sea_i[rows, :].astype(F32)
        f0[SEA, src, :] = sea
        to_south = to_north = None
        for a in range(4):
            for l in range(4):
                field = sea if 4 * a + l == SEA else f0[4 * a + l, src, :]
                if a < 2:
                    field = field * sea
                    f0[4 * a + l, src, :] = field
                at = 32 * l + 8 * a
                moved = pltpu.roll(field, at, 1) if at else field
                if to_south is None:
                    to_south = to_north = moved
                else:
                    to_south = jnp.where((lane >= at) & (lane < at + 8), moved, to_south)
                    to_north = jnp.where((lane >= at - 8) & (lane < at), moved, to_north)
        sb[rows, :] = to_south
        nb[rows, :] = to_north
        return carry

    lax.fori_loop(0, N // PACK, pack, 0)
    pl.semaphore_wait(barrier, 8)

    first, last = pl.ds(0, 8), pl.ds(N - 8, 8)
    moves = (
        (nb, ns.at[1, 8 : 8 + N], (ox, above)),
        (sb, ns.at[0, 8 : 8 + N], (ox, below)),
        (f0.at[:, N + 8 : N + 16], xw, (east, oy)),
        (f0.at[:, 16:24], xe, (west, oy)),
        (nb.at[last], ns.at[1, 0:8], (east, above)),
        (sb.at[last], ns.at[0, 0:8], (east, below)),
        (nb.at[first], ns.at[1, N + 8 : EXT], (west, above)),
        (sb.at[first], ns.at[0, N + 8 : EXT], (west, below)),
    )
    sends = [
        pltpu.make_async_remote_copy(
            src_ref=src, dst_ref=dst, send_sem=send_sem.at[k], recv_sem=recv_sem.at[k],
            device_id=peer, device_id_type=MESH,
        )
        for k, (src, dst, peer) in enumerate(moves)
    ]
    for copy in reversed(sends):
        copy.start()

    for copy in loads[6:]:
        copy.wait()
    build_weights(c1, c2, c3, first_w, second_w, last_w, rows24)
    for l in range(LAYERS):
        consts[l : l + 1, :] = jnp.full((1, N), grav[l], F32)
    for k, bias in enumerate((s1, s2)):
        half = bias[...].reshape(1, HID) * 0.5
        consts[4 + k : 5 + k, :] = jnp.concatenate([half, half], axis=1)

    def inner_continuity(k, carry):
        continuity(f0, p0, t0, grav, CONT * k + 16, CONT)
        return carry

    lax.fori_loop(0, N // CONT, inner_continuity, 0)

    def inner_momentum(k, carry):
        coriolis = coriolis_of(oy * N + lanes(MOM), ny)
        momentum(f0, p0, t0, zo, vo, (fs,), coriolis, MOM * k + 16, MOM)
        return carry

    lax.fori_loop(0, N // MOM, inner_momentum, 0)

    def inner_pack(k, carry):
        src = pl.ds(pl.multiple_of(OWN * k + 16, 8), OWN)
        rows = pl.ds(pl.multiple_of(OWN * k, 8), OWN)
        for a in range(4):
            own[a, rows, :] = own_pack(lambda l: f0[4 * a + l, src, :], lanes(OWN))
        return carry

    lax.fori_loop(0, N // OWN, inner_pack, 0)

    def inner_turn(k, carry):
        rows = pl.ds(pl.multiple_of(16 * k + 24, 8), 32)
        ft[k] = fs[:, rows, :].reshape(N, N).T
        return carry

    lax.fori_loop(0, 6, inner_turn, 0)
    for copy in sends:
        copy.wait()


def exchange(fields, grav, conv1, conv2, conv3, bias1, bias2):
    hbm = pl.BlockSpec(memory_space=HBM)
    vmem = pl.BlockSpec(memory_space=pltpu.VMEM)

    def array(*shape, dtype=F32):
        return jax.ShapeDtypeStruct(shape, dtype)

    return pl.pallas_call(
        exchange_kernel,
        out_shape=(
            array(FIELDS, PAD, N), array(LAYERS, PAD, N), array(LAYERS, PAD, N),
            array(LAYERS, PAD, N), array(LAYERS, PAD, N), array(4, PAD, N),
            array(6, N, N), array(4, N, N), array(2, EXT, N),
            array(FIELDS, 8, N), array(FIELDS, 8, N),
            array(3 * N, 16 * HID, dtype=BF16), array(18 * HID, 4 * HID, dtype=BF16),
            array(32, 2 * N, dtype=BF16), array(8, N),
        ),
        in_specs=[hbm] * 12,
        out_specs=(vmem,) * 15,
        scratch_shapes=[
            pltpu.VMEM((N, N), jnp.int32),
            pltpu.VMEM((N, N), F32),
            pltpu.VMEM((N, N), F32),
            pltpu.VMEM((32, 2 * N), F32),
            pltpu.VMEM(conv1.shape, BF16),
            pltpu.VMEM(conv2.shape, BF16),
            pltpu.VMEM(conv3.shape, BF16),
            pltpu.SMEM((LAYERS,), F32),
            pltpu.VMEM((HID,), F32),
            pltpu.VMEM((HID,), F32),
            pltpu.SemaphoreType.DMA((12,)),
            pltpu.SemaphoreType.DMA((8,)),
            pltpu.SemaphoreType.DMA((8,)),
        ],
        compiler_params=pltpu.CompilerParams(
            collective_id=0, has_side_effects=True, vmem_limit_bytes=16 * 2**20
        ),
        name="exchange",
    )(*fields, grav, conv1, conv2, conv3, bias1, bias2)


def build_weights(conv1, conv2, conv3, first_w, second_w, last_w, rows24):
    lane = lax.broadcasted_iota(jnp.int32, (8, N), 1)
    right = lane >= HID
    row = lax.broadcasted_iota(jnp.int32, (8, N), 0)

    nt = (((1,), (1,)), ((), ()))
    taps = {}
    for a in range(3):
        for b in range(3):
            one = conv1[a, b].astype(F32) * 0.5
            taps[a, b] = jnp.concatenate([one, one], axis=1)
    for b in range(3):
        for c in range(4):
            vecs = [jnp.broadcast_to(taps[a, b][c : c + 1], (8, N)) for a in range(3)]
            for jp in range(8):
                parts = []
                for i in range(4):
                    gap = row + 8 * i - 2 * jp - jnp.where(right, 1, 0) - 4
                    val = jnp.zeros((8, N), F32)
                    for a in range(3):
                        val = jnp.where(gap == a, vecs[a], val)
                    parts.append(val)
                start = 128 * b + 32 * c
                first_w[start : start + 32, N * jp : N * jp + N] = jnp.concatenate(parts, 0).astype(BF16)

    eye = lax.broadcasted_iota(jnp.int32, (HID, HID), 0) == lax.broadcasted_iota(jnp.int32, (HID, HID), 1)
    eye = jnp.where(eye, 0.5, 0.0).astype(BF16)
    side = lax.broadcasted_iota(jnp.int32, (HID, N), 1) >= HID
    for b in range(3):
        turned = []
        for a in range(3):
            one = conv2[a, b]
            both = jnp.concatenate([one, one], axis=0)
            turned.append(lax.dot_general(eye, both, nt, preferred_element_type=F32))
        zero = jnp.zeros((HID, N), F32)
        for m in range(6):
            for jp in range(2):
                tap = m - 2 * jp
                left = turned[tap] if 0 <= tap < 3 else zero
                other = turned[tap - 1] if 0 <= tap - 1 < 3 else zero
                start = (6 * b + m) * HID
                second_w[start : start + HID, N * jp : N * jp + N] = jnp.where(side, other, left).astype(BF16)

    rows24[...] = jnp.zeros((32, 2 * N), F32)
    for b in range(3):
        for place, i in ((0, 3), (1, 4), (2, 5), (5, 0), (6, 1), (7, 2)):
            for m in range(4):
                a = m - i + 2
                if 0 <= a < 3:
                    rows24[8 * b + place : 8 * b + place + 1, HID * m : HID * m + HID] = conv3[a, 0, b : b + 1].astype(F32)
    last_w[...] = rows24[...].astype(BF16)


def step_kernel(
    f0, p0, t0, zo, vo, fs0, ft0, own, ns, xw, xe, first_w, second_w, last_w, consts,
    z_out, v_out, h_out, visc_out,
    fe, pe, te, ze, ve, fse, q, pq, hq, zq, vq, fsq, fs, ft, zm, vm, hm, h1, d0, d1, rs, re, nat,
    store_sem,
):
    oy, ny = lax.axis_index("oy"), lax.axis_size("oy")
    has_north = (oy < ny - 1).astype(F32)
    has_south = (oy > 0).astype(F32)
    ones = jnp.ones((8, N), F32)
    grav = [consts[l : l + 1, :] for l in range(LAYERS)]

    for e, (rows, src) in enumerate((((8, xw), (16, 16)), ((0, N), (16, xe)))):
        (halo_at, halo), (own_at, own_from) = (rows, src) if e == 0 else (src, rows)
        pad = 0 if e == 0 else 24
        for k in range(FIELDS):
            fe[e, k, halo_at : halo_at + 8, :] = halo[k]
            fe[e, k, own_at : own_at + 16, :] = f0[k, own_from : own_from + 16, :]
            fe[e, k, pad : pad + 8, :] = ones
        inner_at, inner_from = (24, 24) if e == 0 else (0, N)
        for k in range(LAYERS):
            pe[e, k, pad : pad + 8, :] = ones
            pe[e, k, inner_at : inner_at + 8, :] = p0[k, inner_from : inner_from + 8, :]
    for e in range(2):
        continuity(fe.at[e], pe.at[e], te.at[e], grav, 8, 16)
    for e in range(2):
        coriolis = coriolis_of(oy * N + lanes(16), ny)
        momentum(fe.at[e], pe.at[e], te.at[e], ze.at[e], ve.at[e], (fse.at[e],), coriolis, 8, 16)

    for k in range(7):
        q[k, 0:8, :] = ones
        q[k, PAD - 8 : PAD, :] = ones
    pq[0:8, :] = ones
    pq[PAD - 8 : PAD, :] = ones
    for c in range(4):
        fs[c, EXT + 8 : TALL, :] = jnp.zeros((TALL - EXT - 8, N), F32)
        fsq[c, EXT + 8 : TALL, :] = jnp.zeros((TALL - EXT - 8, N), F32)

    def spread(start, size, groups):
        lane = lanes(size)
        part = lax.rem(lane, 32)
        seg = lane // 32
        inside = jnp.where(part < 8, has_south, jnp.where(part < 24, 1.0, has_north))
        rows = pl.ds(start + 8 if isinstance(start, int) else pl.multiple_of(start + 8, 8), size)
        src = pl.ds(start if isinstance(start, int) else pl.multiple_of(start, 8), size)
        from_north, from_south = ns[0, src, :], ns[1, src, :]
        full = []
        for a in range(4):
            high = pltpu.roll(from_north, (24 - 8 * a) % N, 1)
            low = pltpu.roll(from_south, (8 - 8 * a) % N, 1)
            full.append(jnp.where(part < 8, low, jnp.where(part < 24, groups(a), high)))
        q[0, rows, :] = full[0] * inside
        q[1, rows, :] = full[1] * inside
        q[2, rows, :] = full[2]
        for k, s in ((3, 0), (4, 1)):
            one = jnp.where(seg == s, full[3] * inside, 0.0)
            one = one + pltpu.roll(one, 32, 1)
            q[k, rows, :] = one + pltpu.roll(one, 64, 1)
        for k, s in ((5, 2), (6, 3)):
            q[k, rows, :] = jnp.where(seg == 0, pltpu.roll(full[3], N - 32 * s, 1), 0.0)

    for at, strip in ((0, xw), (N + 8, xe)):
        spread(at, 8, lambda a: own_pack(lambda l: strip[4 * a + l], lanes(8)))

    def spread_body(k, carry):
        rows = pl.ds(pl.multiple_of(SPREAD * k, 8), SPREAD)
        spread(SPREAD * k + 8, SPREAD, lambda a: own[a, rows, :])
        return carry

    lax.fori_loop(0, N // SPREAD, spread_body, 0)

    def packed_continuity(k, carry):
        size = QC
        lane = lanes(size)
        part, seg = lax.rem(lane, 32), lane // 32
        inside = jnp.where(part < 8, has_south, jnp.where(part < 24, 1.0, has_north))
        weight = jnp.where(seg == 0, grav[0], jnp.where(seg == 1, grav[1], jnp.where(seg == 2, grav[2], grav[3])))
        rows, up, down = shifted(size * k + 8, size)
        thick = q[2, rows, :]
        fn, fs_ = near(q[1, rows, :] * thick)
        fe_ = q[0, up, :] * q[2, up, :]
        fw_ = q[0, down, :] * q[2, down, :]
        diverge = (fe_ - fw_) * 0.5 + (fn - fs_) * 0.5
        new = thick - DT * q[3, rows, :] * diverge
        hq[rows, :] = new
        a = new - REST
        face = a
        for n in (1, 2, 3):
            face = face + jnp.where(seg < 4 - n, pltpu.roll(a, N - 32 * n, 1), 0.0)
        term = weight * face
        total = term
        for n in (1, 2, 3):
            total = total + jnp.where(seg >= n, pltpu.roll(term, 32 * n, 1), 0.0)
        pq[rows, :] = total * inside
        return carry

    lax.fori_loop(0, EXT // QC, packed_continuity, 0)

    def packed_momentum(k, carry):
        size = QM
        lane = lanes(size)
        part, seg = lax.rem(lane, 32), lane // 32
        coriolis = coriolis_of(oy * N + part + jnp.where(part < 16, -8, 104), ny)
        drag = jnp.where(seg == 3, DRAG, 0.0)
        rows, up, down = shifted(size * k + 8, size)
        zc, vc, sea = q[0, rows, :], q[1, rows, :], q[3, rows, :]
        coef = coefficients(q[4, rows, :], q[4, up, :], q[4, down, :])
        pn, ps = near(pq[rows, :])
        gx = (pq[up, :] - pq[down, :]) * 0.5
        gy = (pn - ps) * 0.5
        thick = hq[rows, :]
        fz = coriolis * vc - gx + viscous(coef, zc, q[0, up, :], q[0, down, :])
        fv = -coriolis * zc - gy + viscous(coef, vc, q[1, up, :], q[1, down, :])
        fz = fz + q[5, rows, :] / thick - drag * zc
        fv = fv + q[6, rows, :] / thick - drag * vc
        z_new = sea * (zc + DT * fz)
        v_new = sea * (vc + DT * fv)
        zq[rows, :] = z_new
        vq[rows, :] = v_new
        sums = []
        for one in (thick * (z_new * z_new + v_new * v_new), thick):
            one = one + pltpu.roll(one, 64, 1)
            sums.append(one + pltpu.roll(one, 32, 1))
        fsq[0, rows, :] = z_new
        fsq[1, rows, :] = v_new
        fsq[2, rows, :] = sea * (thick - REST)
        fsq[3, rows, :] = sea * (0.5 * sums[0] / sums[1])
        return carry

    lax.fori_loop(0, EXT // QM, packed_momentum, 0)

    for c in range(4):
        fs[c, 8:24, :] = fse[0, c, 8:24, :]
        fs[c, 24:40, :] = fs0[c, 24:40, :]
        fs[c, N - 8 : N + 8, :] = fs0[c, N - 8 : N + 8, :]
        fs[c, N + 8 : N + 24, :] = fse[1, c, 8:24, :]

    row = lax.broadcasted_iota(jnp.int32, (8, N), 0)
    for k in range(9):
        if 1 <= k <= 6:
            inner = ft0[k - 1]
        else:
            inner = fs[:, 16 * k + 8 : 16 * k + 40, :].reshape(N, N).T
        ends = fsq[:, 16 * k + 8 : 16 * k + 40, :].reshape(N, N).T
        low = jnp.where(row < 4, ends[8:16], inner[0:8])
        high = jnp.where(row >= 4, ends[16:24], inner[N - 8 : N])
        ft[k, 0:8, :] = ends[0:8]
        ft[k, 8:16, :] = low
        ft[k, 16:N, :] = inner[8 : N - 8]
        ft[k, N : N + 8, :] = high
        ft[k, N + 8 : N + 16, :] = ends[24:32]
        ft[k, N + 16 : N + 24, :] = ends[0:8]
        ft[k, N + 24 : N + 32, :] = low

    def merge(size, rows, packed_rows, sources):
        lane = lanes(size)
        for packed, out, read in sources:
            whole = packed[packed_rows, :]
            for l in range(LAYERS):
                low = pltpu.roll(whole, (N - 32 * l - 8) % N, 1)
                high = pltpu.roll(whole, (104 - 32 * l) % N, 1)
                out[l, rows, :] = jnp.where(lane < 4, low, jnp.where(lane >= N - 4, high, read(l)))

    order = lax.broadcasted_iota(jnp.int32, (EXT, 2 * N), 0)
    lat = 9 * lax.rem(order, 16) + order // 16
    keep = jnp.where(lat < N, 1.0, jnp.where(lat < N + 8, has_north, has_south)) > 0.5
    b1 = jnp.concatenate([consts[4:5, :]] * 2, axis=1)
    b2 = jnp.concatenate([consts[5:6, :]] * 2, axis=1)

    def activate(x, bias):
        x = x + bias
        return jnp.where(keep, x + x * jnp.tanh(x), 0.0)

    def first_layer(k, quarters):
        parts = []
        for b in range(3):
            pieces = []
            for t in range(TILES):
                for half in range(2):
                    pieces.append(ft[k, pl.ds(7 + t + b + 72 * half, 8, stride=9), :])
            parts.append(jnp.concatenate(pieces, axis=0).astype(BF16))
        left = jnp.concatenate(parts, axis=1)
        for quarter in range(quarters):
            out = jnp.dot(left, first_w[:, 256 * quarter : 256 * quarter + 256], preferred_element_type=F32)
            out = activate(out, b1)
            at = 4 * k + quarter
            for p in range(2):
                one = out[:, N * p : N * p + N]
                h1[at, p, 16 : 16 + EXT, :] = one.astype(BF16)
                h1[at, p, 0:16, :] = pltpu.roll(one[EXT - 16 : EXT], 1, 0).astype(BF16)
                h1[at, p, 16 + EXT : 32 + EXT, :] = pltpu.roll(one[0:16], 15, 0).astype(BF16)

    def first_body(k, carry):
        first_layer(k, 4)
        rows = pl.ds(pl.multiple_of(16 * k + 8, 8), 16)
        wide = pl.ds(pl.multiple_of(16 * k + 24, 8), 16)
        merge(16, rows, wide, (
            (zq, zm, lambda l: zo[l, wide, :]),
            (vq, vm, lambda l: vo[l, wide, :]),
            (hq, hm, lambda l: t0[l, wide, :]),
        ))
        return carry

    lax.fori_loop(0, 7, first_body, 0)
    for e, (at, inner) in enumerate(((0, 16), (N - 8, 8))):
        merge(8, pl.ds(at, 8), pl.ds(at + 16, 8), (
            (zq, zm, lambda l: ze[e, l, inner : inner + 8, :]),
            (vq, vm, lambda l: ve[e, l, inner : inner + 8, :]),
            (hq, hm, lambda l: te[e, l, inner : inner + 8, :]),
        ))
    first_layer(7, 4)
    first_layer(8, 2)
    stores = [
        pltpu.make_async_copy(src, dst, store_sem.at[k])
        for k, (src, dst) in enumerate(((zm, z_out), (vm, v_out), (hm, h_out)))
    ]
    for copy in stores:
        copy.start()

    def second_matmul(k, ref):
        g = k * STEP
        parts = []
        for b in range(3):
            for d in range(3):
                block = h1[pl.ds(g + d // 2, STEP), d % 2, 16 * b : 16 * b + EXT, :]
                parts.append(block.reshape(BLOCK, N))
        left = jnp.concatenate(parts, axis=1)
        ref[...] = jnp.dot(left, second_w[...], preferred_element_type=F32)

    def finish(k, ref):
        for i in range(STEP):
            one = activate(ref[i * EXT : (i + 1) * EXT], b2).astype(BF16)
            sums = lax.dot_general(
                last_w[...], one, (((1,), (1,)), ((), ())), preferred_element_type=F32
            )
            rs[k * STEP + i] = sums[0:24, 0:N]
            re[k * STEP + i, :, 0:16] = sums[0:24, N:EXT]

    second_matmul(0, d0)

    def second_layer(k, carry):
        second_matmul(2 * k + 1, d1)
        finish(2 * k, d0)
        second_matmul(2 * k + 2, d0)
        finish(2 * k + 1, d1)
        return carry

    lax.fori_loop(0, 5, second_layer, 0)
    finish(10, d0)

    upper = lax.broadcasted_iota(jnp.int32, (8, N), 0) < 4
    for b in range(3):
        blocks = []
        for ref in (rs, re):
            rows = []
            for k in range(N // 8):
                x, y, zz = (ref[2 * k + i, 8 * b : 8 * b + 8, :] for i in range(3))
                y = pltpu.roll(y, 4, 0)
                rows.append(jnp.where(upper, x, y) + jnp.where(upper, y, zz))
            blocks.append(jnp.concatenate(rows, axis=0).T)
        for t in range(TILES):
            for half in range(2):
                block, at = (blocks[0], 16 * t) if t < 8 else (blocks[1], 0)
                at = at + 8 * half
                nat[b, pl.ds(8 + t + 72 * half, 8, stride=9), :] = block[at : at + 8]
        nat[b, 0:8, :] = nat[b, EXT : EXT + 8, :]
    total = nat[0, 7 : 7 + N, :] + nat[1, 8 : 8 + N, :] + nat[2, 9 : 9 + N, :]
    visc_out[...] = jnp.exp(total.T)
    for copy in stores:
        copy.wait()


PACK, CONT, MOM, OWN, SPREAD, QC, QM = 32, 32, 16, 32, 32, 48, 24


def step(state):
    vmem = pl.BlockSpec(memory_space=pltpu.VMEM)
    hbm = pl.BlockSpec(memory_space=HBM)
    whole = jax.ShapeDtypeStruct((LAYERS, N, N), F32)
    return pl.pallas_call(
        step_kernel,
        out_shape=(whole, whole, whole, jax.ShapeDtypeStruct((N, N), F32)),
        in_specs=[vmem] * 15,
        out_specs=[hbm] * 3 + [vmem],
        scratch_shapes=[
            pltpu.VMEM((2, FIELDS, EDGE, N), F32),
            pltpu.VMEM((2, LAYERS, EDGE, N), F32),
            pltpu.VMEM((2, LAYERS, EDGE, N), F32),
            pltpu.VMEM((2, LAYERS, EDGE, N), F32),
            pltpu.VMEM((2, LAYERS, EDGE, N), F32),
            pltpu.VMEM((2, 4, EDGE, N), F32),
            pltpu.VMEM((7, PAD, N), F32),
            pltpu.VMEM((PAD, N), F32),
            pltpu.VMEM((PAD, N), F32),
            pltpu.VMEM((PAD, N), F32),
            pltpu.VMEM((PAD, N), F32),
            pltpu.VMEM((4, TALL, N), F32),
            pltpu.VMEM((4, TALL, N), F32),
            pltpu.VMEM((9, EXT + 16, N), F32),
            pltpu.VMEM((LAYERS, N, N), F32),
            pltpu.VMEM((LAYERS, N, N), F32),
            pltpu.VMEM((LAYERS, N, N), F32),
            pltpu.VMEM((PAIRS // 2, 2, EXT + 32, N), BF16),
            pltpu.VMEM((BLOCK, 2 * N), F32),
            pltpu.VMEM((BLOCK, 2 * N), F32),
            pltpu.VMEM((GROUPS, 24, N), F32),
            pltpu.VMEM((GROUPS, 24, N), F32),
            pltpu.VMEM((3, EXT + 16, N), F32),
            pltpu.SemaphoreType.DMA((3,)),
        ],
        compiler_params=pltpu.CompilerParams(vmem_limit_bytes=24 * 2**20),
        name="step",
    )(*state)


def local(z, v, h, ls, vi, w, grav, conv1, bias1, conv2, bias2, conv3):
    conv1 = jnp.transpose(conv1, (0, 1, 3, 2))
    conv3 = jnp.transpose(conv3, (0, 2, 1, 3))
    held = [pltpu.with_memory_space_constraint(x, HBM) for x in (z, v, h, ls, vi, w, grav, conv1, conv2, conv3, bias1, bias2)]
    return step(exchange(held[:6], *held[6:]))


def solution(mesh):
    block, flat = P(None, "ox", "oy"), P("ox", "oy")
    return jax.shard_map(
        local,
        mesh=mesh,
        in_specs=(block, block, block, flat, flat, block) + (P(),) * 6,
        out_specs=(block, block, block, flat),
        check_vma=False,
    )
```

```python
import jax
import jax.numpy as jnp
from jax import lax
from jax.experimental import pallas as pl
from jax.experimental.pallas import tpu as pltpu
from jax.sharding import PartitionSpec as P

MESH = pl.DeviceIdType.MESH
F32 = jnp.float32
BF16 = jnp.bfloat16

DT = 0.05
REST = 1.4
DRAG = 0.5
LAYERS = 4
N = 128
HID = 64
FIELDS = 16
SEA, VISC, WIND = 12, 13, 14
EXT = N + 16
PAD = N + 32
TALL = N + 40
PAIRS = 72
GROUPS = 33
STEP = 3
TILES = EXT // 16
BLOCK = STEP * EXT


HBM = pltpu.HBM
EDGE = 32


def lanes(rows):
    return lax.broadcasted_iota(jnp.int32, (rows, N), 1)


def near(x):
    return pltpu.roll(x, N - 1, 1), pltpu.roll(x, 1, 1)


def shifted(start, size):
    aligned = start if isinstance(start, int) else pl.multiple_of(start, 8)
    return pl.ds(aligned, size), pl.ds(start + 1, size), pl.ds(start - 1, size)


def continuity(f, press, depth, grav, start, size):
    rows, up, down = shifted(start, size)
    sea = f[SEA, rows, :]
    anomaly = []
    for l in range(LAYERS):
        thick = f[8 + l, rows, :]
        fn, fs = near(f[4 + l, rows, :] * thick)
        fe = f[l, up, :] * f[8 + l, up, :]
        fw = f[l, down, :] * f[8 + l, down, :]
        diverge = (fe - fw) * 0.5 + (fn - fs) * 0.5
        new = thick - DT * sea * diverge
        depth[l, rows, :] = new
        anomaly.append(new - REST)
    faces = [anomaly[3]]
    for l in (2, 1, 0):
        faces.insert(0, faces[0] + anomaly[l])
    total = grav[0] * faces[0]
    press[0, rows, :] = total
    for l in range(1, LAYERS):
        total = total + grav[l] * faces[l]
        press[l, rows, :] = total


def coefficients(visc, up, down):
    return [0.5 * (visc + other) for other in (up, down, *near(visc))]


def viscous(coef, centre, up, down):
    total = None
    for c, q in zip(coef, (up, down, *near(centre))):
        term = c * (q - centre)
        total = term if total is None else total + term
    return total


def coriolis_of(lat, ny):
    return 0.3 + 1.4 * (lat.astype(F32) + 0.5) / (N * ny)


def momentum(f, press, depth, zo, vo, feature_refs, coriolis, start, size):
    rows, up, down = shifted(start, size)
    sea = f[SEA, rows, :]
    coef = coefficients(f[VISC, rows, :], f[VISC, up, :], f[VISC, down, :])
    kinetic = column = None
    for l in range(LAYERS):
        zc, vc = f[l, rows, :], f[4 + l, rows, :]
        pn, ps = near(press[l, rows, :])
        gx = (press[l, up, :] - press[l, down, :]) * 0.5
        gy = (pn - ps) * 0.5
        thick = depth[l, rows, :]
        fz = coriolis * vc - gx + viscous(coef, zc, f[l, up, :], f[l, down, :])
        fv = -coriolis * zc - gy + viscous(coef, vc, f[4 + l, up, :], f[4 + l, down, :])
        if l == 0:
            fz = fz + f[WIND, rows, :] / thick
            fv = fv + f[WIND + 1, rows, :] / thick
        if l == LAYERS - 1:
            fz = fz - DRAG * zc
            fv = fv - DRAG * vc
        z_new = sea * (zc + DT * fz)
        v_new = sea * (vc + DT * fv)
        zo[l, rows, :] = z_new
        vo[l, rows, :] = v_new
        part = thick * (z_new * z_new + v_new * v_new)
        kinetic = part if l == 0 else kinetic + part
        column = thick if l == 0 else column + thick
        if l == 0:
            feature_refs[0][0, rows, :] = z_new
            feature_refs[0][1, rows, :] = v_new
            feature_refs[0][2, rows, :] = sea * (thick - REST)
    feature_refs[0][3, rows, :] = sea * (0.5 * kinetic / column)


def own_pack(read, lane):
    packed = None
    for l in range(4):
        field = read(l)
        for at, shift in ((32 * l + 8, 32 * l + 8), (32 * l + 16, 32 * l + 16 + 8)):
            moved = pltpu.roll(field, shift % N, 1)
            packed = moved if packed is None else jnp.where((lane >= at) & (lane < at + 8), moved, packed)
    return packed


def exchange_kernel(
    z, v, h, ls, vi, w, grav_in, conv1, conv2, conv3, bias1, bias2,
    f0, p0, t0, zo, vo, fs, ft, own, ns, xw, xe, first_w, second_w, last_w, consts,
    sea_i, sb, nb, rows24, c1, c2, c3, grav, s1, s2, load_sem, send_sem, recv_sem,
):
    ox, oy = lax.axis_index("ox"), lax.axis_index("oy")
    nx, ny = lax.axis_size("ox"), lax.axis_size("oy")
    east, west = lax.rem(ox + 1, nx), lax.rem(ox + nx - 1, nx)
    above, below = lax.rem(oy + 1, ny), lax.rem(oy + ny - 1, ny)
    peers = (
        (east, oy), (west, oy),
        (ox, above), (east, above), (west, above),
        (ox, below), (east, below), (west, below),
    )
    barrier = pltpu.get_barrier_semaphore()
    has_north, has_south = oy < ny - 1, oy > 0

    def greet(first_peer, last_peer):
        for peer in peers[first_peer:last_peer]:
            pl.semaphore_signal(barrier, inc=1, device_id=peer, device_id_type=MESH)

    greet(0, 2)
    pl.when(has_north)(lambda: greet(2, 5))
    pl.when(has_south)(lambda: greet(5, 8))
    mid = pl.ds(16, N)
    loads = [
        pltpu.make_async_copy(src, dst, load_sem.at[k])
        for k, (src, dst) in enumerate((
            (ls, sea_i), (z, f0.at[0:4, mid]), (v, f0.at[4:8, mid]), (h, f0.at[8:12, mid]),
            (vi, f0.at[VISC, mid]), (w, f0.at[WIND : WIND + 2, mid]),
            (conv1, c1), (conv2, c2), (conv3, c3), (grav_in, grav), (bias1, s1), (bias2, s2),
        ))
    ]
    for copy in loads:
        copy.start()
    ones = jnp.ones((8, N), F32)
    for rows in (pl.ds(8, 8), pl.ds(N + 16, 8)):
        for k in range(FIELDS):
            f0[k, rows, :] = ones
        for k in range(LAYERS):
            p0[k, rows, :] = ones
    for copy in loads[:6]:
        copy.wait()

    def pack(k, carry):
        src = pl.ds(pl.multiple_of(PACK * k + 16, 8), PACK)
        rows = pl.ds(pl.multiple_of(PACK * k, 8), PACK)
        lane = lanes(PACK)
        sea = sea_i[rows, :].astype(F32)
        f0[SEA, src, :] = sea
        to_south = to_north = None
        for a in range(4):
            for l in range(4):
                field = sea if 4 * a + l == SEA else f0[4 * a + l, src, :]
                if a < 2:
                    field = field * sea
                    f0[4 * a + l, src, :] = field
                at = 32 * l + 8 * a
                moved = pltpu.roll(field, at, 1) if at else field
                if to_south is None:
                    to_south = to_north = moved
                else:
                    to_south = jnp.where((lane >= at) & (lane < at + 8), moved, to_south)
                    to_north = jnp.where((lane >= at - 8) & (lane < at), moved, to_north)
        sb[rows, :] = to_south
        nb[rows, :] = to_north
        return carry

    lax.fori_loop(0, N // PACK, pack, 0)
    pl.semaphore_wait(barrier, 2 + 3 * has_north.astype(jnp.int32) + 3 * has_south.astype(jnp.int32))

    first, last = pl.ds(0, 8), pl.ds(N - 8, 8)
    def move(k, src, dst, peer):
        return pltpu.make_async_remote_copy(
            src_ref=src, dst_ref=dst, send_sem=send_sem.at[k], recv_sem=recv_sem.at[k],
            device_id=peer, device_id_type=MESH,
        )

    along = (
        move(0, f0.at[:, N + 8 : N + 16], xw, (east, oy)),
        move(1, f0.at[:, 16:24], xe, (west, oy)),
    )
    northward = (
        move(2, nb.at[last], ns.at[1, 0:8], (east, above)),
        move(3, nb.at[first], ns.at[1, N + 8 : EXT], (west, above)),
        move(4, nb, ns.at[1, 8 : 8 + N], (ox, above)),
    )
    southward = (
        move(5, sb.at[last], ns.at[0, 0:8], (east, below)),
        move(6, sb.at[first], ns.at[0, N + 8 : EXT], (west, below)),
        move(7, sb, ns.at[0, 8 : 8 + N], (ox, below)),
    )

    def start(copies):
        for copy in copies:
            copy.start()

    pl.when(has_north)(lambda: start(northward[:2]))
    pl.when(has_south)(lambda: start(southward[:2]))
    start(along)
    pl.when(has_north)(lambda: start(northward[2:]))
    pl.when(has_south)(lambda: start(southward[2:]))

    @pl.when(jnp.logical_not(has_north))
    def _():
        ns[0] = jnp.ones((EXT, N), F32)

    @pl.when(jnp.logical_not(has_south))
    def _():
        ns[1] = jnp.ones((EXT, N), F32)

    for copy in loads[6:]:
        copy.wait()
    build_weights(c1, c2, c3, first_w, second_w, last_w, rows24)
    for l in range(LAYERS):
        consts[l : l + 1, :] = jnp.full((1, N), grav[l], F32)
    for k, bias in enumerate((s1, s2)):
        half = bias[...].reshape(1, HID) * 0.5
        consts[4 + k : 5 + k, :] = jnp.concatenate([half, half], axis=1)

    def inner_continuity(k, carry):
        continuity(f0, p0, t0, grav, CONT * k + 16, CONT)
        return carry

    lax.fori_loop(0, N // CONT, inner_continuity, 0)

    def inner_momentum(k, carry):
        coriolis = coriolis_of(oy * N + lanes(MOM), ny)
        momentum(f0, p0, t0, zo, vo, (fs,), coriolis, MOM * k + 16, MOM)
        return carry

    lax.fori_loop(0, N // MOM, inner_momentum, 0)

    def inner_pack(k, carry):
        src = pl.ds(pl.multiple_of(OWN * k + 16, 8), OWN)
        rows = pl.ds(pl.multiple_of(OWN * k, 8), OWN)
        for a in range(4):
            own[a, rows, :] = own_pack(lambda l: f0[4 * a + l, src, :], lanes(OWN))
        return carry

    lax.fori_loop(0, N // OWN, inner_pack, 0)

    def inner_turn(k, carry):
        rows = pl.ds(pl.multiple_of(16 * k + 24, 8), 32)
        ft[k] = fs[:, rows, :].reshape(N, N).T
        return carry

    lax.fori_loop(0, 6, inner_turn, 0)

    def sent(copies):
        for copy in copies:
            copy.wait_send()

    def received(copies):
        for copy in copies:
            copy.wait_recv()

    sent(along)
    pl.when(has_north)(lambda: sent(northward))
    pl.when(has_south)(lambda: sent(southward))
    received(along)
    pl.when(has_north)(lambda: received(southward))
    pl.when(has_south)(lambda: received(northward))


def exchange(fields, grav, conv1, conv2, conv3, bias1, bias2):
    hbm = pl.BlockSpec(memory_space=HBM)
    vmem = pl.BlockSpec(memory_space=pltpu.VMEM)

    def array(*shape, dtype=F32):
        return jax.ShapeDtypeStruct(shape, dtype)

    return pl.pallas_call(
        exchange_kernel,
        out_shape=(
            array(FIELDS, PAD, N), array(LAYERS, PAD, N), array(LAYERS, PAD, N),
            array(LAYERS, PAD, N), array(LAYERS, PAD, N), array(4, PAD, N),
            array(6, N, N), array(4, N, N), array(2, EXT, N),
            array(FIELDS, 8, N), array(FIELDS, 8, N),
            array(3 * N, 16 * HID, dtype=BF16), array(18 * HID, 4 * HID, dtype=BF16),
            array(32, 2 * N, dtype=BF16), array(8, N),
        ),
        in_specs=[hbm] * 12,
        out_specs=(vmem,) * 15,
        scratch_shapes=[
            pltpu.VMEM((N, N), jnp.int32),
            pltpu.VMEM((N, N), F32),
            pltpu.VMEM((N, N), F32),
            pltpu.VMEM((32, 2 * N), F32),
            pltpu.VMEM(conv1.shape, BF16),
            pltpu.VMEM(conv2.shape, BF16),
            pltpu.VMEM(conv3.shape, BF16),
            pltpu.SMEM((LAYERS,), F32),
            pltpu.VMEM((HID,), F32),
            pltpu.VMEM((HID,), F32),
            pltpu.SemaphoreType.DMA((12,)),
            pltpu.SemaphoreType.DMA((8,)),
            pltpu.SemaphoreType.DMA((8,)),
        ],
        compiler_params=pltpu.CompilerParams(
            collective_id=0, has_side_effects=True, vmem_limit_bytes=16 * 2**20
        ),
        name="exchange",
    )(*fields, grav, conv1, conv2, conv3, bias1, bias2)


def build_weights(conv1, conv2, conv3, first_w, second_w, last_w, rows24):
    lane = lax.broadcasted_iota(jnp.int32, (8, N), 1)
    right = lane >= HID
    row = lax.broadcasted_iota(jnp.int32, (8, N), 0)

    nt = (((1,), (1,)), ((), ()))
    taps = {}
    for a in range(3):
        for b in range(3):
            one = conv1[a, b].astype(F32) * 0.5
            taps[a, b] = jnp.concatenate([one, one], axis=1)
    for b in range(3):
        for c in range(4):
            vecs = [jnp.broadcast_to(taps[a, b][c : c + 1], (8, N)) for a in range(3)]
            for jp in range(8):
                parts = []
                for i in range(4):
                    gap = row + 8 * i - 2 * jp - jnp.where(right, 1, 0) - 4
                    val = jnp.zeros((8, N), F32)
                    for a in range(3):
                        val = jnp.where(gap == a, vecs[a], val)
                    parts.append(val)
                start = 128 * b + 32 * c
                first_w[start : start + 32, N * jp : N * jp + N] = jnp.concatenate(parts, 0).astype(BF16)

    eye = lax.broadcasted_iota(jnp.int32, (HID, HID), 0) == lax.broadcasted_iota(jnp.int32, (HID, HID), 1)
    eye = jnp.where(eye, 0.5, 0.0).astype(BF16)
    side = lax.broadcasted_iota(jnp.int32, (HID, N), 1) >= HID
    for b in range(3):
        turned = []
        for a in range(3):
            one = conv2[a, b]
            both = jnp.concatenate([one, one], axis=0)
            turned.append(lax.dot_general(eye, both, nt, preferred_element_type=F32))
        zero = jnp.zeros((HID, N), F32)
        for m in range(6):
            for jp in range(2):
                tap = m - 2 * jp
                left = turned[tap] if 0 <= tap < 3 else zero
                other = turned[tap - 1] if 0 <= tap - 1 < 3 else zero
                start = (6 * b + m) * HID
                second_w[start : start + HID, N * jp : N * jp + N] = jnp.where(side, other, left).astype(BF16)

    rows24[...] = jnp.zeros((32, 2 * N), F32)
    for b in range(3):
        for place, i in ((0, 3), (1, 4), (2, 5), (5, 0), (6, 1), (7, 2)):
            for m in range(4):
                a = m - i + 2
                if 0 <= a < 3:
                    rows24[8 * b + place : 8 * b + place + 1, HID * m : HID * m + HID] = conv3[a, 0, b : b + 1].astype(F32)
    last_w[...] = rows24[...].astype(BF16)


def step_kernel(
    f0, p0, t0, zo, vo, fs0, ft0, own, ns, xw, xe, first_w, second_w, last_w, consts,
    z_out, v_out, h_out, visc_out,
    fe, pe, te, ze, ve, fse, q, pq, hq, zq, vq, fsq, fs, ft, zm, vm, hm, h1, d0, d1, rs, re, nat,
    store_sem,
):
    oy, ny = lax.axis_index("oy"), lax.axis_size("oy")
    has_north = (oy < ny - 1).astype(F32)
    has_south = (oy > 0).astype(F32)
    ones = jnp.ones((8, N), F32)
    grav = [consts[l : l + 1, :] for l in range(LAYERS)]

    for e, (rows, src) in enumerate((((8, xw), (16, 16)), ((0, N), (16, xe)))):
        (halo_at, halo), (own_at, own_from) = (rows, src) if e == 0 else (src, rows)
        pad = 0 if e == 0 else 24
        for k in range(FIELDS):
            fe[e, k, halo_at : halo_at + 8, :] = halo[k]
            fe[e, k, own_at : own_at + 16, :] = f0[k, own_from : own_from + 16, :]
            fe[e, k, pad : pad + 8, :] = ones
        inner_at, inner_from = (24, 24) if e == 0 else (0, N)
        for k in range(LAYERS):
            pe[e, k, pad : pad + 8, :] = ones
            pe[e, k, inner_at : inner_at + 8, :] = p0[k, inner_from : inner_from + 8, :]
    for e in range(2):
        continuity(fe.at[e], pe.at[e], te.at[e], grav, 8, 16)
    for e in range(2):
        coriolis = coriolis_of(oy * N + lanes(16), ny)
        momentum(fe.at[e], pe.at[e], te.at[e], ze.at[e], ve.at[e], (fse.at[e],), coriolis, 8, 16)

    for k in range(7):
        q[k, 0:8, :] = ones
        q[k, PAD - 8 : PAD, :] = ones
    pq[0:8, :] = ones
    pq[PAD - 8 : PAD, :] = ones
    for c in range(4):
        fs[c, EXT + 8 : TALL, :] = jnp.zeros((TALL - EXT - 8, N), F32)
        fsq[c, EXT + 8 : TALL, :] = jnp.zeros((TALL - EXT - 8, N), F32)

    def spread(start, size, groups):
        lane = lanes(size)
        part = lax.rem(lane, 32)
        seg = lane // 32
        inside = jnp.where(part < 8, has_south, jnp.where(part < 24, 1.0, has_north))
        rows = pl.ds(start + 8 if isinstance(start, int) else pl.multiple_of(start + 8, 8), size)
        src = pl.ds(start if isinstance(start, int) else pl.multiple_of(start, 8), size)
        from_north, from_south = ns[0, src, :], ns[1, src, :]
        full = []
        for a in range(4):
            high = pltpu.roll(from_north, (24 - 8 * a) % N, 1)
            low = pltpu.roll(from_south, (8 - 8 * a) % N, 1)
            full.append(jnp.where(part < 8, low, jnp.where(part < 24, groups(a), high)))
        q[0, rows, :] = full[0] * inside
        q[1, rows, :] = full[1] * inside
        q[2, rows, :] = full[2]
        for k, s in ((3, 0), (4, 1)):
            one = jnp.where(seg == s, full[3] * inside, 0.0)
            one = one + pltpu.roll(one, 32, 1)
            q[k, rows, :] = one + pltpu.roll(one, 64, 1)
        for k, s in ((5, 2), (6, 3)):
            q[k, rows, :] = jnp.where(seg == 0, pltpu.roll(full[3], N - 32 * s, 1), 0.0)

    for at, strip in ((0, xw), (N + 8, xe)):
        spread(at, 8, lambda a: own_pack(lambda l: strip[4 * a + l], lanes(8)))

    def spread_body(k, carry):
        rows = pl.ds(pl.multiple_of(SPREAD * k, 8), SPREAD)
        spread(SPREAD * k + 8, SPREAD, lambda a: own[a, rows, :])
        return carry

    lax.fori_loop(0, N // SPREAD, spread_body, 0)

    def packed_continuity(k, carry):
        size = QC
        lane = lanes(size)
        part, seg = lax.rem(lane, 32), lane // 32
        inside = jnp.where(part < 8, has_south, jnp.where(part < 24, 1.0, has_north))
        weight = jnp.where(seg == 0, grav[0], jnp.where(seg == 1, grav[1], jnp.where(seg == 2, grav[2], grav[3])))
        rows, up, down = shifted(size * k + 8, size)
        thick = q[2, rows, :]
        fn, fs_ = near(q[1, rows, :] * thick)
        fe_ = q[0, up, :] * q[2, up, :]
        fw_ = q[0, down, :] * q[2, down, :]
        diverge = (fe_ - fw_) * 0.5 + (fn - fs_) * 0.5
        new = thick - DT * q[3, rows, :] * diverge
        hq[rows, :] = new
        a = new - REST
        face = a
        for n in (1, 2, 3):
            face = face + jnp.where(seg < 4 - n, pltpu.roll(a, N - 32 * n, 1), 0.0)
        term = weight * face
        total = term
        for n in (1, 2, 3):
            total = total + jnp.where(seg >= n, pltpu.roll(term, 32 * n, 1), 0.0)
        pq[rows, :] = total * inside
        return carry

    lax.fori_loop(0, EXT // QC, packed_continuity, 0)

    def packed_momentum(k, carry):
        size = QM
        lane = lanes(size)
        part, seg = lax.rem(lane, 32), lane // 32
        coriolis = coriolis_of(oy * N + part + jnp.where(part < 16, -8, 104), ny)
        drag = jnp.where(seg == 3, DRAG, 0.0)
        rows, up, down = shifted(size * k + 8, size)
        zc, vc, sea = q[0, rows, :], q[1, rows, :], q[3, rows, :]
        coef = coefficients(q[4, rows, :], q[4, up, :], q[4, down, :])
        pn, ps = near(pq[rows, :])
        gx = (pq[up, :] - pq[down, :]) * 0.5
        gy = (pn - ps) * 0.5
        thick = hq[rows, :]
        fz = coriolis * vc - gx + viscous(coef, zc, q[0, up, :], q[0, down, :])
        fv = -coriolis * zc - gy + viscous(coef, vc, q[1, up, :], q[1, down, :])
        fz = fz + q[5, rows, :] / thick - drag * zc
        fv = fv + q[6, rows, :] / thick - drag * vc
        z_new = sea * (zc + DT * fz)
        v_new = sea * (vc + DT * fv)
        zq[rows, :] = z_new
        vq[rows, :] = v_new
        sums = []
        for one in (thick * (z_new * z_new + v_new * v_new), thick):
            one = one + pltpu.roll(one, 64, 1)
            sums.append(one + pltpu.roll(one, 32, 1))
        fsq[0, rows, :] = z_new
        fsq[1, rows, :] = v_new
        fsq[2, rows, :] = sea * (thick - REST)
        fsq[3, rows, :] = sea * (0.5 * sums[0] / sums[1])
        return carry

    lax.fori_loop(0, EXT // QM, packed_momentum, 0)

    for c in range(4):
        fs[c, 8:24, :] = fse[0, c, 8:24, :]
        fs[c, 24:40, :] = fs0[c, 24:40, :]
        fs[c, N - 8 : N + 8, :] = fs0[c, N - 8 : N + 8, :]
        fs[c, N + 8 : N + 24, :] = fse[1, c, 8:24, :]

    row = lax.broadcasted_iota(jnp.int32, (8, N), 0)
    for k in range(9):
        if 1 <= k <= 6:
            inner = ft0[k - 1]
        else:
            inner = fs[:, 16 * k + 8 : 16 * k + 40, :].reshape(N, N).T
        ends = fsq[:, 16 * k + 8 : 16 * k + 40, :].reshape(N, N).T
        low = jnp.where(row < 4, ends[8:16], inner[0:8])
        high = jnp.where(row >= 4, ends[16:24], inner[N - 8 : N])
        ft[k, 0:8, :] = ends[0:8]
        ft[k, 8:16, :] = low
        ft[k, 16:N, :] = inner[8 : N - 8]
        ft[k, N : N + 8, :] = high
        ft[k, N + 8 : N + 16, :] = ends[24:32]
        ft[k, N + 16 : N + 24, :] = ends[0:8]
        ft[k, N + 24 : N + 32, :] = low

    def merge(size, rows, packed_rows, sources):
        lane = lanes(size)
        for packed, out, read in sources:
            whole = packed[packed_rows, :]
            for l in range(LAYERS):
                low = pltpu.roll(whole, (N - 32 * l - 8) % N, 1)
                high = pltpu.roll(whole, (104 - 32 * l) % N, 1)
                out[l, rows, :] = jnp.where(lane < 4, low, jnp.where(lane >= N - 4, high, read(l)))

    order = lax.broadcasted_iota(jnp.int32, (EXT, 2 * N), 0)
    lat = 9 * lax.rem(order, 16) + order // 16
    keep = jnp.where(lat < N, 1.0, jnp.where(lat < N + 8, has_north, has_south)) > 0.5
    b1 = jnp.concatenate([consts[4:5, :]] * 2, axis=1)
    b2 = jnp.concatenate([consts[5:6, :]] * 2, axis=1)

    def activate(x, bias):
        x = x + bias
        return jnp.where(keep, x + x * jnp.tanh(x), 0.0)

    def first_layer(k, quarters):
        parts = []
        for b in range(3):
            pieces = []
            for t in range(TILES):
                for half in range(2):
                    pieces.append(ft[k, pl.ds(7 + t + b + 72 * half, 8, stride=9), :])
            parts.append(jnp.concatenate(pieces, axis=0).astype(BF16))
        left = jnp.concatenate(parts, axis=1)
        for quarter in range(quarters):
            out = jnp.dot(left, first_w[:, 256 * quarter : 256 * quarter + 256], preferred_element_type=F32)
            out = activate(out, b1)
            at = 4 * k + quarter
            for p in range(2):
                one = out[:, N * p : N * p + N]
                h1[at, p, 16 : 16 + EXT, :] = one.astype(BF16)
                h1[at, p, 0:16, :] = pltpu.roll(one[EXT - 16 : EXT], 1, 0).astype(BF16)
                h1[at, p, 16 + EXT : 32 + EXT, :] = pltpu.roll(one[0:16], 15, 0).astype(BF16)

    def first_body(k, carry):
        first_layer(k, 4)
        rows = pl.ds(pl.multiple_of(16 * k + 8, 8), 16)
        wide = pl.ds(pl.multiple_of(16 * k + 24, 8), 16)
        merge(16, rows, wide, (
            (zq, zm, lambda l: zo[l, wide, :]),
            (vq, vm, lambda l: vo[l, wide, :]),
            (hq, hm, lambda l: t0[l, wide, :]),
        ))
        return carry

    for k in range(7):
        first_body(k, 0)
    for e, (at, inner) in enumerate(((0, 16), (N - 8, 8))):
        merge(8, pl.ds(at, 8), pl.ds(at + 16, 8), (
            (zq, zm, lambda l: ze[e, l, inner : inner + 8, :]),
            (vq, vm, lambda l: ve[e, l, inner : inner + 8, :]),
            (hq, hm, lambda l: te[e, l, inner : inner + 8, :]),
        ))
    first_layer(7, 4)
    first_layer(8, 2)
    stores = [
        pltpu.make_async_copy(src, dst, store_sem.at[k])
        for k, (src, dst) in enumerate(((zm, z_out), (vm, v_out), (hm, h_out)))
    ]
    for copy in stores:
        copy.start()

    def second_matmul(k, ref):
        g = k * STEP
        parts = []
        for b in range(3):
            for d in range(3):
                block = h1[pl.ds(g + d // 2, STEP), d % 2, 16 * b : 16 * b + EXT, :]
                parts.append(block.reshape(BLOCK, N))
        left = jnp.concatenate(parts, axis=1)
        ref[...] = jnp.dot(left, second_w[...], preferred_element_type=F32)

    def finish(k, ref):
        for i in range(STEP):
            one = activate(ref[i * EXT : (i + 1) * EXT], b2).astype(BF16)
            sums = lax.dot_general(
                last_w[...], one, (((1,), (1,)), ((), ())), preferred_element_type=F32
            )
            rs[k * STEP + i] = sums[0:24, 0:N]
            re[k * STEP + i, :, 0:16] = sums[0:24, N:EXT]

    held = (d0, d1)
    for k in range(11):
        second_matmul(k, held[k % 2])
        if k:
            finish(k - 1, held[(k - 1) % 2])
    finish(10, held[10 % 2])

    upper = lax.broadcasted_iota(jnp.int32, (8, N), 0) < 4
    for b in range(3):
        blocks = []
        for ref in (rs, re):
            rows = []
            for k in range(N // 8):
                x, y, zz = (ref[2 * k + i, 8 * b : 8 * b + 8, :] for i in range(3))
                y = pltpu.roll(y, 4, 0)
                rows.append(jnp.where(upper, x, y) + jnp.where(upper, y, zz))
            blocks.append(jnp.concatenate(rows, axis=0).T)
        for t in range(TILES):
            for half in range(2):
                block, at = (blocks[0], 16 * t) if t < 8 else (blocks[1], 0)
                at = at + 8 * half
                nat[b, pl.ds(8 + t + 72 * half, 8, stride=9), :] = block[at : at + 8]
        nat[b, 0:8, :] = nat[b, EXT : EXT + 8, :]
    total = nat[0, 7 : 7 + N, :] + nat[1, 8 : 8 + N, :] + nat[2, 9 : 9 + N, :]
    visc_out[...] = jnp.exp(total.T)
    for copy in stores:
        copy.wait()


PACK, CONT, MOM, OWN, SPREAD, QC, QM = 64, 32, 16, 32, 128, 144, 144


def step(state):
    vmem = pl.BlockSpec(memory_space=pltpu.VMEM)
    hbm = pl.BlockSpec(memory_space=HBM)
    whole = jax.ShapeDtypeStruct((LAYERS, N, N), F32)
    return pl.pallas_call(
        step_kernel,
        out_shape=(whole, whole, whole, jax.ShapeDtypeStruct((N, N), F32)),
        in_specs=[vmem] * 15,
        out_specs=[hbm] * 3 + [vmem],
        scratch_shapes=[
            pltpu.VMEM((2, FIELDS, EDGE, N), F32),
            pltpu.VMEM((2, LAYERS, EDGE, N), F32),
            pltpu.VMEM((2, LAYERS, EDGE, N), F32),
            pltpu.VMEM((2, LAYERS, EDGE, N), F32),
            pltpu.VMEM((2, LAYERS, EDGE, N), F32),
            pltpu.VMEM((2, 4, EDGE, N), F32),
            pltpu.VMEM((7, PAD, N), F32),
            pltpu.VMEM((PAD, N), F32),
            pltpu.VMEM((PAD, N), F32),
            pltpu.VMEM((PAD, N), F32),
            pltpu.VMEM((PAD, N), F32),
            pltpu.VMEM((4, TALL, N), F32),
            pltpu.VMEM((4, TALL, N), F32),
            pltpu.VMEM((9, EXT + 16, N), F32),
            pltpu.VMEM((LAYERS, N, N), F32),
            pltpu.VMEM((LAYERS, N, N), F32),
            pltpu.VMEM((LAYERS, N, N), F32),
            pltpu.VMEM((PAIRS // 2, 2, EXT + 32, N), BF16),
            pltpu.VMEM((BLOCK, 2 * N), F32),
            pltpu.VMEM((BLOCK, 2 * N), F32),
            pltpu.VMEM((33, 24, N), F32),
            pltpu.VMEM((33, 24, N), F32),
            pltpu.VMEM((3, EXT + 16, N), F32),
            pltpu.SemaphoreType.DMA((3,)),
        ],
        compiler_params=pltpu.CompilerParams(vmem_limit_bytes=24 * 2**20),
        name="step",
    )(*state)


def local(z, v, h, ls, vi, w, grav, conv1, bias1, conv2, bias2, conv3):
    conv1 = jnp.transpose(conv1, (0, 1, 3, 2))
    conv3 = jnp.transpose(conv3, (0, 2, 1, 3))
    held = [pltpu.with_memory_space_constraint(x, HBM) for x in (z, v, h, ls, vi, w, grav, conv1, conv2, conv3, bias1, bias2)]
    return step(exchange(held[:6], *held[6:]))


def solution(mesh):
    block, flat = P(None, "ox", "oy"), P("ox", "oy")
    return jax.shard_map(
        local,
        mesh=mesh,
        in_specs=(block, block, block, flat, flat, block) + (P(),) * 6,
        out_specs=(block, block, block, flat),
        check_vma=False,
    )
```

```python
import jax
import jax.numpy as jnp
from jax import lax
from jax.experimental import pallas as pl
from jax.experimental.pallas import tpu as pltpu
from jax.sharding import PartitionSpec as P

MESH = pl.DeviceIdType.MESH
F32 = jnp.float32
BF16 = jnp.bfloat16

DT = 0.05
REST = 1.4
DRAG = 0.5
LAYERS = 4
N = 128
HID = 64
FIELDS = 16
SEA, VISC, WIND = 12, 13, 14
EXT = N + 16
PAD = N + 32
TALL = N + 40
PAIRS = 72
GROUPS = 33
STEP = 3
TILES = EXT // 16
BLOCK = STEP * EXT


HBM = pltpu.HBM
EDGE = 32


def lanes(rows):
    return lax.broadcasted_iota(jnp.int32, (rows, N), 1)


def near(x):
    return pltpu.roll(x, N - 1, 1), pltpu.roll(x, 1, 1)


def shifted(start, size):
    aligned = start if isinstance(start, int) else pl.multiple_of(start, 8)
    return pl.ds(aligned, size), pl.ds(start + 1, size), pl.ds(start - 1, size)


def continuity(f, press, depth, grav, start, size):
    rows, up, down = shifted(start, size)
    sea = f[SEA, rows, :]
    anomaly = []
    for l in range(LAYERS):
        thick = f[8 + l, rows, :]
        fn, fs = near(f[4 + l, rows, :] * thick)
        fe = f[l, up, :] * f[8 + l, up, :]
        fw = f[l, down, :] * f[8 + l, down, :]
        diverge = (fe - fw) * 0.5 + (fn - fs) * 0.5
        new = thick - DT * sea * diverge
        depth[l, rows, :] = new
        anomaly.append(new - REST)
    faces = [anomaly[3]]
    for l in (2, 1, 0):
        faces.insert(0, faces[0] + anomaly[l])
    total = grav[0] * faces[0]
    press[0, rows, :] = total
    for l in range(1, LAYERS):
        total = total + grav[l] * faces[l]
        press[l, rows, :] = total


def coefficients(visc, up, down):
    return [0.5 * (visc + other) for other in (up, down, *near(visc))]


def viscous(coef, centre, up, down):
    total = None
    for c, q in zip(coef, (up, down, *near(centre))):
        term = c * (q - centre)
        total = term if total is None else total + term
    return total


def coriolis_of(lat, ny):
    return 0.3 + 1.4 * (lat.astype(F32) + 0.5) / (N * ny)


def momentum(f, press, depth, zo, vo, feature_refs, coriolis, start, size):
    rows, up, down = shifted(start, size)
    sea = f[SEA, rows, :]
    coef = coefficients(f[VISC, rows, :], f[VISC, up, :], f[VISC, down, :])
    kinetic = column = None
    for l in range(LAYERS):
        zc, vc = f[l, rows, :], f[4 + l, rows, :]
        pn, ps = near(press[l, rows, :])
        gx = (press[l, up, :] - press[l, down, :]) * 0.5
        gy = (pn - ps) * 0.5
        thick = depth[l, rows, :]
        fz = coriolis * vc - gx + viscous(coef, zc, f[l, up, :], f[l, down, :])
        fv = -coriolis * zc - gy + viscous(coef, vc, f[4 + l, up, :], f[4 + l, down, :])
        if l == 0:
            fz = fz + f[WIND, rows, :] / thick
            fv = fv + f[WIND + 1, rows, :] / thick
        if l == LAYERS - 1:
            fz = fz - DRAG * zc
            fv = fv - DRAG * vc
        z_new = sea * (zc + DT * fz)
        v_new = sea * (vc + DT * fv)
        zo[l, rows, :] = z_new
        vo[l, rows, :] = v_new
        part = thick * (z_new * z_new + v_new * v_new)
        kinetic = part if l == 0 else kinetic + part
        column = thick if l == 0 else column + thick
        if l == 0:
            feature_refs[0][0, rows, :] = z_new
            feature_refs[0][1, rows, :] = v_new
            feature_refs[0][2, rows, :] = sea * (thick - REST)
    feature_refs[0][3, rows, :] = sea * (0.5 * kinetic / column)


def own_pack(read, lane):
    packed = None
    for l in range(4):
        field = read(l)
        for at, shift in ((32 * l + 8, 32 * l + 8), (32 * l + 16, 32 * l + 16 + 8)):
            moved = pltpu.roll(field, shift % N, 1)
            packed = moved if packed is None else jnp.where((lane >= at) & (lane < at + 8), moved, packed)
    return packed


def exchange_kernel(
    z, v, h, ls, vi, w, grav_in, conv1, conv2, conv3, bias1, bias2,
    f0, p0, t0, zo, vo, fs, ft, own, ns, xw, xe, first_w, second_w, last_w, consts,
    sea_i, sb, nb, rows24, c1, c2, c3, grav, s1, s2, load_sem, send_sem, recv_sem,
):
    ox, oy = lax.axis_index("ox"), lax.axis_index("oy")
    nx, ny = lax.axis_size("ox"), lax.axis_size("oy")
    east, west = lax.rem(ox + 1, nx), lax.rem(ox + nx - 1, nx)
    above, below = lax.rem(oy + 1, ny), lax.rem(oy + ny - 1, ny)
    peers = (
        (east, oy), (west, oy),
        (ox, above), (east, above), (west, above),
        (ox, below), (east, below), (west, below),
    )
    barrier = pltpu.get_barrier_semaphore()
    has_north, has_south = oy < ny - 1, oy > 0

    def greet(first_peer, last_peer):
        for peer in peers[first_peer:last_peer]:
            pl.semaphore_signal(barrier, inc=1, device_id=peer, device_id_type=MESH)

    greet(0, 2)
    pl.when(has_north)(lambda: greet(2, 5))
    pl.when(has_south)(lambda: greet(5, 8))

    def load(at, size, sems):
        here, there = pl.ds(at, size), pl.ds(at + 16, size)
        pairs = (
            (ls.at[here], sea_i.at[here]),
            (z.at[:, here], f0.at[0:4, there]),
            (v.at[:, here], f0.at[4:8, there]),
            (h.at[:, here], f0.at[8:12, there]),
            (vi.at[here], f0.at[VISC, there]),
            (w.at[:, here], f0.at[WIND : WIND + 2, there]),
        )
        return [
            pltpu.make_async_copy(src, dst, load_sem.at[sems + k]) for k, (src, dst) in enumerate(pairs)
        ]

    ends = load(0, 8, 0) + load(N - 8, 8, 6)
    middle = load(8, N - 16, 12)
    rest = [
        pltpu.make_async_copy(src, dst, load_sem.at[18 + k])
        for k, (src, dst) in enumerate((
            (conv1, c1), (conv2, c2), (conv3, c3), (grav_in, grav), (bias1, s1), (bias2, s2),
        ))
    ]
    for copy in ends + middle + rest:
        copy.start()

    def pack(at, size):
        rows, src = pl.ds(at, size), pl.ds(at + 16, size)
        lane = lanes(size)
        sea = sea_i[rows, :].astype(F32)
        f0[SEA, src, :] = sea
        to_south = to_north = None
        for a in range(4):
            for l in range(4):
                field = sea if 4 * a + l == SEA else f0[4 * a + l, src, :]
                if a < 2:
                    field = field * sea
                    f0[4 * a + l, src, :] = field
                at_lane = 32 * l + 8 * a
                moved = pltpu.roll(field, at_lane, 1) if at_lane else field
                if to_south is None:
                    to_south = to_north = moved
                else:
                    to_south = jnp.where((lane >= at_lane) & (lane < at_lane + 8), moved, to_south)
                    to_north = jnp.where((lane >= at_lane - 8) & (lane < at_lane), moved, to_north)
        sb[rows, :] = to_south
        nb[rows, :] = to_north

    for copy in ends:
        copy.wait()
    pack(0, 8)
    pack(N - 8, 8)
    for copy in middle:
        copy.wait()
    pack(8, N - 16)
    pl.semaphore_wait(barrier, 2 + 3 * has_north.astype(jnp.int32) + 3 * has_south.astype(jnp.int32))

    first, last = pl.ds(0, 8), pl.ds(N - 8, 8)
    def move(k, src, dst, peer):
        return pltpu.make_async_remote_copy(
            src_ref=src, dst_ref=dst, send_sem=send_sem.at[k], recv_sem=recv_sem.at[k],
            device_id=peer, device_id_type=MESH,
        )

    along = (
        move(0, f0.at[:, N + 8 : N + 16], xw, (east, oy)),
        move(1, f0.at[:, 16:24], xe, (west, oy)),
    )
    northward = (
        move(2, nb.at[last], ns.at[1, 0:8], (east, above)),
        move(3, nb.at[first], ns.at[1, N + 8 : EXT], (west, above)),
        move(4, nb, ns.at[1, 8 : 8 + N], (ox, above)),
    )
    southward = (
        move(5, sb.at[last], ns.at[0, 0:8], (east, below)),
        move(6, sb.at[first], ns.at[0, N + 8 : EXT], (west, below)),
        move(7, sb, ns.at[0, 8 : 8 + N], (ox, below)),
    )

    def start(copies):
        for copy in copies:
            copy.start()

    pl.when(has_north)(lambda: start(northward[:2]))
    pl.when(has_south)(lambda: start(southward[:2]))
    pl.when(has_north)(lambda: start(northward[2:]))
    pl.when(has_south)(lambda: start(southward[2:]))
    start(along)

    @pl.when(jnp.logical_not(has_north))
    def _():
        ns[0] = jnp.ones((EXT, N), F32)

    @pl.when(jnp.logical_not(has_south))
    def _():
        ns[1] = jnp.ones((EXT, N), F32)

    ones = jnp.ones((8, N), F32)
    for rows in (pl.ds(8, 8), pl.ds(N + 16, 8)):
        for k in range(FIELDS):
            f0[k, rows, :] = ones
        for k in range(LAYERS):
            p0[k, rows, :] = ones
    for copy in rest:
        copy.wait()
    build_weights(c1, c2, c3, first_w, second_w, last_w, rows24)
    for l in range(LAYERS):
        consts[l : l + 1, :] = jnp.full((1, N), grav[l], F32)
    for k, bias in enumerate((s1, s2)):
        half = bias[...].reshape(1, HID) * 0.5
        consts[4 + k : 5 + k, :] = jnp.concatenate([half, half], axis=1)

    def inner_continuity(k, carry):
        continuity(f0, p0, t0, grav, CONT * k + 16, CONT)
        return carry

    lax.fori_loop(0, N // CONT, inner_continuity, 0)

    def inner_momentum(k, carry):
        coriolis = coriolis_of(oy * N + lanes(MOM), ny)
        momentum(f0, p0, t0, zo, vo, (fs,), coriolis, MOM * k + 16, MOM)
        return carry

    lax.fori_loop(0, N // MOM, inner_momentum, 0)

    def inner_pack(k, carry):
        src = pl.ds(pl.multiple_of(OWN * k + 16, 8), OWN)
        rows = pl.ds(pl.multiple_of(OWN * k, 8), OWN)
        for a in range(4):
            own[a, rows, :] = own_pack(lambda l: f0[4 * a + l, src, :], lanes(OWN))
        return carry

    lax.fori_loop(0, N // OWN, inner_pack, 0)

    def inner_turn(k, carry):
        rows = pl.ds(pl.multiple_of(16 * k + 24, 8), 32)
        ft[k] = fs[:, rows, :].reshape(N, N).T
        return carry

    lax.fori_loop(0, 6, inner_turn, 0)

    def sent(copies):
        for copy in copies:
            copy.wait_send()

    def received(copies):
        for copy in copies:
            copy.wait_recv()

    sent(along)
    pl.when(has_north)(lambda: sent(northward))
    pl.when(has_south)(lambda: sent(southward))
    received(along)
    pl.when(has_north)(lambda: received(southward))
    pl.when(has_south)(lambda: received(northward))


def exchange(fields, grav, conv1, conv2, conv3, bias1, bias2):
    hbm = pl.BlockSpec(memory_space=HBM)
    vmem = pl.BlockSpec(memory_space=pltpu.VMEM)

    def array(*shape, dtype=F32):
        return jax.ShapeDtypeStruct(shape, dtype)

    return pl.pallas_call(
        exchange_kernel,
        out_shape=(
            array(FIELDS, PAD, N), array(LAYERS, PAD, N), array(LAYERS, PAD, N),
            array(LAYERS, PAD, N), array(LAYERS, PAD, N), array(4, PAD, N),
            array(6, N, N), array(4, N, N), array(2, EXT, N),
            array(FIELDS, 8, N), array(FIELDS, 8, N),
            array(3 * N, 16 * HID, dtype=BF16), array(18 * HID, 4 * HID, dtype=BF16),
            array(32, 2 * N, dtype=BF16), array(8, N),
        ),
        in_specs=[hbm] * 12,
        out_specs=(vmem,) * 15,
        scratch_shapes=[
            pltpu.VMEM((N, N), jnp.int32),
            pltpu.VMEM((N, N), F32),
            pltpu.VMEM((N, N), F32),
            pltpu.VMEM((32, 2 * N), F32),
            pltpu.VMEM(conv1.shape, BF16),
            pltpu.VMEM(conv2.shape, BF16),
            pltpu.VMEM(conv3.shape, BF16),
            pltpu.SMEM((LAYERS,), F32),
            pltpu.VMEM((HID,), F32),
            pltpu.VMEM((HID,), F32),
            pltpu.SemaphoreType.DMA((24,)),
            pltpu.SemaphoreType.DMA((8,)),
            pltpu.SemaphoreType.DMA((8,)),
        ],
        compiler_params=pltpu.CompilerParams(
            collective_id=0, has_side_effects=True, vmem_limit_bytes=16 * 2**20
        ),
        name="exchange",
    )(*fields, grav, conv1, conv2, conv3, bias1, bias2)


def build_weights(conv1, conv2, conv3, first_w, second_w, last_w, rows24):
    lane = lax.broadcasted_iota(jnp.int32, (8, N), 1)
    right = lane >= HID
    row = lax.broadcasted_iota(jnp.int32, (8, N), 0)

    nt = (((1,), (1,)), ((), ()))
    taps = {}
    for a in range(3):
        for b in range(3):
            one = conv1[a, b].astype(F32) * 0.5
            taps[a, b] = jnp.concatenate([one, one], axis=1)
    for b in range(3):
        for c in range(4):
            vecs = [jnp.broadcast_to(taps[a, b][c : c + 1], (8, N)) for a in range(3)]
            for jp in range(8):
                parts = []
                for i in range(4):
                    gap = row + 8 * i - 2 * jp - jnp.where(right, 1, 0) - 4
                    val = jnp.zeros((8, N), F32)
                    for a in range(3):
                        val = jnp.where(gap == a, vecs[a], val)
                    parts.append(val)
                start = 128 * b + 32 * c
                first_w[start : start + 32, N * jp : N * jp + N] = jnp.concatenate(parts, 0).astype(BF16)

    eye = lax.broadcasted_iota(jnp.int32, (HID, HID), 0) == lax.broadcasted_iota(jnp.int32, (HID, HID), 1)
    eye = jnp.where(eye, 0.5, 0.0).astype(BF16)
    side = lax.broadcasted_iota(jnp.int32, (HID, N), 1) >= HID
    for b in range(3):
        turned = []
        for a in range(3):
            one = conv2[a, b]
            both = jnp.concatenate([one, one], axis=0)
            turned.append(lax.dot_general(eye, both, nt, preferred_element_type=F32))
        zero = jnp.zeros((HID, N), F32)
        for m in range(6):
            for jp in range(2):
                tap = m - 2 * jp
                left = turned[tap] if 0 <= tap < 3 else zero
                other = turned[tap - 1] if 0 <= tap - 1 < 3 else zero
                start = (6 * b + m) * HID
                second_w[start : start + HID, N * jp : N * jp + N] = jnp.where(side, other, left).astype(BF16)

    rows24[...] = jnp.zeros((32, 2 * N), F32)
    for b in range(3):
        for place, i in ((0, 3), (1, 4), (2, 5), (5, 0), (6, 1), (7, 2)):
            for m in range(4):
                a = m - i + 2
                if 0 <= a < 3:
                    rows24[8 * b + place : 8 * b + place + 1, HID * m : HID * m + HID] = conv3[a, 0, b : b + 1].astype(F32)
    last_w[...] = rows24[...].astype(BF16)


def step_kernel(
    f0, p0, t0, zo, vo, fs0, ft0, own, ns, xw, xe, first_w, second_w, last_w, consts,
    z_out, v_out, h_out, visc_out,
    fe, pe, te, ze, ve, fse, q, pq, hq, zq, vq, fsq, fs, ft, zm, vm, hm, h1, d0, d1, rs, re, nat,
    store_sem,
):
    oy, ny = lax.axis_index("oy"), lax.axis_size("oy")
    has_north = (oy < ny - 1).astype(F32)
    has_south = (oy > 0).astype(F32)
    ones = jnp.ones((8, N), F32)
    grav = [consts[l : l + 1, :] for l in range(LAYERS)]

    for e, (rows, src) in enumerate((((8, xw), (16, 16)), ((0, N), (16, xe)))):
        (halo_at, halo), (own_at, own_from) = (rows, src) if e == 0 else (src, rows)
        pad = 0 if e == 0 else 24
        for k in range(FIELDS):
            fe[e, k, halo_at : halo_at + 8, :] = halo[k]
            fe[e, k, own_at : own_at + 16, :] = f0[k, own_from : own_from + 16, :]
            fe[e, k, pad : pad + 8, :] = ones
        inner_at, inner_from = (24, 24) if e == 0 else (0, N)
        for k in range(LAYERS):
            pe[e, k, pad : pad + 8, :] = ones
            pe[e, k, inner_at : inner_at + 8, :] = p0[k, inner_from : inner_from + 8, :]
    for e in range(2):
        continuity(fe.at[e], pe.at[e], te.at[e], grav, 8, 16)
    for e in range(2):
        coriolis = coriolis_of(oy * N + lanes(16), ny)
        momentum(fe.at[e], pe.at[e], te.at[e], ze.at[e], ve.at[e], (fse.at[e],), coriolis, 8, 16)

    for k in range(7):
        q[k, 0:8, :] = ones
        q[k, PAD - 8 : PAD, :] = ones
    pq[0:8, :] = ones
    pq[PAD - 8 : PAD, :] = ones
    for c in range(4):
        fs[c, EXT + 8 : TALL, :] = jnp.zeros((TALL - EXT - 8, N), F32)
        fsq[c, EXT + 8 : TALL, :] = jnp.zeros((TALL - EXT - 8, N), F32)

    def spread(start, size, groups):
        lane = lanes(size)
        part = lax.rem(lane, 32)
        seg = lane // 32
        inside = jnp.where(part < 8, has_south, jnp.where(part < 24, 1.0, has_north))
        rows = pl.ds(start + 8 if isinstance(start, int) else pl.multiple_of(start + 8, 8), size)
        src = pl.ds(start if isinstance(start, int) else pl.multiple_of(start, 8), size)
        from_north, from_south = ns[0, src, :], ns[1, src, :]
        full = []
        for a in range(4):
            high = pltpu.roll(from_north, (24 - 8 * a) % N, 1)
            low = pltpu.roll(from_south, (8 - 8 * a) % N, 1)
            full.append(jnp.where(part < 8, low, jnp.where(part < 24, groups(a), high)))
        q[0, rows, :] = full[0] * inside
        q[1, rows, :] = full[1] * inside
        q[2, rows, :] = full[2]
        for k, s in ((3, 0), (4, 1)):
            one = jnp.where(seg == s, full[3] * inside, 0.0)
            one = one + pltpu.roll(one, 32, 1)
            q[k, rows, :] = one + pltpu.roll(one, 64, 1)
        for k, s in ((5, 2), (6, 3)):
            q[k, rows, :] = jnp.where(seg == 0, pltpu.roll(full[3], N - 32 * s, 1), 0.0)

    for at, strip in ((0, xw), (N + 8, xe)):
        spread(at, 8, lambda a: own_pack(lambda l: strip[4 * a + l], lanes(8)))

    def spread_body(k, carry):
        rows = pl.ds(pl.multiple_of(SPREAD * k, 8), SPREAD)
        spread(SPREAD * k + 8, SPREAD, lambda a: own[a, rows, :])
        return carry

    lax.fori_loop(0, N // SPREAD, spread_body, 0)

    def packed_continuity(k, carry):
        size = QC
        lane = lanes(size)
        part, seg = lax.rem(lane, 32), lane // 32
        inside = jnp.where(part < 8, has_south, jnp.where(part < 24, 1.0, has_north))
        weight = jnp.where(seg == 0, grav[0], jnp.where(seg == 1, grav[1], jnp.where(seg == 2, grav[2], grav[3])))
        rows, up, down = shifted(size * k + 8, size)
        thick = q[2, rows, :]
        fn, fs_ = near(q[1, rows, :] * thick)
        fe_ = q[0, up, :] * q[2, up, :]
        fw_ = q[0, down, :] * q[2, down, :]
        diverge = (fe_ - fw_) * 0.5 + (fn - fs_) * 0.5
        new = thick - DT * q[3, rows, :] * diverge
        hq[rows, :] = new
        a = new - REST
        face = a
        for n in (1, 2, 3):
            face = face + jnp.where(seg < 4 - n, pltpu.roll(a, N - 32 * n, 1), 0.0)
        term = weight * face
        total = term
        for n in (1, 2, 3):
            total = total + jnp.where(seg >= n, pltpu.roll(term, 32 * n, 1), 0.0)
        pq[rows, :] = total * inside
        return carry

    lax.fori_loop(0, EXT // QC, packed_continuity, 0)

    def packed_momentum(k, carry):
        size = QM
        lane = lanes(size)
        part, seg = lax.rem(lane, 32), lane // 32
        coriolis = coriolis_of(oy * N + part + jnp.where(part < 16, -8, 104), ny)
        drag = jnp.where(seg == 3, DRAG, 0.0)
        rows, up, down = shifted(size * k + 8, size)
        zc, vc, sea = q[0, rows, :], q[1, rows, :], q[3, rows, :]
        coef = coefficients(q[4, rows, :], q[4, up, :], q[4, down, :])
        pn, ps = near(pq[rows, :])
        gx = (pq[up, :] - pq[down, :]) * 0.5
        gy = (pn - ps) * 0.5
        thick = hq[rows, :]
        fz = coriolis * vc - gx + viscous(coef, zc, q[0, up, :], q[0, down, :])
        fv = -coriolis * zc - gy + viscous(coef, vc, q[1, up, :], q[1, down, :])
        fz = fz + q[5, rows, :] / thick - drag * zc
        fv = fv + q[6, rows, :] / thick - drag * vc
        z_new = sea * (zc + DT * fz)
        v_new = sea * (vc + DT * fv)
        zq[rows, :] = z_new
        vq[rows, :] = v_new
        sums = []
        for one in (thick * (z_new * z_new + v_new * v_new), thick):
            one = one + pltpu.roll(one, 64, 1)
            sums.append(one + pltpu.roll(one, 32, 1))
        fsq[0, rows, :] = z_new
        fsq[1, rows, :] = v_new
        fsq[2, rows, :] = sea * (thick - REST)
        fsq[3, rows, :] = sea * (0.5 * sums[0] / sums[1])
        return carry

    lax.fori_loop(0, EXT // QM, packed_momentum, 0)

    for c in range(4):
        fs[c, 8:24, :] = fse[0, c, 8:24, :]
        fs[c, 24:40, :] = fs0[c, 24:40, :]
        fs[c, N - 8 : N + 8, :] = fs0[c, N - 8 : N + 8, :]
        fs[c, N + 8 : N + 24, :] = fse[1, c, 8:24, :]

    row = lax.broadcasted_iota(jnp.int32, (8, N), 0)
    for k in range(9):
        if 1 <= k <= 6:
            inner = ft0[k - 1]
        else:
            inner = fs[:, 16 * k + 8 : 16 * k + 40, :].reshape(N, N).T
        ends = fsq[:, 16 * k + 8 : 16 * k + 40, :].reshape(N, N).T
        low = jnp.where(row < 4, ends[8:16], inner[0:8])
        high = jnp.where(row >= 4, ends[16:24], inner[N - 8 : N])
        ft[k, 0:8, :] = ends[0:8]
        ft[k, 8:16, :] = low
        ft[k, 16:N, :] = inner[8 : N - 8]
        ft[k, N : N + 8, :] = high
        ft[k, N + 8 : N + 16, :] = ends[24:32]
        ft[k, N + 16 : N + 24, :] = ends[0:8]
        ft[k, N + 24 : N + 32, :] = low

    def merge(size, rows, packed_rows, sources):
        lane = lanes(size)
        for packed, out, read in sources:
            whole = packed[packed_rows, :]
            for l in range(LAYERS):
                low = pltpu.roll(whole, (N - 32 * l - 8) % N, 1)
                high = pltpu.roll(whole, (104 - 32 * l) % N, 1)
                out[l, rows, :] = jnp.where(lane < 4, low, jnp.where(lane >= N - 4, high, read(l)))

    order = lax.broadcasted_iota(jnp.int32, (EXT, 2 * N), 0)
    lat = 9 * lax.rem(order, 16) + order // 16
    keep = jnp.where(lat < N, 1.0, jnp.where(lat < N + 8, has_north, has_south)) > 0.5
    b1 = jnp.concatenate([consts[4:5, :]] * 2, axis=1)
    b2 = jnp.concatenate([consts[5:6, :]] * 2, axis=1)

    def activate(x, bias):
        x = x + bias
        return jnp.where(keep, x + x * jnp.tanh(x), 0.0)

    def first_layer(k, quarters):
        parts = []
        for b in range(3):
            pieces = []
            for t in range(TILES):
                for half in range(2):
                    pieces.append(ft[k, pl.ds(7 + t + b + 72 * half, 8, stride=9), :])
            parts.append(jnp.concatenate(pieces, axis=0).astype(BF16))
        left = jnp.concatenate(parts, axis=1)
        for quarter in range(quarters):
            out = jnp.dot(left, first_w[:, 256 * quarter : 256 * quarter + 256], preferred_element_type=F32)
            out = activate(out, b1)
            at = 4 * k + quarter
            for p in range(2):
                one = out[:, N * p : N * p + N]
                h1[at, p, 16 : 16 + EXT, :] = one.astype(BF16)
                h1[at, p, 0:16, :] = pltpu.roll(one[EXT - 16 : EXT], 1, 0).astype(BF16)
                h1[at, p, 16 + EXT : 32 + EXT, :] = pltpu.roll(one[0:16], 15, 0).astype(BF16)

    def first_body(k, carry):
        first_layer(k, 4)
        rows = pl.ds(pl.multiple_of(16 * k + 8, 8), 16)
        wide = pl.ds(pl.multiple_of(16 * k + 24, 8), 16)
        merge(16, rows, wide, (
            (zq, zm, lambda l: zo[l, wide, :]),
            (vq, vm, lambda l: vo[l, wide, :]),
            (hq, hm, lambda l: t0[l, wide, :]),
        ))
        return carry

    for k in range(7):
        first_body(k, 0)
    for e, (at, inner) in enumerate(((0, 16), (N - 8, 8))):
        merge(8, pl.ds(at, 8), pl.ds(at + 16, 8), (
            (zq, zm, lambda l: ze[e, l, inner : inner + 8, :]),
            (vq, vm, lambda l: ve[e, l, inner : inner + 8, :]),
            (hq, hm, lambda l: te[e, l, inner : inner + 8, :]),
        ))
    first_layer(7, 4)
    first_layer(8, 2)
    stores = [
        pltpu.make_async_copy(src, dst, store_sem.at[k])
        for k, (src, dst) in enumerate(((zm, z_out), (vm, v_out), (hm, h_out)))
    ]
    for copy in stores:
        copy.start()

    def second_matmul(k, ref):
        g = k * STEP
        parts = []
        for b in range(3):
            for d in range(3):
                block = h1[pl.ds(g + d // 2, STEP), d % 2, 16 * b : 16 * b + EXT, :]
                parts.append(block.reshape(BLOCK, N))
        left = jnp.concatenate(parts, axis=1)
        ref[...] = jnp.dot(left, second_w[...], preferred_element_type=F32)

    def finish(k, ref):
        for i in range(STEP):
            one = activate(ref[i * EXT : (i + 1) * EXT], b2).astype(BF16)
            sums = lax.dot_general(
                last_w[...], one, (((1,), (1,)), ((), ())), preferred_element_type=F32
            )
            rs[k * STEP + i] = sums[0:24, 0:N]
            re[k * STEP + i, :, 0:16] = sums[0:24, N:EXT]

    held = (d0, d1)
    for k in range(11):
        second_matmul(k, held[k % 2])
        if k:
            finish(k - 1, held[(k - 1) % 2])
    finish(10, held[10 % 2])

    upper = lax.broadcasted_iota(jnp.int32, (8, N), 0) < 4
    for b in range(3):
        blocks = []
        for ref in (rs, re):
            rows = []
            for k in range(N // 8):
                x, y, zz = (ref[2 * k + i, 8 * b : 8 * b + 8, :] for i in range(3))
                y = pltpu.roll(y, 4, 0)
                rows.append(jnp.where(upper, x, y) + jnp.where(upper, y, zz))
            blocks.append(jnp.concatenate(rows, axis=0).T)
        for t in range(TILES):
            for half in range(2):
                block, at = (blocks[0], 16 * t) if t < 8 else (blocks[1], 0)
                at = at + 8 * half
                nat[b, pl.ds(8 + t + 72 * half, 8, stride=9), :] = block[at : at + 8]
        nat[b, 0:8, :] = nat[b, EXT : EXT + 8, :]
    total = nat[0, 7 : 7 + N, :] + nat[1, 8 : 8 + N, :] + nat[2, 9 : 9 + N, :]
    visc_out[...] = jnp.exp(total.T)
    for copy in stores:
        copy.wait()


CONT, MOM, OWN, SPREAD, QC, QM = 32, 16, 32, 128, 144, 144


def step(state):
    vmem = pl.BlockSpec(memory_space=pltpu.VMEM)
    hbm = pl.BlockSpec(memory_space=HBM)
    whole = jax.ShapeDtypeStruct((LAYERS, N, N), F32)
    return pl.pallas_call(
        step_kernel,
        out_shape=(whole, whole, whole, jax.ShapeDtypeStruct((N, N), F32)),
        in_specs=[vmem] * 15,
        out_specs=[hbm] * 3 + [vmem],
        scratch_shapes=[
            pltpu.VMEM((2, FIELDS, EDGE, N), F32),
            pltpu.VMEM((2, LAYERS, EDGE, N), F32),
            pltpu.VMEM((2, LAYERS, EDGE, N), F32),
            pltpu.VMEM((2, LAYERS, EDGE, N), F32),
            pltpu.VMEM((2, LAYERS, EDGE, N), F32),
            pltpu.VMEM((2, 4, EDGE, N), F32),
            pltpu.VMEM((7, PAD, N), F32),
            pltpu.VMEM((PAD, N), F32),
            pltpu.VMEM((PAD, N), F32),
            pltpu.VMEM((PAD, N), F32),
            pltpu.VMEM((PAD, N), F32),
            pltpu.VMEM((4, TALL, N), F32),
            pltpu.VMEM((4, TALL, N), F32),
            pltpu.VMEM((9, EXT + 16, N), F32),
            pltpu.VMEM((LAYERS, N, N), F32),
            pltpu.VMEM((LAYERS, N, N), F32),
            pltpu.VMEM((LAYERS, N, N), F32),
            pltpu.VMEM((PAIRS // 2, 2, EXT + 32, N), BF16),
            pltpu.VMEM((BLOCK, 2 * N), F32),
            pltpu.VMEM((BLOCK, 2 * N), F32),
            pltpu.VMEM((33, 24, N), F32),
            pltpu.VMEM((33, 24, N), F32),
            pltpu.VMEM((3, EXT + 16, N), F32),
            pltpu.SemaphoreType.DMA((3,)),
        ],
        compiler_params=pltpu.CompilerParams(vmem_limit_bytes=24 * 2**20),
        name="step",
    )(*state)


def local(z, v, h, ls, vi, w, grav, conv1, bias1, conv2, bias2, conv3):
    conv1 = jnp.transpose(conv1, (0, 1, 3, 2))
    conv3 = jnp.transpose(conv3, (0, 2, 1, 3))
    held = [pltpu.with_memory_space_constraint(x, HBM) for x in (z, v, h, ls, vi, w, grav, conv1, conv2, conv3, bias1, bias2)]
    return step(exchange(held[:6], *held[6:]))


def solution(mesh):
    block, flat = P(None, "ox", "oy"), P("ox", "oy")
    return jax.shard_map(
        local,
        mesh=mesh,
        in_specs=(block, block, block, flat, flat, block) + (P(),) * 6,
        out_specs=(block, block, block, flat),
        check_vma=False,
    )
```

```python
import jax
import jax.numpy as jnp
from jax import lax
from jax.experimental import pallas as pl
from jax.experimental.pallas import tpu as pltpu
from jax.sharding import PartitionSpec as P

MESH = pl.DeviceIdType.MESH
F32 = jnp.float32
BF16 = jnp.bfloat16

DT = 0.05
REST = 1.4
DRAG = 0.5
LAYERS = 4
N = 128
HID = 64
FIELDS = 16
SEA, VISC, WIND = 12, 13, 14
EXT = N + 16
PAD = N + 32
TALL = N + 40
PAIRS = 72
GROUPS = 33
STEP = 3
TILES = EXT // 16
BLOCK = STEP * EXT


HBM = pltpu.HBM
EDGE = 32


def lanes(rows):
    return lax.broadcasted_iota(jnp.int32, (rows, N), 1)


def near(x):
    return pltpu.roll(x, N - 1, 1), pltpu.roll(x, 1, 1)


def shifted(start, size):
    aligned = start if isinstance(start, int) else pl.multiple_of(start, 8)
    return pl.ds(aligned, size), pl.ds(start + 1, size), pl.ds(start - 1, size)


def continuity(f, press, depth, grav, start, size):
    rows, up, down = shifted(start, size)
    sea = f[SEA, rows, :]
    anomaly = []
    for l in range(LAYERS):
        thick = f[8 + l, rows, :]
        fn, fs = near(f[4 + l, rows, :] * thick)
        fe = f[l, up, :] * f[8 + l, up, :]
        fw = f[l, down, :] * f[8 + l, down, :]
        diverge = (fe - fw) * 0.5 + (fn - fs) * 0.5
        new = thick - DT * sea * diverge
        depth[l, rows, :] = new
        anomaly.append(new - REST)
    faces = [anomaly[3]]
    for l in (2, 1, 0):
        faces.insert(0, faces[0] + anomaly[l])
    total = grav[0] * faces[0]
    press[0, rows, :] = total
    for l in range(1, LAYERS):
        total = total + grav[l] * faces[l]
        press[l, rows, :] = total


def coefficients(visc, up, down):
    return [0.5 * (visc + other) for other in (up, down, *near(visc))]


def viscous(coef, centre, up, down):
    total = None
    for c, q in zip(coef, (up, down, *near(centre))):
        term = c * (q - centre)
        total = term if total is None else total + term
    return total


def coriolis_of(lat, ny):
    return 0.3 + 1.4 * (lat.astype(F32) + 0.5) / (N * ny)


def momentum(f, press, depth, zo, vo, feature_refs, coriolis, start, size):
    rows, up, down = shifted(start, size)
    sea = f[SEA, rows, :]
    coef = coefficients(f[VISC, rows, :], f[VISC, up, :], f[VISC, down, :])
    kinetic = column = None
    for l in range(LAYERS):
        zc, vc = f[l, rows, :], f[4 + l, rows, :]
        pn, ps = near(press[l, rows, :])
        gx = (press[l, up, :] - press[l, down, :]) * 0.5
        gy = (pn - ps) * 0.5
        thick = depth[l, rows, :]
        fz = coriolis * vc - gx + viscous(coef, zc, f[l, up, :], f[l, down, :])
        fv = -coriolis * zc - gy + viscous(coef, vc, f[4 + l, up, :], f[4 + l, down, :])
        if l == 0:
            fz = fz + f[WIND, rows, :] / thick
            fv = fv + f[WIND + 1, rows, :] / thick
        if l == LAYERS - 1:
            fz = fz - DRAG * zc
            fv = fv - DRAG * vc
        z_new = sea * (zc + DT * fz)
        v_new = sea * (vc + DT * fv)
        zo[l, rows, :] = z_new
        vo[l, rows, :] = v_new
        part = thick * (z_new * z_new + v_new * v_new)
        kinetic = part if l == 0 else kinetic + part
        column = thick if l == 0 else column + thick
        if l == 0:
            feature_refs[0][0, rows, :] = z_new
            feature_refs[0][1, rows, :] = v_new
            feature_refs[0][2, rows, :] = sea * (thick - REST)
    feature_refs[0][3, rows, :] = sea * (0.5 * kinetic / column)


def own_pack(read, lane):
    packed = None
    for l in range(4):
        field = read(l)
        for at, shift in ((32 * l + 8, 32 * l + 8), (32 * l + 16, 32 * l + 16 + 8)):
            moved = pltpu.roll(field, shift % N, 1)
            packed = moved if packed is None else jnp.where((lane >= at) & (lane < at + 8), moved, packed)
    return packed


def exchange_kernel(
    z, v, h, ls, vi, w, grav_in, conv1, conv2, conv3, bias1, bias2,
    f0, p0, t0, zo, vo, fs, ft, own, ns, xw, xe, first_w, second_w, last_w, consts,
    sea_i, sb, nb, rows24, c1, c2, c3, grav, s1, s2, load_sem, send_sem, recv_sem,
):
    ox, oy = lax.axis_index("ox"), lax.axis_index("oy")
    nx, ny = lax.axis_size("ox"), lax.axis_size("oy")
    east, west = lax.rem(ox + 1, nx), lax.rem(ox + nx - 1, nx)
    above, below = lax.rem(oy + 1, ny), lax.rem(oy + ny - 1, ny)
    peers = (
        (east, oy), (west, oy),
        (ox, above), (east, above), (west, above),
        (ox, below), (east, below), (west, below),
    )
    barrier = pltpu.get_barrier_semaphore()
    has_north, has_south = oy < ny - 1, oy > 0

    def greet(first_peer, last_peer):
        for peer in peers[first_peer:last_peer]:
            pl.semaphore_signal(barrier, inc=1, device_id=peer, device_id_type=MESH)

    greet(0, 2)
    pl.when(has_north)(lambda: greet(2, 5))
    pl.when(has_south)(lambda: greet(5, 8))

    def load(at, size, sems):
        here, there = pl.ds(at, size), pl.ds(at + 16, size)
        pairs = (
            (ls.at[here], sea_i.at[here]),
            (z.at[:, here], f0.at[0:4, there]),
            (v.at[:, here], f0.at[4:8, there]),
            (h.at[:, here], f0.at[8:12, there]),
            (vi.at[here], f0.at[VISC, there]),
            (w.at[:, here], f0.at[WIND : WIND + 2, there]),
        )
        return [
            pltpu.make_async_copy(src, dst, load_sem.at[sems + k]) for k, (src, dst) in enumerate(pairs)
        ]

    ends = load(0, 8, 0) + load(N - 8, 8, 6)
    middle = load(8, N - 16, 12)
    rest = [
        pltpu.make_async_copy(src, dst, load_sem.at[18 + k])
        for k, (src, dst) in enumerate((
            (conv1, c1), (conv2, c2), (conv3, c3), (grav_in, grav), (bias1, s1), (bias2, s2),
        ))
    ]
    for copy in ends + middle + rest:
        copy.start()

    def pack(at, size):
        rows, src = pl.ds(at, size), pl.ds(at + 16, size)
        lane = lanes(size)
        sea = sea_i[rows, :].astype(F32)
        f0[SEA, src, :] = sea
        to_south = to_north = None
        for a in range(4):
            for l in range(4):
                field = sea if 4 * a + l == SEA else f0[4 * a + l, src, :]
                if a < 2:
                    field = field * sea
                    f0[4 * a + l, src, :] = field
                at_lane = 32 * l + 8 * a
                moved = pltpu.roll(field, at_lane, 1) if at_lane else field
                if to_south is None:
                    to_south = to_north = moved
                else:
                    to_south = jnp.where((lane >= at_lane) & (lane < at_lane + 8), moved, to_south)
                    to_north = jnp.where((lane >= at_lane - 8) & (lane < at_lane), moved, to_north)
        sb[rows, :] = to_south
        nb[rows, :] = to_north

    for copy in ends:
        copy.wait()
    pack(0, 8)
    pack(N - 8, 8)
    for copy in middle:
        copy.wait()
    pack(8, N - 16)
    pl.semaphore_wait(barrier, 2 + 3 * has_north.astype(jnp.int32) + 3 * has_south.astype(jnp.int32))

    first, last = pl.ds(0, 8), pl.ds(N - 8, 8)
    def move(k, src, dst, peer):
        return pltpu.make_async_remote_copy(
            src_ref=src, dst_ref=dst, send_sem=send_sem.at[k], recv_sem=recv_sem.at[k],
            device_id=peer, device_id_type=MESH,
        )

    along = (
        move(0, f0.at[:, N + 8 : N + 16], xw, (east, oy)),
        move(1, f0.at[:, 16:24], xe, (west, oy)),
    )
    northward = (
        move(2, nb.at[last], ns.at[1, 0:8], (east, above)),
        move(3, nb.at[first], ns.at[1, N + 8 : EXT], (west, above)),
        move(4, nb, ns.at[1, 8 : 8 + N], (ox, above)),
    )
    southward = (
        move(5, sb.at[last], ns.at[0, 0:8], (east, below)),
        move(6, sb.at[first], ns.at[0, N + 8 : EXT], (west, below)),
        move(7, sb, ns.at[0, 8 : 8 + N], (ox, below)),
    )

    def start(copies):
        for copy in copies:
            copy.start()

    pl.when(has_north)(lambda: start(northward[:2]))
    pl.when(has_south)(lambda: start(southward[:2]))
    pl.when(has_north)(lambda: start(northward[2:]))
    pl.when(has_south)(lambda: start(southward[2:]))
    start(along)

    @pl.when(jnp.logical_not(has_north))
    def _():
        ns[0] = jnp.ones((EXT, N), F32)

    @pl.when(jnp.logical_not(has_south))
    def _():
        ns[1] = jnp.ones((EXT, N), F32)

    ones = jnp.ones((8, N), F32)
    for rows in (pl.ds(8, 8), pl.ds(N + 16, 8)):
        for k in range(FIELDS):
            f0[k, rows, :] = ones
        for k in range(LAYERS):
            p0[k, rows, :] = ones
    for copy in rest:
        copy.wait()
    build_weights(c1, c2, c3, first_w, second_w, last_w, rows24)
    for l in range(LAYERS):
        consts[l : l + 1, :] = jnp.full((1, N), grav[l], F32)
    for k, bias in enumerate((s1, s2)):
        half = bias[...].reshape(1, HID) * 0.5
        consts[4 + k : 5 + k, :] = jnp.concatenate([half, half], axis=1)

    def inner_continuity(k, carry):
        continuity(f0, p0, t0, grav, CONT * k + 16, CONT)
        return carry

    lax.fori_loop(0, N // CONT, inner_continuity, 0)

    def inner_momentum(k, carry):
        coriolis = coriolis_of(oy * N + lanes(MOM), ny)
        momentum(f0, p0, t0, zo, vo, (fs,), coriolis, MOM * k + 16, MOM)
        return carry

    lax.fori_loop(0, N // MOM, inner_momentum, 0)

    def inner_pack(k, carry):
        src = pl.ds(pl.multiple_of(OWN * k + 16, 8), OWN)
        rows = pl.ds(pl.multiple_of(OWN * k, 8), OWN)
        for a in range(4):
            own[a, rows, :] = own_pack(lambda l: f0[4 * a + l, src, :], lanes(OWN))
        return carry

    lax.fori_loop(0, N // OWN, inner_pack, 0)

    def inner_turn(k, carry):
        block = fs[:, pl.ds(pl.multiple_of(8 * k + 24, 8), 16), :].reshape(HID, N)
        ft[k] = jnp.concatenate([block, block], axis=0).T
        return carry

    lax.fori_loop(0, 13, inner_turn, 0)

    def sent(copies):
        for copy in copies:
            copy.wait_send()

    def received(copies):
        for copy in copies:
            copy.wait_recv()

    sent(along)
    pl.when(has_north)(lambda: sent(northward))
    pl.when(has_south)(lambda: sent(southward))
    received(along)
    pl.when(has_north)(lambda: received(southward))
    pl.when(has_south)(lambda: received(northward))


def exchange(fields, grav, conv1, conv2, conv3, bias1, bias2):
    hbm = pl.BlockSpec(memory_space=HBM)
    vmem = pl.BlockSpec(memory_space=pltpu.VMEM)

    def array(*shape, dtype=F32):
        return jax.ShapeDtypeStruct(shape, dtype)

    return pl.pallas_call(
        exchange_kernel,
        out_shape=(
            array(FIELDS, PAD, N), array(LAYERS, PAD, N), array(LAYERS, PAD, N),
            array(LAYERS, PAD, N), array(LAYERS, PAD, N), array(4, PAD, N),
            array(13, N, N), array(4, N, N), array(2, EXT, N),
            array(FIELDS, 8, N), array(FIELDS, 8, N),
            array(2 * N, 8 * HID, dtype=BF16), array(18 * HID, 4 * HID, dtype=BF16),
            array(32, 2 * N, dtype=BF16), array(8, N),
        ),
        in_specs=[hbm] * 12,
        out_specs=(vmem,) * 15,
        scratch_shapes=[
            pltpu.VMEM((N, N), jnp.int32),
            pltpu.VMEM((N, N), F32),
            pltpu.VMEM((N, N), F32),
            pltpu.VMEM((32, 2 * N), F32),
            pltpu.VMEM(conv1.shape, BF16),
            pltpu.VMEM(conv2.shape, BF16),
            pltpu.VMEM(conv3.shape, BF16),
            pltpu.SMEM((LAYERS,), F32),
            pltpu.VMEM((HID,), F32),
            pltpu.VMEM((HID,), F32),
            pltpu.SemaphoreType.DMA((24,)),
            pltpu.SemaphoreType.DMA((8,)),
            pltpu.SemaphoreType.DMA((8,)),
        ],
        compiler_params=pltpu.CompilerParams(
            collective_id=0, has_side_effects=True, vmem_limit_bytes=16 * 2**20
        ),
        name="exchange",
    )(*fields, grav, conv1, conv2, conv3, bias1, bias2)


def build_weights(conv1, conv2, conv3, first_w, second_w, last_w, rows24):
    lane = lax.broadcasted_iota(jnp.int32, (8, N), 1)
    right = lane >= HID
    row = lax.broadcasted_iota(jnp.int32, (8, N), 0)

    nt = (((1,), (1,)), ((), ()))
    taps = {}
    for a in range(3):
        for b in range(3):
            one = conv1[a, b].astype(F32) * 0.5
            taps[a, b] = jnp.concatenate([one, one], axis=1)
    for b in range(3):
        for c in range(4):
            vecs = [jnp.broadcast_to(taps[a, b][c : c + 1], (8, N)) for a in range(3)]
            for jp in range(4):
                parts = []
                for i in range(2):
                    gap = row + 8 * i - 2 * jp - jnp.where(right, 1, 0) - 4
                    val = jnp.zeros((8, N), F32)
                    for a in range(3):
                        val = jnp.where(gap == a, vecs[a], val)
                    parts.append(val)
                start = 64 * b + 16 * c
                first_w[start : start + 16, N * jp : N * jp + N] = jnp.concatenate(parts, 0).astype(BF16)
    first_w[192:256, :] = jnp.zeros((64, 8 * HID), BF16)

    eye = lax.broadcasted_iota(jnp.int32, (HID, HID), 0) == lax.broadcasted_iota(jnp.int32, (HID, HID), 1)
    eye = jnp.where(eye, 0.5, 0.0).astype(BF16)
    side = lax.broadcasted_iota(jnp.int32, (HID, N), 1) >= HID
    for b in range(3):
        turned = []
        for a in range(3):
            one = conv2[a, b]
            both = jnp.concatenate([one, one], axis=0)
            turned.append(lax.dot_general(eye, both, nt, preferred_element_type=F32))
        zero = jnp.zeros((HID, N), F32)
        for m in range(6):
            for jp in range(2):
                tap = m - 2 * jp
                left = turned[tap] if 0 <= tap < 3 else zero
                other = turned[tap - 1] if 0 <= tap - 1 < 3 else zero
                start = (6 * b + m) * HID
                second_w[start : start + HID, N * jp : N * jp + N] = jnp.where(side, other, left).astype(BF16)

    rows24[...] = jnp.zeros((32, 2 * N), F32)
    for b in range(3):
        for place, i in ((0, 3), (1, 4), (2, 5), (5, 0), (6, 1), (7, 2)):
            for m in range(4):
                a = m - i + 2
                if 0 <= a < 3:
                    rows24[8 * b + place : 8 * b + place + 1, HID * m : HID * m + HID] = conv3[a, 0, b : b + 1].astype(F32)
    last_w[...] = rows24[...].astype(BF16)


def step_kernel(
    f0, p0, t0, zo, vo, fs0, ft0, own, ns, xw, xe, first_w, second_w, last_w, consts,
    z_out, v_out, h_out, visc_out,
    fe, pe, te, ze, ve, fse, q, pq, hq, zq, vq, fsq, fs, ft, zm, vm, hm, h1, d0, d1, rs, re, nat,
    store_sem,
):
    oy, ny = lax.axis_index("oy"), lax.axis_size("oy")
    has_north = (oy < ny - 1).astype(F32)
    has_south = (oy > 0).astype(F32)
    ones = jnp.ones((8, N), F32)
    grav = [consts[l : l + 1, :] for l in range(LAYERS)]

    for e, (rows, src) in enumerate((((8, xw), (16, 16)), ((0, N), (16, xe)))):
        (halo_at, halo), (own_at, own_from) = (rows, src) if e == 0 else (src, rows)
        pad = 0 if e == 0 else 24
        for k in range(FIELDS):
            fe[e, k, halo_at : halo_at + 8, :] = halo[k]
            fe[e, k, own_at : own_at + 16, :] = f0[k, own_from : own_from + 16, :]
            fe[e, k, pad : pad + 8, :] = ones
        inner_at, inner_from = (24, 24) if e == 0 else (0, N)
        for k in range(LAYERS):
            pe[e, k, pad : pad + 8, :] = ones
            pe[e, k, inner_at : inner_at + 8, :] = p0[k, inner_from : inner_from + 8, :]
    for e in range(2):
        continuity(fe.at[e], pe.at[e], te.at[e], grav, 8, 16)
    for e in range(2):
        coriolis = coriolis_of(oy * N + lanes(16), ny)
        momentum(fe.at[e], pe.at[e], te.at[e], ze.at[e], ve.at[e], (fse.at[e],), coriolis, 8, 16)

    for k in range(7):
        q[k, 0:8, :] = ones
        q[k, PAD - 8 : PAD, :] = ones
    pq[0:8, :] = ones
    pq[PAD - 8 : PAD, :] = ones
    for c in range(4):
        fs[c, EXT + 8 : TALL, :] = jnp.zeros((TALL - EXT - 8, N), F32)
        fsq[c, EXT + 8 : TALL, :] = jnp.zeros((TALL - EXT - 8, N), F32)

    def spread(start, size, groups):
        lane = lanes(size)
        part = lax.rem(lane, 32)
        seg = lane // 32
        inside = jnp.where(part < 8, has_south, jnp.where(part < 24, 1.0, has_north))
        rows = pl.ds(start + 8 if isinstance(start, int) else pl.multiple_of(start + 8, 8), size)
        src = pl.ds(start if isinstance(start, int) else pl.multiple_of(start, 8), size)
        from_north, from_south = ns[0, src, :], ns[1, src, :]
        full = []
        for a in range(4):
            high = pltpu.roll(from_north, (24 - 8 * a) % N, 1)
            low = pltpu.roll(from_south, (8 - 8 * a) % N, 1)
            full.append(jnp.where(part < 8, low, jnp.where(part < 24, groups(a), high)))
        q[0, rows, :] = full[0] * inside
        q[1, rows, :] = full[1] * inside
        q[2, rows, :] = full[2]
        for k, s in ((3, 0), (4, 1)):
            one = jnp.where(seg == s, full[3] * inside, 0.0)
            one = one + pltpu.roll(one, 32, 1)
            q[k, rows, :] = one + pltpu.roll(one, 64, 1)
        for k, s in ((5, 2), (6, 3)):
            q[k, rows, :] = jnp.where(seg == 0, pltpu.roll(full[3], N - 32 * s, 1), 0.0)

    for at, strip in ((0, xw), (N + 8, xe)):
        spread(at, 8, lambda a: own_pack(lambda l: strip[4 * a + l], lanes(8)))

    def spread_body(k, carry):
        rows = pl.ds(pl.multiple_of(SPREAD * k, 8), SPREAD)
        spread(SPREAD * k + 8, SPREAD, lambda a: own[a, rows, :])
        return carry

    lax.fori_loop(0, N // SPREAD, spread_body, 0)

    def packed_continuity(k, carry):
        size = QC
        lane = lanes(size)
        part, seg = lax.rem(lane, 32), lane // 32
        inside = jnp.where(part < 8, has_south, jnp.where(part < 24, 1.0, has_north))
        weight = jnp.where(seg == 0, grav[0], jnp.where(seg == 1, grav[1], jnp.where(seg == 2, grav[2], grav[3])))
        rows, up, down = shifted(size * k + 8, size)
        thick = q[2, rows, :]
        fn, fs_ = near(q[1, rows, :] * thick)
        fe_ = q[0, up, :] * q[2, up, :]
        fw_ = q[0, down, :] * q[2, down, :]
        diverge = (fe_ - fw_) * 0.5 + (fn - fs_) * 0.5
        new = thick - DT * q[3, rows, :] * diverge
        hq[rows, :] = new
        a = new - REST
        face = a
        for n in (1, 2, 3):
            face = face + jnp.where(seg < 4 - n, pltpu.roll(a, N - 32 * n, 1), 0.0)
        term = weight * face
        total = term
        for n in (1, 2, 3):
            total = total + jnp.where(seg >= n, pltpu.roll(term, 32 * n, 1), 0.0)
        pq[rows, :] = total * inside
        return carry

    lax.fori_loop(0, EXT // QC, packed_continuity, 0)

    def packed_momentum(k, carry):
        size = QM
        lane = lanes(size)
        part, seg = lax.rem(lane, 32), lane // 32
        coriolis = coriolis_of(oy * N + part + jnp.where(part < 16, -8, 104), ny)
        drag = jnp.where(seg == 3, DRAG, 0.0)
        rows, up, down = shifted(size * k + 8, size)
        zc, vc, sea = q[0, rows, :], q[1, rows, :], q[3, rows, :]
        coef = coefficients(q[4, rows, :], q[4, up, :], q[4, down, :])
        pn, ps = near(pq[rows, :])
        gx = (pq[up, :] - pq[down, :]) * 0.5
        gy = (pn - ps) * 0.5
        thick = hq[rows, :]
        fz = coriolis * vc - gx + viscous(coef, zc, q[0, up, :], q[0, down, :])
        fv = -coriolis * zc - gy + viscous(coef, vc, q[1, up, :], q[1, down, :])
        fz = fz + q[5, rows, :] / thick - drag * zc
        fv = fv + q[6, rows, :] / thick - drag * vc
        z_new = sea * (zc + DT * fz)
        v_new = sea * (vc + DT * fv)
        zq[rows, :] = z_new
        vq[rows, :] = v_new
        sums = []
        for one in (thick * (z_new * z_new + v_new * v_new), thick):
            one = one + pltpu.roll(one, 64, 1)
            sums.append(one + pltpu.roll(one, 32, 1))
        fsq[0, rows, :] = z_new
        fsq[1, rows, :] = v_new
        fsq[2, rows, :] = sea * (thick - REST)
        fsq[3, rows, :] = sea * (0.5 * sums[0] / sums[1])
        return carry

    lax.fori_loop(0, EXT // QM, packed_momentum, 0)

    for c in range(4):
        fs[c, 8:24, :] = fse[0, c, 8:24, :]
        fs[c, 24:40, :] = fs0[c, 24:40, :]
        fs[c, N - 8 : N + 8, :] = fs0[c, N - 8 : N + 8, :]
        fs[c, N + 8 : N + 24, :] = fse[1, c, 8:24, :]

    row = lax.broadcasted_iota(jnp.int32, (8, N), 0)
    own_tap = lax.broadcasted_iota(jnp.int32, (EXT + 16, N), 1) < HID

    def turned(ref, k):
        block = ref[:, 8 * k + 8 : 8 * k + 24, :].reshape(HID, N)
        return jnp.concatenate([block, block], axis=0).T

    for k in range(17):
        inner = ft0[k - 2] if 2 <= k <= 14 else turned(fs, k)
        ends = turned(fsq, k)
        low = jnp.where(row < 4, ends[8:16], inner[0:8])
        high = jnp.where(row >= 4, ends[16:24], inner[N - 8 : N])
        whole = jnp.concatenate(
            [ends[0:8], low, inner[8 : N - 8], high, ends[24:32], ends[0:8], low], axis=0
        )
        ft[k] = jnp.where(own_tap, whole, pltpu.roll(whole, EXT + 15, 0))

    def merge(size, rows, packed_rows, sources):
        lane = lanes(size)
        for packed, out, read in sources:
            whole = packed[packed_rows, :]
            for l in range(LAYERS):
                low = pltpu.roll(whole, (N - 32 * l - 8) % N, 1)
                high = pltpu.roll(whole, (104 - 32 * l) % N, 1)
                out[l, rows, :] = jnp.where(lane < 4, low, jnp.where(lane >= N - 4, high, read(l)))

    order = lax.broadcasted_iota(jnp.int32, (EXT, 2 * N), 0)
    lat = 9 * lax.rem(order, 16) + order // 16
    keep = jnp.where(lat < N, 1.0, jnp.where(lat < N + 8, has_north, has_south)) > 0.5
    b1 = jnp.concatenate([consts[4:5, :]] * 2, axis=1)
    b2 = jnp.concatenate([consts[5:6, :]] * 2, axis=1)

    def activate(x, bias):
        x = x + bias
        return jnp.where(keep, x + x * jnp.tanh(x), 0.0)

    def first_layer(k, quarters):
        parts = []
        for b in (0, 2):
            pieces = []
            for t in range(TILES):
                for half in range(2):
                    pieces.append(ft[k, pl.ds(7 + t + b + 72 * half, 8, stride=9), :])
            parts.append(jnp.concatenate(pieces, axis=0).astype(BF16))
        left = jnp.concatenate(parts, axis=1)
        for quarter in range(quarters):
            out = jnp.dot(left, first_w[:, 256 * quarter : 256 * quarter + 256], preferred_element_type=F32)
            out = activate(out, b1)
            at = 2 * k + quarter
            for p in range(2):
                one = out[:, N * p : N * p + N]
                h1[at, p, 16 : 16 + EXT, :] = one.astype(BF16)
                h1[at, p, 0:16, :] = pltpu.roll(one[EXT - 16 : EXT], 1, 0).astype(BF16)
                h1[at, p, 16 + EXT : 32 + EXT, :] = pltpu.roll(one[0:16], 15, 0).astype(BF16)

    def first_body(k, carry):
        first_layer(2 * k, 2)
        first_layer(2 * k + 1, 2)
        rows = pl.ds(pl.multiple_of(16 * k + 8, 8), 16)
        wide = pl.ds(pl.multiple_of(16 * k + 24, 8), 16)
        merge(16, rows, wide, (
            (zq, zm, lambda l: zo[l, wide, :]),
            (vq, vm, lambda l: vo[l, wide, :]),
            (hq, hm, lambda l: t0[l, wide, :]),
        ))
        return carry

    for k in range(7):
        first_body(k, 0)
    for e, (at, inner) in enumerate(((0, 16), (N - 8, 8))):
        merge(8, pl.ds(at, 8), pl.ds(at + 16, 8), (
            (zq, zm, lambda l: ze[e, l, inner : inner + 8, :]),
            (vq, vm, lambda l: ve[e, l, inner : inner + 8, :]),
            (hq, hm, lambda l: te[e, l, inner : inner + 8, :]),
        ))
    for k in (14, 15, 16):
        first_layer(k, 2)
    stores = [
        pltpu.make_async_copy(src, dst, store_sem.at[k])
        for k, (src, dst) in enumerate(((zm, z_out), (vm, v_out), (hm, h_out)))
    ]
    for copy in stores:
        copy.start()

    def second_matmul(k, ref):
        g = k * STEP
        parts = []
        for b in range(3):
            for d in range(3):
                block = h1[pl.ds(g + d // 2, STEP), d % 2, 16 * b : 16 * b + EXT, :]
                parts.append(block.reshape(BLOCK, N))
        left = jnp.concatenate(parts, axis=1)
        ref[...] = jnp.dot(left, second_w[...], preferred_element_type=F32)

    def finish(k, ref):
        for i in range(STEP):
            one = activate(ref[i * EXT : (i + 1) * EXT], b2).astype(BF16)
            sums = lax.dot_general(
                last_w[...], one, (((1,), (1,)), ((), ())), preferred_element_type=F32
            )
            rs[k * STEP + i] = sums[0:24, 0:N]
            re[k * STEP + i, :, 0:16] = sums[0:24, N:EXT]

    held = (d0, d1)
    for k in range(11):
        second_matmul(k, held[k % 2])
        if k:
            finish(k - 1, held[(k - 1) % 2])
    finish(10, held[10 % 2])

    upper = lax.broadcasted_iota(jnp.int32, (8, N), 0) < 4
    for b in range(3):
        blocks = []
        for ref in (rs, re):
            rows = []
            for k in range(N // 8):
                x, y, zz = (ref[2 * k + i, 8 * b : 8 * b + 8, :] for i in range(3))
                y = pltpu.roll(y, 4, 0)
                rows.append(jnp.where(upper, x, y) + jnp.where(upper, y, zz))
            blocks.append(jnp.concatenate(rows, axis=0).T)
        for t in range(TILES):
            for half in range(2):
                block, at = (blocks[0], 16 * t) if t < 8 else (blocks[1], 0)
                at = at + 8 * half
                nat[b, pl.ds(8 + t + 72 * half, 8, stride=9), :] = block[at : at + 8]
        nat[b, 0:8, :] = nat[b, EXT : EXT + 8, :]
    total = nat[0, 7 : 7 + N, :] + nat[1, 8 : 8 + N, :] + nat[2, 9 : 9 + N, :]
    visc_out[...] = jnp.exp(total.T)
    for copy in stores:
        copy.wait()


CONT, MOM, OWN, SPREAD, QC, QM = 32, 16, 32, 128, 144, 144


def step(state):
    vmem = pl.BlockSpec(memory_space=pltpu.VMEM)
    hbm = pl.BlockSpec(memory_space=HBM)
    whole = jax.ShapeDtypeStruct((LAYERS, N, N), F32)
    return pl.pallas_call(
        step_kernel,
        out_shape=(whole, whole, whole, jax.ShapeDtypeStruct((N, N), F32)),
        in_specs=[vmem] * 15,
        out_specs=[hbm] * 3 + [vmem],
        scratch_shapes=[
            pltpu.VMEM((2, FIELDS, EDGE, N), F32),
            pltpu.VMEM((2, LAYERS, EDGE, N), F32),
            pltpu.VMEM((2, LAYERS, EDGE, N), F32),
            pltpu.VMEM((2, LAYERS, EDGE, N), F32),
            pltpu.VMEM((2, LAYERS, EDGE, N), F32),
            pltpu.VMEM((2, 4, EDGE, N), F32),
            pltpu.VMEM((7, PAD, N), F32),
            pltpu.VMEM((PAD, N), F32),
            pltpu.VMEM((PAD, N), F32),
            pltpu.VMEM((PAD, N), F32),
            pltpu.VMEM((PAD, N), F32),
            pltpu.VMEM((4, TALL, N), F32),
            pltpu.VMEM((4, TALL, N), F32),
            pltpu.VMEM((17, EXT + 16, N), F32),
            pltpu.VMEM((LAYERS, N, N), F32),
            pltpu.VMEM((LAYERS, N, N), F32),
            pltpu.VMEM((LAYERS, N, N), F32),
            pltpu.VMEM((PAIRS // 2, 2, EXT + 32, N), BF16),
            pltpu.VMEM((BLOCK, 2 * N), F32),
            pltpu.VMEM((BLOCK, 2 * N), F32),
            pltpu.VMEM((33, 24, N), F32),
            pltpu.VMEM((33, 24, N), F32),
            pltpu.VMEM((3, EXT + 16, N), F32),
            pltpu.SemaphoreType.DMA((3,)),
        ],
        compiler_params=pltpu.CompilerParams(vmem_limit_bytes=24 * 2**20),
        name="step",
    )(*state)


def local(z, v, h, ls, vi, w, grav, conv1, bias1, conv2, bias2, conv3):
    conv1 = jnp.transpose(conv1, (0, 1, 3, 2))
    conv3 = jnp.transpose(conv3, (0, 2, 1, 3))
    held = [pltpu.with_memory_space_constraint(x, HBM) for x in (z, v, h, ls, vi, w, grav, conv1, conv2, conv3, bias1, bias2)]
    return step(exchange(held[:6], *held[6:]))


def solution(mesh):
    block, flat = P(None, "ox", "oy"), P("ox", "oy")
    return jax.shard_map(
        local,
        mesh=mesh,
        in_specs=(block, block, block, flat, flat, block) + (P(),) * 6,
        out_specs=(block, block, block, flat),
        check_vma=False,
    )
```

```python
import jax
import jax.numpy as jnp
from jax import lax
from jax.experimental import pallas as pl
from jax.experimental.pallas import tpu as pltpu
from jax.sharding import PartitionSpec as P

MESH = pl.DeviceIdType.MESH
F32 = jnp.float32
BF16 = jnp.bfloat16

DT = 0.05
REST = 1.4
DRAG = 0.5
LAYERS = 4
N = 128
HID = 64
FIELDS = 16
SEA, VISC, WIND = 12, 13, 14
EXT = N + 16
PAD = N + 32
TALL = N + 40
PAIRS = 72
GROUPS = 33
STEP = 3
TILES = EXT // 16
BLOCK = STEP * EXT


HBM = pltpu.HBM
EDGE = 32


def lanes(rows):
    return lax.broadcasted_iota(jnp.int32, (rows, N), 1)


def near(x):
    return pltpu.roll(x, N - 1, 1), pltpu.roll(x, 1, 1)


def shifted(start, size):
    aligned = start if isinstance(start, int) else pl.multiple_of(start, 8)
    return pl.ds(aligned, size), pl.ds(start + 1, size), pl.ds(start - 1, size)


def continuity(f, press, depth, grav, start, size):
    rows, up, down = shifted(start, size)
    sea = f[SEA, rows, :]
    anomaly = []
    for l in range(LAYERS):
        thick = f[8 + l, rows, :]
        fn, fs = near(f[4 + l, rows, :] * thick)
        fe = f[l, up, :] * f[8 + l, up, :]
        fw = f[l, down, :] * f[8 + l, down, :]
        diverge = (fe - fw) * 0.5 + (fn - fs) * 0.5
        new = thick - DT * sea * diverge
        depth[l, rows, :] = new
        anomaly.append(new - REST)
    faces = [anomaly[3]]
    for l in (2, 1, 0):
        faces.insert(0, faces[0] + anomaly[l])
    total = grav[0] * faces[0]
    press[0, rows, :] = total
    for l in range(1, LAYERS):
        total = total + grav[l] * faces[l]
        press[l, rows, :] = total


def coefficients(visc, up, down):
    return [0.5 * (visc + other) for other in (up, down, *near(visc))]


def viscous(coef, centre, up, down):
    total = None
    for c, q in zip(coef, (up, down, *near(centre))):
        term = c * (q - centre)
        total = term if total is None else total + term
    return total


def coriolis_of(lat, ny):
    return 0.3 + 1.4 * (lat.astype(F32) + 0.5) / (N * ny)


def momentum(f, press, depth, zo, vo, feature_refs, coriolis, start, size):
    rows, up, down = shifted(start, size)
    sea = f[SEA, rows, :]
    coef = coefficients(f[VISC, rows, :], f[VISC, up, :], f[VISC, down, :])
    kinetic = column = None
    for l in range(LAYERS):
        zc, vc = f[l, rows, :], f[4 + l, rows, :]
        pn, ps = near(press[l, rows, :])
        gx = (press[l, up, :] - press[l, down, :]) * 0.5
        gy = (pn - ps) * 0.5
        thick = depth[l, rows, :]
        fz = coriolis * vc - gx + viscous(coef, zc, f[l, up, :], f[l, down, :])
        fv = -coriolis * zc - gy + viscous(coef, vc, f[4 + l, up, :], f[4 + l, down, :])
        if l == 0:
            fz = fz + f[WIND, rows, :] / thick
            fv = fv + f[WIND + 1, rows, :] / thick
        if l == LAYERS - 1:
            fz = fz - DRAG * zc
            fv = fv - DRAG * vc
        z_new = sea * (zc + DT * fz)
        v_new = sea * (vc + DT * fv)
        zo[l, rows, :] = z_new
        vo[l, rows, :] = v_new
        part = thick * (z_new * z_new + v_new * v_new)
        kinetic = part if l == 0 else kinetic + part
        column = thick if l == 0 else column + thick
        if l == 0:
            feature_refs[0][0, rows, :] = z_new
            feature_refs[0][1, rows, :] = v_new
            feature_refs[0][2, rows, :] = sea * (thick - REST)
    feature_refs[0][3, rows, :] = sea * (0.5 * kinetic / column)


def own_pack(read, lane):
    packed = None
    for l in range(4):
        field = read(l)
        for at, shift in ((32 * l + 8, 32 * l + 8), (32 * l + 16, 32 * l + 16 + 8)):
            moved = pltpu.roll(field, shift % N, 1)
            packed = moved if packed is None else jnp.where((lane >= at) & (lane < at + 8), moved, packed)
    return packed


def exchange_kernel(
    z, v, h, ls, vi, w, grav_in, conv1, conv2, conv3, bias1, bias2,
    f0, p0, t0, zo, vo, fs, ft, own, ns, xw, xe, first_w, second_w, last_w, consts,
    sea_i, sb, nb, rows24, c1, c2, c3, grav, s1, s2, load_sem, send_sem, recv_sem,
):
    ox, oy = lax.axis_index("ox"), lax.axis_index("oy")
    nx, ny = lax.axis_size("ox"), lax.axis_size("oy")
    east, west = lax.rem(ox + 1, nx), lax.rem(ox + nx - 1, nx)
    above, below = lax.rem(oy + 1, ny), lax.rem(oy + ny - 1, ny)
    peers = (
        (east, oy), (west, oy),
        (ox, above), (east, above), (west, above),
        (ox, below), (east, below), (west, below),
    )
    barrier = pltpu.get_barrier_semaphore()
    has_north, has_south = oy < ny - 1, oy > 0

    def greet(first_peer, last_peer):
        for peer in peers[first_peer:last_peer]:
            pl.semaphore_signal(barrier, inc=1, device_id=peer, device_id_type=MESH)

    greet(0, 2)
    pl.when(has_north)(lambda: greet(2, 5))
    pl.when(has_south)(lambda: greet(5, 8))

    def load(at, size, sems):
        here, there = pl.ds(at, size), pl.ds(at + 16, size)
        pairs = (
            (ls.at[here], sea_i.at[here]),
            (z.at[:, here], f0.at[0:4, there]),
            (v.at[:, here], f0.at[4:8, there]),
            (h.at[:, here], f0.at[8:12, there]),
            (vi.at[here], f0.at[VISC, there]),
            (w.at[:, here], f0.at[WIND : WIND + 2, there]),
        )
        return [
            pltpu.make_async_copy(src, dst, load_sem.at[sems + k]) for k, (src, dst) in enumerate(pairs)
        ]

    ends = load(0, 8, 0) + load(N - 8, 8, 6)
    middle = load(8, N - 16, 12)
    rest = [
        pltpu.make_async_copy(src, dst, load_sem.at[18 + k])
        for k, (src, dst) in enumerate((
            (conv1, c1), (conv2, c2), (conv3, c3), (grav_in, grav), (bias1, s1), (bias2, s2),
        ))
    ]
    for copy in ends + middle + rest:
        copy.start()

    def pack(at, size):
        rows, src = pl.ds(at, size), pl.ds(at + 16, size)
        lane = lanes(size)
        sea = sea_i[rows, :].astype(F32)
        f0[SEA, src, :] = sea
        to_south = to_north = None
        for a in range(4):
            for l in range(4):
                field = sea if 4 * a + l == SEA else f0[4 * a + l, src, :]
                if a < 2:
                    field = field * sea
                    f0[4 * a + l, src, :] = field
                at_lane = 32 * l + 8 * a
                moved = pltpu.roll(field, at_lane, 1) if at_lane else field
                if to_south is None:
                    to_south = to_north = moved
                else:
                    to_south = jnp.where((lane >= at_lane) & (lane < at_lane + 8), moved, to_south)
                    to_north = jnp.where((lane >= at_lane - 8) & (lane < at_lane), moved, to_north)
        sb[rows, :] = to_south
        nb[rows, :] = to_north

    for copy in ends:
        copy.wait()
    pack(0, 8)
    pack(N - 8, 8)
    for copy in middle:
        copy.wait()
    pack(8, N - 16)
    pl.semaphore_wait(barrier, 2 + 3 * has_north.astype(jnp.int32) + 3 * has_south.astype(jnp.int32))

    first, last = pl.ds(0, 8), pl.ds(N - 8, 8)
    def move(k, src, dst, peer):
        return pltpu.make_async_remote_copy(
            src_ref=src, dst_ref=dst, send_sem=send_sem.at[k], recv_sem=recv_sem.at[k],
            device_id=peer, device_id_type=MESH,
        )

    along = (
        move(0, f0.at[:, N + 8 : N + 16], xw, (east, oy)),
        move(1, f0.at[:, 16:24], xe, (west, oy)),
    )
    northward = (
        move(2, nb.at[last], ns.at[1, 0:8], (east, above)),
        move(3, nb.at[first], ns.at[1, N + 8 : EXT], (west, above)),
        move(4, nb, ns.at[1, 8 : 8 + N], (ox, above)),
    )
    southward = (
        move(5, sb.at[last], ns.at[0, 0:8], (east, below)),
        move(6, sb.at[first], ns.at[0, N + 8 : EXT], (west, below)),
        move(7, sb, ns.at[0, 8 : 8 + N], (ox, below)),
    )

    def start(copies):
        for copy in copies:
            copy.start()

    pl.when(has_north)(lambda: start(northward[:2]))
    pl.when(has_south)(lambda: start(southward[:2]))
    pl.when(has_north)(lambda: start(northward[2:]))
    pl.when(has_south)(lambda: start(southward[2:]))
    start(along)

    @pl.when(jnp.logical_not(has_north))
    def _():
        ns[0] = jnp.ones((EXT, N), F32)

    @pl.when(jnp.logical_not(has_south))
    def _():
        ns[1] = jnp.ones((EXT, N), F32)

    ones = jnp.ones((8, N), F32)
    for rows in (pl.ds(8, 8), pl.ds(N + 16, 8)):
        for k in range(FIELDS):
            f0[k, rows, :] = ones
        for k in range(LAYERS):
            p0[k, rows, :] = ones
    for copy in rest:
        copy.wait()
    build_weights(c1, c2, c3, first_w, second_w, last_w, rows24)
    for l in range(LAYERS):
        consts[l : l + 1, :] = jnp.full((1, N), grav[l], F32)
    for k, bias in enumerate((s1, s2)):
        half = bias[...].reshape(1, HID) * 0.5
        consts[4 + k : 5 + k, :] = jnp.concatenate([half, half], axis=1)

    def inner_continuity(k, carry):
        continuity(f0, p0, t0, grav, CONT * k + 16, CONT)
        return carry

    lax.fori_loop(0, N // CONT, inner_continuity, 0)

    def inner_momentum(k, carry):
        coriolis = coriolis_of(oy * N + lanes(MOM), ny)
        momentum(f0, p0, t0, zo, vo, (fs,), coriolis, MOM * k + 16, MOM)
        return carry

    lax.fori_loop(0, N // MOM, inner_momentum, 0)

    def inner_pack(k, carry):
        src = pl.ds(pl.multiple_of(OWN * k + 16, 8), OWN)
        rows = pl.ds(pl.multiple_of(OWN * k, 8), OWN)
        for a in range(4):
            own[a, rows, :] = own_pack(lambda l: f0[4 * a + l, src, :], lanes(OWN))
        return carry

    lax.fori_loop(0, N // OWN, inner_pack, 0)

    def inner_turn(k, carry):
        block = fs[:, pl.ds(pl.multiple_of(8 * k + 24, 8), 16), :].reshape(HID, N)
        ft[k] = jnp.concatenate([block, block], axis=0).T
        return carry

    lax.fori_loop(0, 13, inner_turn, 0)

    def sent(copies):
        for copy in copies:
            copy.wait_send()

    def received(copies):
        for copy in copies:
            copy.wait_recv()

    sent(along)
    pl.when(has_north)(lambda: sent(northward))
    pl.when(has_south)(lambda: sent(southward))
    received(along)
    pl.when(has_north)(lambda: received(southward))
    pl.when(has_south)(lambda: received(northward))


def exchange(fields, grav, conv1, conv2, conv3, bias1, bias2):
    hbm = pl.BlockSpec(memory_space=HBM)
    vmem = pl.BlockSpec(memory_space=pltpu.VMEM)

    def array(*shape, dtype=F32):
        return jax.ShapeDtypeStruct(shape, dtype)

    return pl.pallas_call(
        exchange_kernel,
        out_shape=(
            array(FIELDS, PAD, N), array(LAYERS, PAD, N), array(LAYERS, PAD, N),
            array(LAYERS, PAD, N), array(LAYERS, PAD, N), array(4, PAD, N),
            array(13, N, N), array(4, N, N), array(2, EXT, N),
            array(FIELDS, 8, N), array(FIELDS, 8, N),
            array(2 * N, 8 * HID, dtype=BF16), array(18 * HID, 4 * HID, dtype=BF16),
            array(32, 2 * N, dtype=BF16), array(8, N),
        ),
        in_specs=[hbm] * 12,
        out_specs=(vmem,) * 15,
        scratch_shapes=[
            pltpu.VMEM((N, N), jnp.int32),
            pltpu.VMEM((N, N), F32),
            pltpu.VMEM((N, N), F32),
            pltpu.VMEM((32, 2 * N), F32),
            pltpu.VMEM(conv1.shape, BF16),
            pltpu.VMEM(conv2.shape, BF16),
            pltpu.VMEM(conv3.shape, BF16),
            pltpu.SMEM((LAYERS,), F32),
            pltpu.VMEM((HID,), F32),
            pltpu.VMEM((HID,), F32),
            pltpu.SemaphoreType.DMA((24,)),
            pltpu.SemaphoreType.DMA((8,)),
            pltpu.SemaphoreType.DMA((8,)),
        ],
        compiler_params=pltpu.CompilerParams(
            collective_id=0, has_side_effects=True, vmem_limit_bytes=16 * 2**20
        ),
        name="exchange",
    )(*fields, grav, conv1, conv2, conv3, bias1, bias2)


def build_weights(conv1, conv2, conv3, first_w, second_w, last_w, rows24):
    lane = lax.broadcasted_iota(jnp.int32, (8, N), 1)
    right = lane >= HID
    row = lax.broadcasted_iota(jnp.int32, (8, N), 0)

    nt = (((1,), (1,)), ((), ()))
    taps = {}
    for a in range(3):
        for b in range(3):
            one = conv1[a, b].astype(F32) * 0.5
            taps[a, b] = jnp.concatenate([one, one], axis=1)
    for b in range(3):
        for c in range(4):
            vecs = [jnp.broadcast_to(taps[a, b][c : c + 1], (8, N)) for a in range(3)]
            for jp in range(4):
                parts = []
                for i in range(2):
                    gap = row + 8 * i - 2 * jp - jnp.where(right, 1, 0) - 4
                    val = jnp.zeros((8, N), F32)
                    for a in range(3):
                        val = jnp.where(gap == a, vecs[a], val)
                    parts.append(val)
                start = 64 * b + 16 * c
                first_w[start : start + 16, N * jp : N * jp + N] = jnp.concatenate(parts, 0).astype(BF16)
    first_w[192:256, :] = jnp.zeros((64, 8 * HID), BF16)

    eye = lax.broadcasted_iota(jnp.int32, (HID, HID), 0) == lax.broadcasted_iota(jnp.int32, (HID, HID), 1)
    eye = jnp.where(eye, 0.5, 0.0).astype(BF16)
    side = lax.broadcasted_iota(jnp.int32, (HID, N), 1) >= HID
    for b in range(3):
        turned = []
        for a in range(3):
            one = conv2[a, b]
            both = jnp.concatenate([one, one], axis=0)
            turned.append(lax.dot_general(eye, both, nt, preferred_element_type=F32))
        zero = jnp.zeros((HID, N), F32)
        for m in range(6):
            for jp in range(2):
                tap = m - 2 * jp
                left = turned[tap] if 0 <= tap < 3 else zero
                other = turned[tap - 1] if 0 <= tap - 1 < 3 else zero
                start = (6 * b + m) * HID
                second_w[start : start + HID, N * jp : N * jp + N] = jnp.where(side, other, left).astype(BF16)

    rows24[...] = jnp.zeros((32, 2 * N), F32)
    for b in range(3):
        for place, i in ((0, 3), (1, 4), (2, 5), (5, 0), (6, 1), (7, 2)):
            for m in range(4):
                a = m - i + 2
                if 0 <= a < 3:
                    rows24[8 * b + place : 8 * b + place + 1, HID * m : HID * m + HID] = conv3[a, 0, b : b + 1].astype(F32)
    last_w[...] = rows24[...].astype(BF16)


def step_kernel(
    f0, p0, t0, zo, vo, fs0, ft0, own, ns, xw, xe, first_w, second_w, last_w, consts,
    z_out, v_out, h_out, visc_out,
    fe, pe, te, ze, ve, fse, q, pq, hq, zq, vq, fsq, fs, ft, zm, vm, hm, h1, d0, d1, rs, re, nat,
    store_sem,
):
    oy, ny = lax.axis_index("oy"), lax.axis_size("oy")
    has_north = (oy < ny - 1).astype(F32)
    has_south = (oy > 0).astype(F32)
    ones = jnp.ones((8, N), F32)
    grav = [consts[l : l + 1, :] for l in range(LAYERS)]

    for e, (rows, src) in enumerate((((8, xw), (16, 16)), ((0, N), (16, xe)))):
        (halo_at, halo), (own_at, own_from) = (rows, src) if e == 0 else (src, rows)
        pad = 0 if e == 0 else 24
        for k in range(FIELDS):
            fe[e, k, halo_at : halo_at + 8, :] = halo[k]
            fe[e, k, own_at : own_at + 16, :] = f0[k, own_from : own_from + 16, :]
            fe[e, k, pad : pad + 8, :] = ones
        inner_at, inner_from = (24, 24) if e == 0 else (0, N)
        for k in range(LAYERS):
            pe[e, k, pad : pad + 8, :] = ones
            pe[e, k, inner_at : inner_at + 8, :] = p0[k, inner_from : inner_from + 8, :]
    for e in range(2):
        continuity(fe.at[e], pe.at[e], te.at[e], grav, 8, 16)
    for e in range(2):
        coriolis = coriolis_of(oy * N + lanes(16), ny)
        momentum(fe.at[e], pe.at[e], te.at[e], ze.at[e], ve.at[e], (fse.at[e],), coriolis, 8, 16)

    for k in range(7):
        q[k, 0:8, :] = ones
        q[k, PAD - 8 : PAD, :] = ones
    pq[0:8, :] = ones
    pq[PAD - 8 : PAD, :] = ones
    for c in range(4):
        fs[c, EXT + 8 : TALL, :] = jnp.zeros((TALL - EXT - 8, N), F32)
        fsq[c, EXT + 8 : TALL, :] = jnp.zeros((TALL - EXT - 8, N), F32)

    def spread(start, size, groups):
        lane = lanes(size)
        part = lax.rem(lane, 32)
        seg = lane // 32
        inside = jnp.where(part < 8, has_south, jnp.where(part < 24, 1.0, has_north))
        rows = pl.ds(start + 8 if isinstance(start, int) else pl.multiple_of(start + 8, 8), size)
        src = pl.ds(start if isinstance(start, int) else pl.multiple_of(start, 8), size)
        from_north, from_south = ns[0, src, :], ns[1, src, :]
        full = []
        for a in range(4):
            high = pltpu.roll(from_north, (24 - 8 * a) % N, 1)
            low = pltpu.roll(from_south, (8 - 8 * a) % N, 1)
            full.append(jnp.where(part < 8, low, jnp.where(part < 24, groups(a), high)))
        q[0, rows, :] = full[0] * inside
        q[1, rows, :] = full[1] * inside
        q[2, rows, :] = full[2]
        for k, s in ((3, 0), (4, 1)):
            one = jnp.where(seg == s, full[3] * inside, 0.0)
            one = one + pltpu.roll(one, 32, 1)
            q[k, rows, :] = one + pltpu.roll(one, 64, 1)
        for k, s in ((5, 2), (6, 3)):
            q[k, rows, :] = jnp.where(seg == 0, pltpu.roll(full[3], N - 32 * s, 1), 0.0)

    for at, strip in ((0, xw), (N + 8, xe)):
        spread(at, 8, lambda a: own_pack(lambda l: strip[4 * a + l], lanes(8)))

    def spread_body(k, carry):
        rows = pl.ds(pl.multiple_of(SPREAD * k, 8), SPREAD)
        spread(SPREAD * k + 8, SPREAD, lambda a: own[a, rows, :])
        return carry

    lax.fori_loop(0, N // SPREAD, spread_body, 0)

    def packed_continuity(k, carry):
        size = QC
        lane = lanes(size)
        part, seg = lax.rem(lane, 32), lane // 32
        inside = jnp.where(part < 8, has_south, jnp.where(part < 24, 1.0, has_north))
        weight = jnp.where(seg == 0, grav[0], jnp.where(seg == 1, grav[1], jnp.where(seg == 2, grav[2], grav[3])))
        rows, up, down = shifted(size * k + 8, size)
        thick = q[2, rows, :]
        fn, fs_ = near(q[1, rows, :] * thick)
        fe_ = q[0, up, :] * q[2, up, :]
        fw_ = q[0, down, :] * q[2, down, :]
        diverge = (fe_ - fw_) * 0.5 + (fn - fs_) * 0.5
        new = thick - DT * q[3, rows, :] * diverge
        hq[rows, :] = new
        a = new - REST
        face = a
        for n in (1, 2, 3):
            face = face + jnp.where(seg < 4 - n, pltpu.roll(a, N - 32 * n, 1), 0.0)
        term = weight * face
        total = term
        for n in (1, 2, 3):
            total = total + jnp.where(seg >= n, pltpu.roll(term, 32 * n, 1), 0.0)
        pq[rows, :] = total * inside
        return carry

    lax.fori_loop(0, EXT // QC, packed_continuity, 0)

    def packed_momentum(k, carry):
        size = QM
        lane = lanes(size)
        part, seg = lax.rem(lane, 32), lane // 32
        coriolis = coriolis_of(oy * N + part + jnp.where(part < 16, -8, 104), ny)
        drag = jnp.where(seg == 3, DRAG, 0.0)
        rows, up, down = shifted(size * k + 8, size)
        zc, vc, sea = q[0, rows, :], q[1, rows, :], q[3, rows, :]
        coef = coefficients(q[4, rows, :], q[4, up, :], q[4, down, :])
        pn, ps = near(pq[rows, :])
        gx = (pq[up, :] - pq[down, :]) * 0.5
        gy = (pn - ps) * 0.5
        thick = hq[rows, :]
        fz = coriolis * vc - gx + viscous(coef, zc, q[0, up, :], q[0, down, :])
        fv = -coriolis * zc - gy + viscous(coef, vc, q[1, up, :], q[1, down, :])
        fz = fz + q[5, rows, :] / thick - drag * zc
        fv = fv + q[6, rows, :] / thick - drag * vc
        z_new = sea * (zc + DT * fz)
        v_new = sea * (vc + DT * fv)
        zq[rows, :] = z_new
        vq[rows, :] = v_new
        sums = []
        for one in (thick * (z_new * z_new + v_new * v_new), thick):
            one = one + pltpu.roll(one, 64, 1)
            sums.append(one + pltpu.roll(one, 32, 1))
        fsq[0, rows, :] = z_new
        fsq[1, rows, :] = v_new
        fsq[2, rows, :] = sea * (thick - REST)
        fsq[3, rows, :] = sea * (0.5 * sums[0] / sums[1])
        return carry

    lax.fori_loop(0, EXT // QM, packed_momentum, 0)

    for c in range(4):
        fs[c, 8:24, :] = fse[0, c, 8:24, :]
        fs[c, 24:40, :] = fs0[c, 24:40, :]
        fs[c, N - 8 : N + 8, :] = fs0[c, N - 8 : N + 8, :]
        fs[c, N + 8 : N + 24, :] = fse[1, c, 8:24, :]

    row = lax.broadcasted_iota(jnp.int32, (8, N), 0)
    own_tap = lax.broadcasted_iota(jnp.int32, (EXT + 16, N), 1) < HID

    def turned(ref, k):
        block = ref[:, 8 * k + 8 : 8 * k + 24, :].reshape(HID, N)
        return jnp.concatenate([block, block], axis=0).T

    for k in range(17):
        inner = ft0[k - 2] if 2 <= k <= 14 else turned(fs, k)
        ends = turned(fsq, k)
        low = jnp.where(row < 4, ends[8:16], inner[0:8])
        high = jnp.where(row >= 4, ends[16:24], inner[N - 8 : N])
        whole = jnp.concatenate(
            [ends[0:8], low, inner[8 : N - 8], high, ends[24:32], ends[0:8], low], axis=0
        )
        ft[k, 0 : EXT + 16, :] = jnp.where(own_tap, whole, pltpu.roll(whole, EXT + 15, 0))

    def merge(size, rows, packed_rows, sources):
        lane = lanes(size)
        for packed, out, read in sources:
            whole = packed[packed_rows, :]
            for l in range(LAYERS):
                low = pltpu.roll(whole, (N - 32 * l - 8) % N, 1)
                high = pltpu.roll(whole, (104 - 32 * l) % N, 1)
                out[l, rows, :] = jnp.where(lane < 4, low, jnp.where(lane >= N - 4, high, read(l)))

    order = lax.broadcasted_iota(jnp.int32, (EXT, 2 * N), 0)
    lat = 9 * lax.rem(order, 16) + order // 16
    keep = jnp.where(lat < N, 1.0, jnp.where(lat < N + 8, has_north, has_south)) > 0.5
    b1 = jnp.concatenate([consts[4:5, :]] * 2, axis=1)
    b2 = jnp.concatenate([consts[5:6, :]] * 2, axis=1)

    def activate(x, bias):
        x = x + bias
        return jnp.where(keep, x + x * jnp.tanh(x), 0.0)

    def first_layer(k, quarters):
        parts = []
        for b in (0, 2):
            pieces = []
            for t in range(TILES):
                for half in range(2):
                    pieces.append(ft[k, pl.ds(7 + t + b + 72 * half, 8, stride=9), :])
            parts.append(jnp.concatenate(pieces, axis=0).astype(BF16))
        left = jnp.concatenate(parts, axis=1)
        for quarter in range(quarters):
            out = jnp.dot(left, first_w[:, 256 * quarter : 256 * quarter + 256], preferred_element_type=F32)
            out = activate(out, b1)
            at = 2 * k + quarter
            for p in range(2):
                one = out[:, N * p : N * p + N]
                h1[at, p, 16 : 16 + EXT, :] = one.astype(BF16)
                h1[at, p, 0:16, :] = pltpu.roll(one[EXT - 16 : EXT], 1, 0).astype(BF16)
                h1[at, p, 16 + EXT : 32 + EXT, :] = pltpu.roll(one[0:16], 15, 0).astype(BF16)

    def first_body(k, carry):
        first_layer(2 * k, 2)
        first_layer(2 * k + 1, 2)
        rows = pl.ds(pl.multiple_of(16 * k + 8, 8), 16)
        wide = pl.ds(pl.multiple_of(16 * k + 24, 8), 16)
        merge(16, rows, wide, (
            (zq, zm, lambda l: zo[l, wide, :]),
            (vq, vm, lambda l: vo[l, wide, :]),
            (hq, hm, lambda l: t0[l, wide, :]),
        ))
        return carry

    for k in range(7):
        first_body(k, 0)
    for e, (at, inner) in enumerate(((0, 16), (N - 8, 8))):
        merge(8, pl.ds(at, 8), pl.ds(at + 16, 8), (
            (zq, zm, lambda l: ze[e, l, inner : inner + 8, :]),
            (vq, vm, lambda l: ve[e, l, inner : inner + 8, :]),
            (hq, hm, lambda l: te[e, l, inner : inner + 8, :]),
        ))
    for k in (14, 15, 16):
        first_layer(k, 2)
    stores = [
        pltpu.make_async_copy(src, dst, store_sem.at[k])
        for k, (src, dst) in enumerate(((zm, z_out), (vm, v_out), (hm, h_out)))
    ]
    for copy in stores:
        copy.start()

    def second_matmul(k, ref):
        g = k * STEP
        parts = []
        for b in range(3):
            for d in range(3):
                block = h1[pl.ds(g + d // 2, STEP), d % 2, 16 * b : 16 * b + EXT, :]
                parts.append(block.reshape(BLOCK, N))
        left = jnp.concatenate(parts, axis=1)
        ref[...] = jnp.dot(left, second_w[...], preferred_element_type=F32)

    def finish(k, ref):
        for i in range(STEP):
            one = activate(ref[i * EXT : (i + 1) * EXT], b2).astype(BF16)
            sums = lax.dot_general(
                last_w[...], one, (((1,), (1,)), ((), ())), preferred_element_type=F32
            )
            rs[k * STEP + i] = sums[0:24, 0:N]
            re[k * STEP + i, :, 0:16] = sums[0:24, N:EXT]

    held = (d0, d1)
    for k in range(11):
        second_matmul(k, held[k % 2])
        if k:
            finish(k - 1, held[(k - 1) % 2])
    finish(10, held[10 % 2])

    upper = lax.broadcasted_iota(jnp.int32, (8, N), 0) < 4
    for b in range(3):
        blocks = []
        for ref in (rs, re):
            rows = []
            for k in range(N // 8):
                x, y, zz = (ref[2 * k + i, 8 * b : 8 * b + 8, :] for i in range(3))
                y = pltpu.roll(y, 4, 0)
                rows.append(jnp.where(upper, x, y) + jnp.where(upper, y, zz))
            blocks.append(jnp.concatenate(rows, axis=0).T)
        for t in range(TILES):
            for half in range(2):
                block, at = (blocks[0], 16 * t) if t < 8 else (blocks[1], 0)
                at = at + 8 * half
                nat[b, pl.ds(8 + t + 72 * half, 8, stride=9), :] = block[at : at + 8]
        nat[b, 0:8, :] = nat[b, EXT : EXT + 8, :]
    total = nat[0, 7 : 7 + N, :] + nat[1, 8 : 8 + N, :] + nat[2, 9 : 9 + N, :]
    visc_out[...] = jnp.exp(total.T)
    for copy in stores:
        copy.wait()


CONT, MOM, OWN, SPREAD, QC, QM = 32, 16, 32, 128, 144, 144


def step(state):
    vmem = pl.BlockSpec(memory_space=pltpu.VMEM)
    hbm = pl.BlockSpec(memory_space=HBM)
    whole = jax.ShapeDtypeStruct((LAYERS, N, N), F32)
    return pl.pallas_call(
        step_kernel,
        out_shape=(whole, whole, whole, jax.ShapeDtypeStruct((N, N), F32)),
        in_specs=[vmem] * 15,
        out_specs=[hbm] * 3 + [vmem],
        scratch_shapes=[
            pltpu.VMEM((2, FIELDS, EDGE, N), F32),
            pltpu.VMEM((2, LAYERS, EDGE, N), F32),
            pltpu.VMEM((2, LAYERS, EDGE, N), F32),
            pltpu.VMEM((2, LAYERS, EDGE, N), F32),
            pltpu.VMEM((2, LAYERS, EDGE, N), F32),
            pltpu.VMEM((2, 4, EDGE, N), F32),
            pltpu.VMEM((7, PAD, N), F32),
            pltpu.VMEM((PAD, N), F32),
            pltpu.VMEM((PAD, N), F32),
            pltpu.VMEM((PAD, N), F32),
            pltpu.VMEM((PAD, N), F32),
            pltpu.VMEM((4, TALL, N), F32),
            pltpu.VMEM((4, TALL, N), F32),
            pltpu.VMEM((17, EXT + 32, N), F32),
            pltpu.VMEM((LAYERS, N, N), F32),
            pltpu.VMEM((LAYERS, N, N), F32),
            pltpu.VMEM((LAYERS, N, N), F32),
            pltpu.VMEM((PAIRS // 2, 2, EXT + 32, N), BF16),
            pltpu.VMEM((BLOCK, 2 * N), F32),
            pltpu.VMEM((BLOCK, 2 * N), F32),
            pltpu.VMEM((33, 24, N), F32),
            pltpu.VMEM((33, 24, N), F32),
            pltpu.VMEM((3, EXT + 32, N), F32),
            pltpu.SemaphoreType.DMA((3,)),
        ],
        compiler_params=pltpu.CompilerParams(vmem_limit_bytes=24 * 2**20),
        name="step",
    )(*state)


def local(z, v, h, ls, vi, w, grav, conv1, bias1, conv2, bias2, conv3):
    conv1 = jnp.transpose(conv1, (0, 1, 3, 2))
    conv3 = jnp.transpose(conv3, (0, 2, 1, 3))
    held = [pltpu.with_memory_space_constraint(x, HBM) for x in (z, v, h, ls, vi, w, grav, conv1, conv2, conv3, bias1, bias2)]
    return step(exchange(held[:6], *held[6:]))


def solution(mesh):
    block, flat = P(None, "ox", "oy"), P("ox", "oy")
    return jax.shard_map(
        local,
        mesh=mesh,
        in_specs=(block, block, block, flat, flat, block) + (P(),) * 6,
        out_specs=(block, block, block, flat),
        check_vma=False,
    )
```
